32 devices in a mesh: gx: 2 (over y), gy: 4 (over x, core), gz: 4 (over z).
Axes of the slice: x: 2, y: 2, z: 4, core: 2. Of those that a mesh axis runs over, the one named last changes fastest.
Arguments:
- positions: float32 [3, 8, 16, 512], P(None, 'gx', 'gy', 'gz'), may hold values from 0 to 1
- charges: float32 [8, 16, 512], P('gx', 'gy', 'gz'), may hold values from -1.2 to 1.2
- counts: int32 [8, 16, 16], P('gx', 'gy', 'gz'), may hold values from 16 to 32
- moment_shift: bfloat16 [8, 81, 81], replicated, may hold values from -0.25 to 0.25
- far_operators: bfloat16 [81, 25600], replicated, may hold values from -0.046875 to 0.046875
- local_shift: bfloat16 [8, 81, 81], replicated, may hold values from -0.625 to 0.625
- lattice_operator: bfloat16 [81, 81], replicated, may hold values from -0.625 to 0.625
Outputs:
- potential: float32 [8, 16, 512], P('gx', 'gy', 'gz')
- electric_field: float32 [3, 8, 16, 512], P(None, 'gx', 'gy', 'gz')
The draws below stay inside these ranges and needn't reach their ends.
Inputs may be any that keep to these rules, and one draw needn't show every extreme that they name: `counts`: number of live charges in each leaf; slots at or past it are pads.
All inputs are finite; a program needn't handle non-finite values.
Results may differ from the reference program's by a relative error of at most 0.00035.
Values sent between devices are 32-bit elements; how exact they have to be, the bound alone decides.
A program may use at most 256 MiB of HBM per device.

```python
import jax
import jax.numpy as jnp
import numpy as np
from jax import lax

ORDER = 8
TERMS = 81
SLOTS = 32
OPERATOR_COLUMNS = 25600
GRID_X = 8
GRID_Y = 16
GRID_Z = 16


def touch_ends(entries, own_key, least, top_value):
    shape = entries.shape
    spot = [jax.random.randint(jax.random.fold_in(own_key, axis), (), 0, shape[axis]) for axis in range(len(shape))]
    entries = entries.at[tuple(spot)].set(least)
    longest = shape.index(max(shape))
    spot[longest] = (spot[longest] + 1) % shape[longest]
    return entries.at[tuple(spot)].set(top_value)


def block_levels(own_key, dims, shards, least, top_value):
    gain = 1.0
    for axis_at, blocks in shards:
        steps = jax.random.uniform(jax.random.fold_in(jax.random.fold_in(own_key, 6), axis_at), (blocks,), jnp.float32, least / len(shards), top_value / len(shards))
        gain = gain * jnp.repeat(jnp.exp(steps), dims[axis_at] // blocks).reshape((-1,) + (1,) * (len(dims) - 1 - axis_at))
    return gain


def bell_draw(rng, shape, deviation, most, split=(), kind=jnp.bfloat16):
    drawn = jax.random.normal(rng, shape, jnp.float32) * deviation
    if len(split) > 0:
        drawn = block_levels(rng, shape, split, -0.22, 0.18) * drawn
    return jnp.clip(drawn, min=-most, max=most).astype(kind)


def setup_inputs(seed: int = 0) -> dict:
    seeds = jax.random.split(jax.random.key(seed), 8)
    return {
        "positions": jnp.clip(1.0 * jax.random.uniform(seeds[0], (3, GRID_X, GRID_Y, GRID_Z * SLOTS), jnp.float32) ** block_levels(seeds[0], (3, GRID_X, GRID_Y, GRID_Z * SLOTS), ((1, 2), (2, 4), (3, 4)), -0.2, 0.2), 0.0, 1.0),
        "charges": bell_draw(seeds[1], (GRID_X, GRID_Y, GRID_Z * SLOTS), 0.2, 1.2, ((0, 2), (1, 4), (2, 4)), jnp.float32),
        "counts": touch_ends(jax.random.randint(seeds[2], (GRID_X, GRID_Y, GRID_Z), SLOTS // 2, SLOTS + 1), jax.random.fold_in(seeds[2], 1), SLOTS // 2, SLOTS).astype(jnp.int32),
        "moment_shift": bell_draw(seeds[3], (8, TERMS, TERMS), (8 * TERMS) ** -0.5, 0.25),
        "far_operators": bell_draw(seeds[4], (TERMS, OPERATOR_COLUMNS), (189 * TERMS) ** -0.5, 0.046875),
        "local_shift": bell_draw(seeds[5], (8, TERMS, TERMS), TERMS ** -0.5, 0.625),
        "lattice_operator": bell_draw(seeds[6], (TERMS, TERMS), TERMS ** -0.5, 0.625),
    }


SOFTENING = 0.0625

def offset_table():
    listed = []
    for shift_x in range(-3, 4):
        for shift_y in range(-3, 4):
            for shift_z in range(-3, 4):
                if max(abs(shift_x), abs(shift_y), abs(shift_z)) >= 2:
                    listed.append((shift_x, shift_y, shift_z))
    return np.array(listed, dtype=np.int32)

def exponent_table(degree):
    listed = []
    for accumulated in range(degree + 1):
        for height in (0, 1):
            for power_x in range(accumulated - height + 1):
                listed.append((power_x, accumulated - height - power_x, height))
    return np.array(listed, dtype=np.int32)

def power_stack(values, degree):
    listed = [jnp.ones_like(values)]
    for exponent in range(degree):
        listed.append(listed[-1] * values)
    return jnp.stack(listed)

def slope_stack(powers, degree):
    listed = [jnp.zeros_like(powers[0])]
    for exponent in range(1, degree + 1):
        listed.append(float(exponent) * powers[exponent - 1])
    return jnp.stack(listed)

def monomials(relative, degree, with_slopes):
    centred = relative - 0.5
    exponents = exponent_table(degree)
    powers_x = power_stack(centred[0], degree)
    powers_y = power_stack(centred[1], degree)
    powers_z = power_stack(centred[2], degree)
    part_x = powers_x[exponents[:, 0]]
    part_y = powers_y[exponents[:, 1]]
    part_z = powers_z[exponents[:, 2]]
    values = part_x * part_y * part_z
    if not with_slopes:
        return (values, None)
    slope_x = slope_stack(powers_x, degree)[exponents[:, 0]]
    slope_y = slope_stack(powers_y, degree)[exponents[:, 1]]
    slope_z = slope_stack(powers_z, degree)[exponents[:, 2]]
    slopes = (slope_x * part_y * part_z, part_x * slope_y * part_z, part_x * part_y * slope_z)
    return (values, slopes)

def to_moments(stacked):
    values = monomials(stacked[:3], ORDER, False)[0]
    return lax.optimization_barrier(jnp.sum(values * stacked[3][None], axis=-1))

def moments_up(child, operators):
    term_count, size_x, size_y, size_z = child.shape
    grouped = child.reshape(term_count, size_x // 2, 2, size_y // 2, 2, size_z // 2, 2)
    accumulated = jnp.zeros((term_count, size_x // 2 * (size_y // 2) * (size_z // 2)), jnp.float32)
    for octant in range(8):
        child_piece = grouped[:, :, octant >> 2 & 1, :, octant >> 1 & 1, :, octant & 1].reshape(term_count, -1)
        accumulated = accumulated + jnp.dot(operators[octant], child_piece, precision=lax.Precision.HIGHEST)
    return accumulated.reshape(term_count, size_x // 2, size_y // 2, size_z // 2)

def locals_down(parent, operators):
    term_count, size_x, size_y, size_z = parent.shape
    flat_parent = parent.reshape(term_count, -1)
    pieces = [jnp.dot(operators[octant], flat_parent, precision=lax.Precision.HIGHEST).reshape(term_count, size_x, size_y, size_z) for octant in range(8)]
    stacked = jnp.stack(pieces, axis=1).reshape(term_count, 2, 2, 2, size_x, size_y, size_z)
    return stacked.transpose(0, 4, 1, 5, 2, 6, 3).reshape(term_count, 2 * size_x, 2 * size_y, 2 * size_z)

def far_terms(source, grid_shape, coords, parity, operators):
    shifts = offset_table()
    offset_count = shifts.shape[0]
    term_count = source.shape[0]
    shift_x = jnp.asarray(shifts[:, 0:1])
    shift_y = jnp.asarray(shifts[:, 1:2])
    shift_z = jnp.asarray(shifts[:, 2:3])
    size_x, size_y, size_z = grid_shape
    coord_x, coord_y, coord_z = coords
    flat_index = ((coord_x[None, :] + shift_x) % size_x * size_y + (coord_y[None, :] + shift_y) % size_y) * size_z + (coord_z[None, :] + shift_z) % size_z
    picked = jnp.take(source, flat_index, axis=1)
    if parity is not None:
        odd_x, odd_y, odd_z = parity
        admitted = (shift_x >= -2 - odd_x[None, :]) & (shift_x <= 3 - odd_x[None, :])
        admitted = admitted & (shift_y >= -2 - odd_y[None, :]) & (shift_y <= 3 - odd_y[None, :])
        admitted = admitted & (shift_z >= -2 - odd_z[None, :]) & (shift_z <= 3 - odd_z[None, :])
        picked = picked * admitted.astype(jnp.float32)[None]
    ordered = jnp.transpose(picked, (1, 0, 2)).reshape(offset_count * term_count, -1)
    return jnp.dot(operators[:, :offset_count * term_count], ordered, precision=lax.Precision.HIGHEST)

def level_terms(moments, restrict, operators):
    term_count, size_x, size_y, size_z = moments.shape
    target_count = size_x * size_y * size_z
    block_size = min(target_count, 512)
    blocks = jnp.arange(target_count, dtype=jnp.int32).reshape(target_count // block_size, block_size)
    source = moments.reshape(term_count, target_count)

    def one_block(block_rows):
        coord_x = block_rows // (size_y * size_z)
        coord_y = block_rows // size_z % size_y
        coord_z = block_rows % size_z
        parity = (coord_x % 2, coord_y % 2, coord_z % 2) if restrict else None
        return far_terms(source, (size_x, size_y, size_z), (coord_x, coord_y, coord_z), parity, operators)
    result = lax.map(one_block, blocks)
    return result.transpose(1, 0, 2).reshape(term_count, size_x, size_y, size_z)

def evaluate(extended, slab_local, live_mask):
    term_count, size_x, size_y, size_z = slab_local.shape
    slot_count = extended.shape[4]
    target = extended[:, 1:size_x + 1, 1:size_y + 1, 1:size_z + 1, :]
    self_mask = (1.0 - jnp.eye(slot_count, dtype=jnp.float32))[:, None, None, None, :]
    near_potential = jnp.zeros((size_x, size_y, size_z, slot_count), jnp.float32)
    near_x = jnp.zeros_like(near_potential)
    near_y = jnp.zeros_like(near_potential)
    near_z = jnp.zeros_like(near_potential)
    for shift_x in (-1, 0, 1):
        for shift_y in (-1, 0, 1):
            for shift_z in (-1, 0, 1):
                source = extended[:, 1 + shift_x:1 + shift_x + size_x, 1 + shift_y:1 + shift_y + size_y, 1 + shift_z:1 + shift_z + size_z, :]
                source = jnp.moveaxis(source, 4, 1)[..., None]
                delta_x = target[0][None] - source[0] - float(shift_x)
                delta_y = target[1][None] - source[1] - float(shift_y)
                delta_z = target[2][None] - source[2] - float(shift_z)
                distance = delta_x * delta_x + delta_y * delta_y + delta_z * delta_z + SOFTENING
                inverse = lax.rsqrt(distance)
                weight = source[3] * inverse
                if shift_x == 0 and shift_y == 0 and (shift_z == 0):
                    weight = weight * self_mask
                near_potential = near_potential + lax.optimization_barrier(jnp.sum(weight, axis=0))
                cubic_weight = weight * inverse * inverse
                near_x = near_x + lax.optimization_barrier(jnp.sum(cubic_weight * delta_x, axis=0))
                near_y = near_y + lax.optimization_barrier(jnp.sum(cubic_weight * delta_y, axis=0))
                near_z = near_z + lax.optimization_barrier(jnp.sum(cubic_weight * delta_z, axis=0))
    values, slopes = monomials(target[:3], ORDER, True)
    expanded = slab_local[..., None]
    potential = (near_potential + lax.optimization_barrier(jnp.sum(expanded * values, axis=0))) * live_mask
    field_out = jnp.stack([near_x - lax.optimization_barrier(jnp.sum(expanded * slopes[0], axis=0)), near_y - lax.optimization_barrier(jnp.sum(expanded * slopes[1], axis=0)), near_z - lax.optimization_barrier(jnp.sum(expanded * slopes[2], axis=0))]) * live_mask[None]
    return (potential, field_out)

def reference(positions, charges, counts, moment_shift, far_operators, local_shift, lattice_operator):
    slots_index = jnp.arange(SLOTS, dtype=jnp.int32)
    live_mask = (slots_index[None, None, None, :] < counts[..., None]).astype(jnp.float32)
    weights = charges.reshape(GRID_X, GRID_Y, GRID_Z, SLOTS) * live_mask
    stacked = jnp.concatenate([positions.reshape(3, GRID_X, GRID_Y, GRID_Z, SLOTS), weights[None]], axis=0)
    upward = moment_shift.astype(jnp.float32)
    across = far_operators.astype(jnp.float32)
    downward = local_shift.astype(jnp.float32)
    lattice = lattice_operator.astype(jnp.float32)
    moments_leaf = jnp.moveaxis(lax.map(to_moments, jnp.moveaxis(stacked, 1, 0)), 0, 1)
    moments_mid = moments_up(moments_leaf, upward)
    moments_upper = moments_up(moments_mid, upward)
    moments_top = moments_up(moments_upper, upward)
    term_count = moments_top.shape[0]
    root_moments = lax.optimization_barrier(jnp.sum(moments_top.reshape(term_count, -1), axis=1))
    lattice_term = jnp.dot(lattice, root_moments[:, None], precision=lax.Precision.HIGHEST).reshape(term_count, 1, 1, 1)
    local_top = 0.125 * (level_terms(moments_top, False, across) + lattice_term)
    local_upper = 0.25 * level_terms(moments_upper, True, across) + locals_down(local_top, downward)
    local_mid = 0.5 * level_terms(moments_mid, True, across) + locals_down(local_upper, downward)
    local_leaf = level_terms(moments_leaf, True, across) + locals_down(local_mid, downward)
    padded = jnp.pad(stacked, ((0, 0), (1, 1), (1, 1), (1, 1), (0, 0)), mode='wrap')

    def one_slab(slab_row):
        extended = lax.dynamic_slice_in_dim(padded, slab_row, 3, axis=1)
        slab_local = lax.dynamic_slice_in_dim(local_leaf, slab_row, 1, axis=1)
        slab_live = lax.dynamic_slice_in_dim(live_mask, slab_row, 1, axis=0)
        return evaluate(extended, slab_local, slab_live)
    potential, field_out = lax.map(one_slab, jnp.arange(GRID_X, dtype=jnp.int32))
    potential = potential.reshape(GRID_X, GRID_Y, GRID_Z * SLOTS)
    field_out = jnp.moveaxis(field_out, 0, 1).reshape(3, GRID_X, GRID_Y, GRID_Z * SLOTS)
    return (potential, field_out)
```

```python
import jax
import jax.numpy as jnp
import numpy as np
from jax import lax
from jax.experimental import pallas as pl
from jax.experimental.pallas import tpu as pltpu
from jax.sharding import PartitionSpec as P

ORDER = 8
SLOTS = 32
SOFTENING = 0.0625
LANES = 128
HALO = 2
F32 = jnp.float32
BF16 = jnp.bfloat16
NT = (((1,), (1,)), ((), ()))
NN = (((1,), (0,)), ((), ()))
PLAN = 16
GROUP = 4
STEPS = 28


def offset_table():
    listed = []
    for shift_x in range(-3, 4):
        for shift_y in range(-3, 4):
            for shift_z in range(-3, 4):
                if max(abs(shift_x), abs(shift_y), abs(shift_z)) >= 2:
                    listed.append((shift_x, shift_y, shift_z))
    return np.array(listed, dtype=np.int32)


def exponent_table(degree):
    listed = []
    for accumulated in range(degree + 1):
        for height in (0, 1):
            for power_x in range(accumulated - height + 1):
                listed.append((power_x, accumulated - height - power_x, height))
    return np.array(listed, dtype=np.int32)


ROW_OF = {tuple(int(v) for v in key): row for row, key in enumerate(exponent_table(ORDER))}


def split_rows(data):
    upper = data.astype(BF16)
    lower = (data - upper.astype(F32)).astype(BF16)
    return upper, lower


def apply(data, operator):
    upper, lower = split_rows(data)
    rows = data.shape[0]
    both = jnp.concatenate([upper.astype(F32), lower.astype(F32)], axis=0).astype(BF16)
    found = lax.dot_general(both, operator, NT, preferred_element_type=F32)
    return found[:rows] + found[rows:]


def powers_of(values):
    listed = [jnp.ones_like(values)]
    for exponent in range(ORDER):
        listed.append(listed[-1] * values)
    return listed


def admits(shift, odd):
    return -2 - odd <= shift <= 3 - odd


def leaf_start(shift):
    return {-3: 7, 3: 8}.get(shift, shift + 2)


def plan_table(block_x, block_z):
    shifts = offset_table()
    wide_x, wide_z = block_x + 2 * HALO, block_z + 2 * HALO
    starts = 2 * (wide_x - 1) // 2 + 4
    triples = STEPS * GROUP
    assert 3 * triples >= shifts.shape[0]
    plan = np.zeros((triples * 3, PLAN), np.int32)
    none_leaf = 7 * wide_z * starts
    mid_x, mid_z = block_x // 2 + 4, block_z // 2 + 4
    none_mid = 7 * mid_z * mid_x
    plan[:, :4] = none_leaf
    plan[:, 4:8] = none_mid
    plan[:, 8:11] = 7
    for row, (dx, dy, dz) in enumerate(shifts):
        for z in range(block_z):
            if admits(dz, z % 2):
                plan[row, z] = ((dy + 3) * wide_z + z + 2 + dz) * starts + leaf_start(dx)
        for x in range(2):
            for z in range(2):
                if admits(dz, z) and admits(dx, x):
                    plan[row, 4 + x * 2 + z] = ((dy + 3) * mid_z + z + 2 + dz) * mid_x + x + 2 + dx
        plan[row, 8:11] = (dx + 3, dy + 3, dz + 3)
    return plan.reshape(-1), triples, none_leaf, none_mid, starts


def field_kernel(
    sizes,
    numbers,
    layout,
    plan_ref,
    positions_hbm,
    charges_hbm,
    counts_hbm,
    shift_hbm,
    far_hbm,
    down_hbm,
    lattice_hbm,
    potential_ref,
    field_ref,
    positions,
    charges,
    counts,
    shift_raw,
    far,
    down_raw,
    lattice,
    raw,
    wide,
    targets,
    partial,
    moments_high,
    moments_low,
    mids,
    shift_rows,
    down_rows,
    uppers,
    operators,
    sources,
    leaf_pages,
    mid_high,
    mid_low,
    mid_pages,
    upper_pages,
    top_pages,
    sums,
    local_rows,
    table,
    loads,
    sends,
    receives,
    mid_send,
    mid_receive,
):
    block_x, block_y, block_z = sizes
    triples, none_leaf, none_mid, starts = layout
    wide_x, wide_z = block_x + 2 * HALO, block_z + 2 * HALO
    rows_y = block_y + 2 * HALO
    columns = block_x * block_y
    leaves = columns * block_z
    terms = lattice.shape[0]
    padded_terms = operators.shape[1]
    offsets = offset_table().shape[0]
    at = tuple(lax.axis_index(axis) for axis in ("gx", "gy", "gz"))
    devices = numbers[0] * numbers[1] * numbers[2]
    rank = (at[0] * numbers[1] + at[1]) * numbers[2] + at[2]
    barrier = pltpu.get_barrier_semaphore()

    def coordinates(step):
        other = lax.rem(rank + step, devices)
        return (
            lax.div(other, numbers[1] * numbers[2]),
            lax.rem(lax.div(other, numbers[2]), numbers[1]),
            lax.rem(other, numbers[2]),
        )

    staged = [
        pltpu.make_async_copy(positions_hbm, positions, loads.at[0]),
        pltpu.make_async_copy(charges_hbm, charges, loads.at[1]),
        pltpu.make_async_copy(counts_hbm, counts, loads.at[2]),
        pltpu.make_async_copy(shift_hbm, shift_raw, loads.at[3]),
        pltpu.make_async_copy(far_hbm, far.at[:, pl.ds(0, far_hbm.shape[1])], loads.at[4]),
        pltpu.make_async_copy(down_hbm, down_raw, loads.at[5]),
        pltpu.make_async_copy(lattice_hbm, lattice, loads.at[6]),
    ]
    for copy in staged:
        copy.start()

    def greet(step, carry):
        pl.semaphore_signal(
            barrier, inc=1, device_id=coordinates(step), device_id_type=pl.DeviceIdType.MESH
        )
        return carry

    lax.fori_loop(1, devices, greet, 0)

    lane = lax.broadcasted_iota(jnp.int32, (columns, LANES), 1)
    group = lane // SLOTS
    row8 = lax.broadcasted_iota(jnp.int32, (8, LANES), 0)
    for copy in staged[:3]:
        copy.wait()
    held = jnp.concatenate([counts[x] for x in range(block_x)], axis=0)
    limit = jnp.broadcast_to(held[:, 0:1], (columns, LANES))
    for z in range(1, block_z):
        limit = jnp.where(group == z, jnp.broadcast_to(held[:, z : z + 1], (columns, LANES)), limit)
    live = (lane % SLOTS < limit).astype(F32)
    parts = [
        jnp.concatenate([positions[c, x] for x in range(block_x)], axis=0) for c in range(3)
    ]
    parts.append(jnp.concatenate([charges[x] for x in range(block_x)], axis=0) * live)
    pieces = []
    for z in range(block_z):
        made = None
        for c in range(4):
            turn = (c - z) * SLOTS % LANES
            moved = pltpu.roll(parts[c], turn, 1) if turn else parts[c]
            made = moved if made is None else jnp.where(group == c, moved, made)
        pieces.append(made)
        for x in range(block_x):
            for pair in range(block_y // 2):
                start = x * block_y + 2 * pair
                raw[1 + pair, HALO + z, HALO + x] = made[start : start + 2]
    own = jnp.concatenate(pieces + pieces, axis=0)
    targets[...] = own.T

    pl.semaphore_wait(barrier, devices - 1)
    copies = []
    pairs = block_y // 2

    def span(move, size, halo):
        if move == 1:
            return pl.ds(size, halo), pl.ds(0, halo)
        if move == -1:
            return pl.ds(halo, halo), pl.ds(size + halo, halo)
        return pl.ds(halo, size), pl.ds(halo, size)

    for count in range(27):
        moves = (count // 9 - 1, count // 3 % 3 - 1, count % 3 - 1)
        if moves == (0, 0, 0):
            continue
        target = tuple(
            lax.rem(at[axis] + moves[axis] + numbers[axis], numbers[axis]) for axis in range(3)
        )
        from_x, to_x = span(moves[0], block_x, HALO)
        from_y, to_y = span(moves[1], pairs, 1)
        from_z, to_z = span(moves[2], block_z, HALO)
        copies.append(
            pltpu.make_async_remote_copy(
                src_ref=raw.at[from_y, from_z, from_x],
                dst_ref=raw.at[to_y, to_z, to_x],
                send_sem=sends.at[count],
                recv_sem=receives.at[count],
                device_id=target,
                device_id_type=pl.DeviceIdType.MESH,
            )
        )
    for copy in copies:
        copy.start()

    partial[pl.ds(terms * 8, partial.shape[0] - terms * 8), :] = jnp.zeros(
        (partial.shape[0] - terms * 8, LANES), F32
    )

    def moments(at_x, at_y, at_z, charge):
        quarter = SLOTS // 8
        centred_z = at_z - 0.5
        centred_y = at_y - 0.5
        powers_x = [value * charge for value in powers_of(at_x - 0.5)]
        power_y = None
        for b in range(ORDER + 1):
            power_y = None if b == 0 else (centred_y if b == 1 else power_y * centred_y)
            for a in range(ORDER + 1 - b):
                flat = powers_x[a] if b == 0 else powers_x[a] * power_y
                for height in (0, 1):
                    if a + b + height > ORDER:
                        continue
                    made = flat * centred_z if height else flat
                    total = made[:8]
                    for piece in range(1, quarter):
                        total = total + made[piece * 8 : piece * 8 + 8]
                    row = ROW_OF[(a, b, height)]
                    partial[row * 8 : row * 8 + 8, :] = total
        found = partial[pl.ds(0, padded_terms, stride=8), :]
        for line in range(1, 8):
            found = found + partial[pl.ds(line, padded_terms, stride=8), :]
        found = jnp.concatenate([found, jnp.zeros((LANES - padded_terms, LANES), F32)], axis=0)
        return found.T

    def rows_from(raw_ref, out_ref):
        out_ref[...] = jnp.zeros(out_ref.shape, F32)
        out_ref[:, :terms] = raw_ref[...].astype(F32).reshape(terms * 8, terms)

    def octant_of(ref, octant):
        return ref[pl.ds(octant, terms, stride=8), :].astype(BF16)

    own_moments = moments(
        targets[:SLOTS], targets[SLOTS : 2 * SLOTS], targets[2 * SLOTS : 3 * SLOTS], targets[3 * SLOTS :]
    )[:leaves]
    staged[3].wait()
    rows_from(shift_raw, shift_rows)
    leaf_row = lax.broadcasted_iota(jnp.int32, (leaves, terms), 0)
    leaf_octant = (
        4 * (leaf_row // block_y % 2) + 2 * (leaf_row % 2) + leaf_row // columns % 2
    )
    lifted = jnp.zeros((leaves, terms), F32)
    for octant in range(8):
        found = apply(own_moments, octant_of(shift_rows, octant))
        lifted = jnp.where(leaf_octant == octant, found, lifted)
    lines = []
    for z in range(block_z // 2):
        both = lifted[2 * z * columns : (2 * z + 1) * columns] + lifted[(2 * z + 1) * columns : (2 * z + 2) * columns]
        for x in range(block_x // 2):
            held = both[x * 8 : x * 8 + 8]
            held = held[:4] + held[4:]
            for y in range(block_y // 2):
                lines.append(held[2 * y : 2 * y + 1] + held[2 * y + 1 : 2 * y + 2])
    spare = jnp.zeros((8, LANES - terms), F32)
    own_slot = mids.at[pl.ds(pl.multiple_of(rank * 8, 8), 8)]
    own_slot[...] = jnp.concatenate([jnp.concatenate(lines, axis=0), spare], axis=1)

    def mid_copy(step):
        return pltpu.make_async_remote_copy(
            src_ref=own_slot,
            dst_ref=own_slot,
            send_sem=mid_send.at[step],
            recv_sem=mid_receive.at[step],
            device_id=coordinates(step),
            device_id_type=pl.DeviceIdType.MESH,
        )

    def send_mid(step, carry):
        mid_copy(step).start()
        return carry

    def wait_mid(step, carry):
        mid_copy(step).wait()
        return carry

    lax.fori_loop(1, devices, send_mid, 0)

    staged[4].wait()
    far[:, pl.ds(far_hbm.shape[1], 2 * LANES)] = jnp.zeros((terms, 2 * LANES), BF16)
    tall = lax.broadcasted_iota(jnp.int32, (padded_terms, LANES), 1)

    def place(triple, carry):
        start = triple * (3 * terms)
        turn = lax.rem(start, LANES)
        base = pl.multiple_of(start - turn, LANES)
        back = lax.rem(LANES - turn, LANES)
        turned = []
        for tile in range(3):
            held = far[:, pl.ds(pl.multiple_of(base + tile * LANES, LANES), LANES)].astype(F32)
            held = jnp.concatenate([held, jnp.zeros((padded_terms - terms, LANES), F32)], axis=0)
            turned.append(pltpu.roll(held, back, 1))
        kept = tall < LANES - turn
        for tile in range(2):
            found = jnp.where(kept, turned[tile], turned[tile + 1])
            operators[triple, :, tile * LANES : (tile + 1) * LANES] = found.astype(BF16)
        return carry

    used = operators.shape[0]
    lax.fori_loop(0, used, place, 0, unroll=2)

    strides = (numbers[1] * numbers[2], numbers[2], 1)
    top_sizes = tuple(number // 2 for number in numbers)
    top_strides = (top_sizes[1] * top_sizes[2], top_sizes[2], 1)
    tops = devices // 8
    for axis in range(3):
        odd = lax.rem(at[axis], 2)
        for entry in range(7):
            shift = entry - 3
            size = numbers[axis]
            place_at = lax.rem(at[axis] + shift + 4 * size, size) * strides[axis]
            if shift == -3:
                place_at = jnp.where(odd == 1, place_at, 4 * devices)
            if shift == 3:
                place_at = jnp.where(odd == 0, place_at, 4 * devices)
            table[axis * 8 + entry] = place_at
            size = top_sizes[axis]
            table[24 + axis * 8 + entry] = (
                lax.rem(lax.div(at[axis], 2) + shift + 4 * size, size) * top_strides[axis]
            )
        table[axis * 8 + 7] = jnp.int32(4 * devices)
        table[24 + axis * 8 + 7] = jnp.int32(4 * devices)

    for copy in copies:
        copy.wait()
    guard = 8
    for ref in (wide, moments_high, moments_low):
        ref[:guard, :] = jnp.zeros((guard, LANES), F32)
        ref[ref.shape[0] - guard :, :] = jnp.zeros((guard, LANES), F32)

    def widen(z, carry):
        for x in range(wide_x):
            column = jnp.concatenate([raw[pair, z, x] for pair in range(pairs + 2)], axis=0)
            wide[pl.ds(pl.multiple_of(guard + (z * wide_x + x) * rows_y, 8), rows_y), :] = column
        return carry

    lax.fori_loop(0, wide_z, widen, 0)

    def window(tile, carry):
        start = pl.multiple_of(guard + tile * LANES, 8)
        turned = wide[pl.ds(start, LANES), :].T
        found = moments(
            turned[:SLOTS], turned[SLOTS : 2 * SLOTS], turned[2 * SLOTS : 3 * SLOTS], turned[3 * SLOTS :]
        )
        upper = found.astype(BF16).astype(F32)
        moments_high[pl.ds(start, LANES), :] = upper
        moments_low[pl.ds(start, LANES), :] = (found - upper).astype(BF16).astype(F32)
        return carry

    lax.fori_loop(0, wide_x * wide_z * rows_y // LANES, window, 0)

    near_shifts = [(x, y, z) for x in (-1, 0, 1) for y in (-1, 0, 1) for z in (-1, 0, 1)]
    lane8 = lax.broadcasted_iota(jnp.int32, (8, LANES), 1)
    group8 = lane8 // SLOTS

    def shifted(shift):
        moved = jnp.where(
            group8 == 0,
            float(shift[0]),
            jnp.where(group8 == 1, float(shift[1]), jnp.where(group8 == 2, float(shift[2]), 0.0)),
        )
        found = []
        for z in range(block_z):
            for x in range(0, block_x, 2):
                spot = (z + HALO + shift[2]) * wide_x + x + HALO + shift[0]
                low = guard + spot * rows_y + HALO + shift[1]
                high = low + rows_y - block_y
                held = jnp.where(row8 < block_y, wide[low : low + 8, :], wide[high : high + 8, :])
                found.append(held + moved)
        return found

    for pair in range((len(near_shifts) + 1) // 2):
        first = shifted(near_shifts[2 * pair])
        if 2 * pair + 1 < len(near_shifts):
            second = shifted(near_shifts[2 * pair + 1])
        else:
            second = [jnp.where(group8 < 3, value, 0.0) for value in first]
        sources[pair * LANES : (pair + 1) * LANES, :] = jnp.concatenate(first + second, axis=0).T

    def third(value):
        return (value, pltpu.roll(value, terms, 1), pltpu.roll(value, 2 * terms - LANES, 1))

    odd_line = row8 % 2 == 1

    def fill_pages(z, carry):
        for shift in range(-3, 4):
            turned = []
            for x in range(wide_x):
                start = guard + (z * wide_x + x) * rows_y + HALO + shift
                page = jnp.where(
                    row8 < block_y,
                    moments_high[pl.ds(start, 8), :],
                    moments_low[pl.ds(start - block_y, 8), :],
                )
                if shift == -3:
                    page = jnp.where(odd_line, page, 0.0)
                if shift == 3:
                    page = jnp.where(odd_line, 0.0, page)
                turned.append(third(page))
            spot = ((shift + 3) * wide_z + z) * starts
            zero = jnp.zeros((8, LANES), F32)
            for kind in range(3):
                listed = [(x, turned[x][kind], turned[x + 1][kind]) for x in range(wide_x - 1)]
                listed.append((7, zero, turned[0][kind]))
                listed.append((9, zero, turned[2][kind]))
                listed.append((8, turned[5][kind], zero))
                listed.append((10, turned[7][kind], zero))
                for entry, low, high in listed:
                    leaf_pages[kind, spot + entry] = jnp.concatenate([low, high], axis=0).astype(BF16)
        return carry

    lax.fori_loop(0, wide_z, fill_pages, 0)
    for kind in range(3):
        for entry in range(3):
            leaf_pages[kind, none_leaf + entry] = jnp.zeros((16, LANES), BF16)

    lax.fori_loop(1, devices, wait_mid, 0)
    mid_x, mid_z = block_x // 2 + 4, block_z // 2 + 4
    for ref in (mid_high, mid_low):
        ref[:guard, :] = jnp.zeros((guard, LANES), F32)
        ref[ref.shape[0] - guard :, :] = jnp.zeros((guard, LANES), F32)
    around = []
    for count in range(27):
        moves = (count // 9 - 1, count // 3 % 3 - 1, count % 3 - 1)
        there = [lax.rem(at[axis] + moves[axis] + numbers[axis], numbers[axis]) for axis in range(3)]
        around.append(((there[0] * numbers[1] + there[1]) * numbers[2] + there[2]) * 8)
    for z in range(mid_z):
        for x in range(mid_x):
            line = (z % 2 * 2 + x % 2) * 2
            listed = []
            for y in range(3):
                base = around[(x // 2 * 3 + y) * 3 + z // 2]
                listed.append(mids[pl.ds(base + line, 2), :])
            listed.append(jnp.zeros((2, LANES), F32))
            held = jnp.concatenate(listed, axis=0)
            upper = held.astype(BF16).astype(F32)
            start = guard + (z * mid_x + x) * 8
            mid_high[start : start + 8, :] = upper
            mid_low[start : start + 8, :] = (held - upper).astype(BF16).astype(F32)

    def fill_mids(z, carry):
        for x in range(mid_x):
            for shift in range(-3, 4):
                start = guard + (z * mid_x + x) * 8 + 2 + shift
                page = jnp.where(
                    row8 < 4,
                    jnp.where(row8 < 2, mid_high[pl.ds(start, 8), :], mid_low[pl.ds(start - 2, 8), :]),
                    jnp.where(row8 < 6, mid_high[pl.ds(start - 4, 8), :], mid_low[pl.ds(start - 6, 8), :]),
                )
                if shift == -3:
                    page = jnp.where(odd_line, page, 0.0)
                if shift == 3:
                    page = jnp.where(odd_line, 0.0, page)
                for kind, value in enumerate(third(page)):
                    mid_pages[kind, ((shift + 3) * mid_z + z) * mid_x + x] = value
        return carry

    lax.fori_loop(0, mid_z, fill_mids, 0)
    for kind in range(3):
        mid_pages[kind, none_mid] = jnp.zeros((8, LANES), F32)

    raised = jnp.zeros((devices, terms), F32)
    for octant in range(8):
        line = (octant % 2 * 2 + octant // 4) * 2 + octant // 2 % 2
        raised = raised + apply(mids[pl.ds(line, devices, stride=8), :], octant_of(shift_rows, octant))
    raised = jnp.concatenate([raised, jnp.zeros((devices, LANES - terms), F32)], axis=1)
    uppers[:devices, :] = raised
    rank_row = lax.broadcasted_iota(jnp.int32, (devices, terms), 0)
    rank_octant = (
        4 * (rank_row // strides[0] % 2) + 2 * (rank_row // strides[1] % 2) + rank_row % 2
    )
    lifted = jnp.zeros((devices, terms), F32)
    for octant in range(8):
        found = apply(raised, octant_of(shift_rows, octant))
        lifted = jnp.where(rank_octant == octant, found, lifted)
    root = jnp.sum(lifted, axis=0, keepdims=True)
    top_rows = (tops + 7) // 8 * 8
    picker_row = lax.broadcasted_iota(jnp.int32, (top_rows, devices), 0)
    picker_rank = lax.broadcasted_iota(jnp.int32, (top_rows, devices), 1)
    parent_of = (
        picker_rank // strides[0] // 2 * top_strides[0]
        + picker_rank // strides[1] % numbers[1] // 2 * top_strides[1]
        + picker_rank % numbers[2] // 2
    )
    picker = (picker_row == parent_of).astype(F32)
    merged = lax.dot_general(
        picker, lifted, NN, precision=lax.Precision.HIGHEST, preferred_element_type=F32
    )
    merged = jnp.concatenate([merged, jnp.zeros((top_rows, LANES - terms), F32)], axis=1)
    uppers[devices : devices + top_rows, :] = merged

    def paired(value, line):
        value = jnp.broadcast_to(value, (8, LANES))
        upper = value.astype(BF16).astype(F32)
        lower = (value - upper).astype(BF16).astype(F32)
        page = jnp.where(row8 == line, upper, jnp.where(row8 == line + 1, lower, 0.0))
        return third(page)

    def fill_uppers(entry, carry):
        for kind, value in enumerate(paired(uppers[pl.ds(entry, 1), :], 0)):
            upper_pages[kind, entry] = value
        return carry

    lax.fori_loop(0, devices, fill_uppers, 0, unroll=4)

    def fill_tops(entry, carry):
        for kind, value in enumerate(paired(uppers[pl.ds(devices + entry, 1), :], 2)):
            top_pages[kind, entry] = value
        return carry

    lax.fori_loop(0, tops, fill_tops, 0)
    for kind in range(3):
        upper_pages[kind, devices] = jnp.zeros((8, LANES), F32)
        top_pages[kind, tops] = jnp.zeros((8, LANES), F32)

    lane16 = lax.broadcasted_iota(jnp.int32, (16, LANES), 1)
    first_part = lane16 < terms
    second_part = lane16 < 2 * terms - LANES

    def far_rows(triple):
        plans = [(3 * triple + kind) * PLAN for kind in range(3)]

        def tiles(held):
            return jnp.concatenate(
                [
                    jnp.where(first_part, held[0], held[1]),
                    jnp.where(second_part, held[1], held[2]),
                ],
                axis=1,
            )

        found = []
        for z in range(block_z):
            spots = [plan_ref[start + z] for start in plans]
            for x in range(block_x // 2):
                found.append(tiles([leaf_pages[kind, spots[kind] + 2 * x] for kind in range(3)]))
        held = []
        for kind in range(3):
            page = [mid_pages[kind, plan_ref[plans[kind] + 4 + entry]] for entry in range(4)]
            low = jnp.where(row8 < 4, page[0], page[1])
            high = jnp.where(row8 < 4, page[2], page[3])
            held.append(jnp.concatenate([low, high], axis=0).astype(BF16))
        found.append(tiles(held))
        held = []
        for kind in range(3):
            entries = [plan_ref[plans[kind] + 8 + axis] for axis in range(3)]
            upper = table[entries[0]] + table[8 + entries[1]] + table[16 + entries[2]]
            top = table[24 + entries[0]] + table[32 + entries[1]] + table[40 + entries[2]]
            page = upper_pages[kind, jnp.minimum(upper, devices)] + top_pages[kind, jnp.minimum(top, tops)]
            held.append(jnp.concatenate([page, jnp.zeros((8, LANES), F32)], axis=0).astype(BF16))
        found.append(tiles(held))
        return jnp.concatenate(found, axis=0)

    total_rows = 2 * leaves + 32
    sums[...] = jnp.zeros(sums.shape, F32)
    per_step = sources.shape[0] // LANES * SLOTS // STEPS

    def both_step(step, totals):
        products = []
        for which in range(GROUP):
            triple = step * GROUP + which
            products.append(
                lax.dot_general(
                    far_rows(triple),
                    operators[jnp.minimum(triple, used - 1)],
                    NT,
                    preferred_element_type=F32,
                )
            )
        sums[...] += (products[0] + products[2]) + (products[1] + products[3])
        sum_p, sum_x, sum_y, sum_z = totals
        first = step * per_step
        base = lax.div(first, SLOTS) * LANES + lax.rem(first, SLOTS)
        for line in range(per_step):
            s_x = sources[pl.ds(base + line, 1), :]
            s_y = sources[pl.ds(base + line + SLOTS, 1), :]
            s_z = sources[pl.ds(base + line + 2 * SLOTS, 1), :]
            s_q = sources[pl.ds(base + line + 3 * SLOTS, 1), :]
            d_x = targets[:SLOTS] - s_x
            d_y = targets[SLOTS : 2 * SLOTS] - s_y
            d_z = targets[2 * SLOTS : 3 * SLOTS] - s_z
            inverse = lax.rsqrt(d_x * d_x + d_y * d_y + d_z * d_z + SOFTENING)
            weight = s_q * inverse
            sum_p = sum_p + weight
            cubic = weight * (inverse * inverse)
            sum_x = sum_x + cubic * d_x
            sum_y = sum_y + cubic * d_y
            sum_z = sum_z + cubic * d_z
        return sum_p, sum_x, sum_y, sum_z

    zero = jnp.zeros((SLOTS, LANES), F32)
    near = lax.fori_loop(0, STEPS, both_step, (zero, zero, zero, zero))

    staged[5].wait()
    staged[6].wait()
    rows_from(down_raw, down_rows)
    first = 2 * leaves + 16
    held = sums[first : first + 8, :terms]
    far_upper = held[0:1] + held[1:2]
    far_top = held[2:3] + held[3:4]

    def lattice_apply(value):
        return apply(jnp.broadcast_to(value, (8, terms)), lattice[...])

    def wider(value):
        return jnp.concatenate([value, jnp.zeros((value.shape[0], LANES - terms), F32)], axis=1)

    top_local = 0.125 * (far_top + lattice_apply(root)[:1])
    octant = lax.rem(at[0], 2) * 4 + lax.rem(at[1], 2) * 2 + lax.rem(at[2], 2)
    moved = apply(jnp.broadcast_to(wider(top_local), (8, LANES)), octant_of(down_rows, octant))
    upper_local = jnp.broadcast_to(wider(0.25 * far_upper + moved[:1]), (8, LANES))
    mid_row = lax.broadcasted_iota(jnp.int32, (8, terms), 0)
    mid_octant = 4 * (mid_row // 2 % 2) + 2 * (mid_row % 2) + mid_row // 4
    held = sums[2 * leaves : 2 * leaves + 16, :terms]
    lines = []
    for z in range(2):
        for x in range(2):
            start = x * 8 + z * 4
            lines.append(held[start : start + 2] + held[start + 2 : start + 4])
    far_mid = jnp.concatenate(lines, axis=0)
    downward = [octant_of(down_rows, entry) for entry in range(8)]
    moved = jnp.zeros((8, terms), F32)
    for entry in range(8):
        moved = jnp.where(mid_octant == entry, apply(upper_local, downward[entry]), moved)
    mid_local = wider(0.5 * far_mid + moved)
    expanded = []
    for z in range(block_z):
        for x in range(block_x // 2):
            line = (z // 2 * 2 + x) * 2
            low = jnp.broadcast_to(mid_local[line : line + 1], (8, LANES))
            high = jnp.broadcast_to(mid_local[line + 1 : line + 2], (8, LANES))
            expanded.append(jnp.where(row8 % 4 < 2, low, high))
    expanded = jnp.concatenate(expanded, axis=0)
    moved = jnp.zeros((leaves, terms), F32)
    for entry in range(8):
        moved = jnp.where(leaf_octant == entry, apply(expanded, downward[entry]), moved)
    row_t = lax.broadcasted_iota(jnp.int32, (8, terms), 0)
    lines = []
    for spot in range(leaves // 8):
        low = sums[spot * 16 : spot * 16 + 8, :terms]
        high = sums[spot * 16 + 8 : spot * 16 + 16, :terms]
        low = low + pltpu.roll(low, 4, 0)
        high = high + pltpu.roll(high, 4, 0)
        lines.append(jnp.where(row_t < 4, low, high))
    local = wider(moved + jnp.concatenate(lines, axis=0))
    local_rows[...] = jnp.concatenate([local, local], axis=0).T

    u_x = targets[:SLOTS] - 0.5
    u_y = targets[SLOTS : 2 * SLOTS] - 0.5
    u_z = targets[2 * SLOTS : 3 * SLOTS] - 0.5
    value = grad_x = grad_y = grad_z = None
    for a in range(ORDER, -1, -1):
        inner = inner_y = inner_z = None
        for b in range(ORDER - a, -1, -1):
            here = local_rows[ROW_OF[(a, b, 0)] : ROW_OF[(a, b, 0)] + 1, :]
            if (a, b, 1) in ROW_OF:
                above = local_rows[ROW_OF[(a, b, 1)] : ROW_OF[(a, b, 1)] + 1, :]
                both = here + above * u_z
                inner_z = above if inner_z is None else inner_z * u_y + above
            else:
                both = here
            if inner is None:
                inner = jnp.broadcast_to(both, (SLOTS, LANES))
            else:
                inner_y = inner if inner_y is None else inner_y * u_y + inner
                inner = inner * u_y + both
        if value is None:
            value, grad_y, grad_z = inner, inner_y, inner_z
        else:
            grad_x = value if grad_x is None else grad_x * u_x + value
            value = value * u_x + inner
            if inner_y is not None:
                grad_y = inner_y if grad_y is None else grad_y * u_x + inner_y
            if inner_z is not None:
                grad_z = inner_z if grad_z is None else grad_z * u_x + inner_z

    def halves(total):
        return total + pltpu.roll(total, leaves, 1)

    self_term = targets[3 * SLOTS :] * (SOFTENING**-0.5)
    results = [
        halves(near[0]) - self_term + value,
        halves(near[1]) - grad_x,
        halves(near[2]) - grad_y,
        halves(near[3]) - grad_z,
    ]
    turned = jnp.concatenate(results, axis=0).T
    for entry in range(4):
        made = None
        for z in range(block_z):
            turn = (z - entry) * SLOTS % LANES
            held = turned[z * columns : (z + 1) * columns]
            held = pltpu.roll(held, turn, 1) if turn else held
            made = held if made is None else jnp.where(group == z, held, made)
        made = made * live
        for x in range(block_x):
            piece = made[x * block_y : (x + 1) * block_y]
            if entry == 0:
                potential_ref[x] = piece
            else:
                field_ref[entry - 1, x] = piece


def per_device(
    positions, charges, counts, moment_shift, far_operators, local_shift, lattice_operator
):
    block_x, block_y, column = charges.shape
    block_z = column // SLOTS
    sizes = (block_x, block_y, block_z)
    numbers = tuple(lax.axis_size(axis) for axis in ("gx", "gy", "gz"))
    devices = numbers[0] * numbers[1] * numbers[2]
    terms = moment_shift.shape[1]
    padded_terms = (terms + 15) // 16 * 16
    leaves = block_x * block_y * block_z
    plan, triples, none_leaf, none_mid, starts = plan_table(block_x, block_z)
    offsets = offset_table().shape[0]
    wide_x, wide_z = block_x + 2 * HALO, block_z + 2 * HALO
    wide_leaves = wide_x * wide_z * (block_y + 2 * HALO)
    mid_columns = (block_x // 2 + 4) * (block_z // 2 + 4)
    tops = devices // 8
    smem = pl.BlockSpec(memory_space=pltpu.SMEM)
    anywhere = pl.BlockSpec(memory_space=pl.ANY)
    vmem = pl.BlockSpec(memory_space=pltpu.VMEM)
    layout = (triples, none_leaf, none_mid, starts)
    potential, field_out = pl.pallas_call(
        lambda *refs: field_kernel(sizes, numbers, layout, *refs),
        out_shape=(
            jax.ShapeDtypeStruct((block_x, block_y, column), F32),
            jax.ShapeDtypeStruct((3, block_x, block_y, column), F32),
        ),
        in_specs=[smem] + [anywhere] * 7,
        out_specs=(vmem, vmem),
        scratch_shapes=[
            pltpu.VMEM(positions.shape, F32),
            pltpu.VMEM(charges.shape, F32),
            pltpu.VMEM(counts.shape, jnp.int32),
            pltpu.VMEM((terms, 8, terms), BF16),
            pltpu.VMEM((terms, far_operators.shape[1] + 2 * LANES), BF16),
            pltpu.VMEM((terms, 8, terms), BF16),
            pltpu.VMEM((terms, terms), BF16),
            pltpu.VMEM((block_y // 2 + 2, wide_z, wide_x, 2, LANES), F32),
            pltpu.VMEM((wide_leaves + 16, LANES), F32),
            pltpu.VMEM((4 * SLOTS, LANES), F32),
            pltpu.VMEM((padded_terms * 8, LANES), F32),
            pltpu.VMEM((wide_leaves + 16, LANES), F32),
            pltpu.VMEM((wide_leaves + 16, LANES), F32),
            pltpu.VMEM((devices * 8, LANES), F32),
            pltpu.VMEM((terms * 8, LANES), F32),
            pltpu.VMEM((terms * 8, LANES), F32),
            pltpu.VMEM((devices + (tops + 7) // 8 * 8, LANES), F32),
            pltpu.VMEM((-(-offsets // 3), padded_terms, 2 * LANES), BF16),
            pltpu.VMEM((14 * LANES, LANES), F32),
            pltpu.VMEM((3, none_leaf + 3, 16, LANES), BF16),
            pltpu.VMEM((mid_columns * 8 + 16, LANES), F32),
            pltpu.VMEM((mid_columns * 8 + 16, LANES), F32),
            pltpu.VMEM((3, none_mid + 1, 8, LANES), F32),
            pltpu.VMEM((3, devices + 1, 8, LANES), F32),
            pltpu.VMEM((3, tops + 1, 8, LANES), F32),
            pltpu.VMEM((2 * leaves + 32, padded_terms), F32),
            pltpu.VMEM((LANES, LANES), F32),
            pltpu.SMEM((48,), jnp.int32),
            pltpu.SemaphoreType.DMA((7,)),
            pltpu.SemaphoreType.DMA((27,)),
            pltpu.SemaphoreType.DMA((27,)),
            pltpu.SemaphoreType.DMA((devices,)),
            pltpu.SemaphoreType.DMA((devices,)),
        ],
        compiler_params=pltpu.CompilerParams(
            vmem_limit_bytes=60 * 1024 * 1024, collective_id=0, has_side_effects=True
        ),
        name="fields",
    )(
        jnp.asarray(plan),
        positions,
        charges,
        counts,
        jnp.transpose(moment_shift, (1, 0, 2)),
        far_operators,
        jnp.transpose(local_shift, (1, 0, 2)),
        lattice_operator,
    )
    return potential, field_out


def solution(mesh):
    placed = (
        P(None, "gx", "gy", "gz"),
        P("gx", "gy", "gz"),
        P("gx", "gy", "gz"),
        P(),
        P(),
        P(),
        P(),
    )
    return jax.shard_map(
        per_device,
        mesh=mesh,
        in_specs=placed,
        out_specs=(P("gx", "gy", "gz"), P(None, "gx", "gy", "gz")),
        check_vma=False,
    )
```

```python
import jax
import jax.numpy as jnp
import numpy as np
from jax import lax
from jax.experimental import pallas as pl
from jax.experimental.pallas import tpu as pltpu
from jax.sharding import PartitionSpec as P

ORDER = 8
SLOTS = 32
SOFTENING = 0.0625
LANES = 128
HALO = 2
F32 = jnp.float32
BF16 = jnp.bfloat16
NT = (((1,), (1,)), ((), ()))
NN = (((1,), (0,)), ((), ()))
PLAN = 4
GROUP = 4
STEPS = 28
PLACED = 9


def offset_table():
    listed = []
    for shift_x in range(-3, 4):
        for shift_y in range(-3, 4):
            for shift_z in range(-3, 4):
                if max(abs(shift_x), abs(shift_y), abs(shift_z)) >= 2:
                    listed.append((shift_x, shift_y, shift_z))
    return np.array(listed, dtype=np.int32)


def exponent_table(degree):
    listed = []
    for accumulated in range(degree + 1):
        for height in (0, 1):
            for power_x in range(accumulated - height + 1):
                listed.append((power_x, accumulated - height - power_x, height))
    return np.array(listed, dtype=np.int32)


ROW_OF = {tuple(int(v) for v in key): row for row, key in enumerate(exponent_table(ORDER))}


def split_rows(data):
    upper = data.astype(BF16)
    lower = (data - upper.astype(F32)).astype(BF16)
    return upper, lower


def apply(data, operator):
    upper, lower = split_rows(data)
    rows = data.shape[0]
    both = jnp.concatenate([upper.astype(F32), lower.astype(F32)], axis=0).astype(BF16)
    found = lax.dot_general(both, operator, NT, preferred_element_type=F32)
    return found[:rows] + found[rows:]


def powers_of(values):
    listed = [jnp.ones_like(values)]
    for exponent in range(ORDER):
        listed.append(listed[-1] * values)
    return listed


def admits(shift, odd):
    return -2 - odd <= shift <= 3 - odd


def leaf_start(shift):
    return {-3: 7, 3: 8}.get(shift, shift + 2)


def plan_table(block_x, block_z):
    shifts = offset_table()
    wide_x, wide_z = block_x + 2 * HALO, block_z + 2 * HALO
    starts = wide_x + 3
    triples = STEPS * GROUP
    assert 3 * triples >= shifts.shape[0]
    plan = np.zeros((triples * 3, PLAN), np.int32)
    none = 7 * wide_z * starts
    plan[:, :2] = none
    plan[:, 2] = 49
    plan[:, 3] = 7
    for row, (dx, dy, dz) in enumerate(shifts):
        for z in range(2):
            if admits(dz, z):
                plan[row, z] = ((dy + 3) * wide_z + z + 2 + dz) * starts + leaf_start(dx)
        plan[row, 2] = (dx + 3) * 7 + dy + 3
        plan[row, 3] = dz + 3
    return plan.reshape(-1), triples, none, starts


def field_kernel(
    sizes,
    numbers,
    layout,
    plan_hbm,
    positions_hbm,
    charges_hbm,
    counts_hbm,
    shift_hbm,
    far_hbm,
    down_hbm,
    lattice_hbm,
    potential_ref,
    field_ref,
    positions,
    charges,
    counts,
    shift_raw,
    far,
    down_raw,
    lattice,
    raw,
    wide,
    targets,
    partial,
    moments_high,
    moments_low,
    mids,
    shift_rows,
    down_rows,
    uppers,
    operators,
    sources,
    pages,
    mid_high,
    mid_low,
    upper_pages,
    sums,
    local_rows,
    plan_ref,
    table,
    reach,
    loads,
    sends,
    receives,
    mid_send,
    mid_receive,
):
    block_x, block_y, block_z = sizes
    triples, none, starts = layout
    wide_x, wide_z = block_x + 2 * HALO, block_z + 2 * HALO
    rows_y = block_y + 2 * HALO
    columns = block_x * block_y
    leaves = columns * block_z
    terms = lattice.shape[0]
    padded_terms = operators.shape[1]
    offsets = offset_table().shape[0]
    at = tuple(lax.axis_index(axis) for axis in ("gx", "gy", "gz"))
    devices = numbers[0] * numbers[1] * numbers[2]
    rank = (at[0] * numbers[1] + at[1]) * numbers[2] + at[2]
    barrier = pltpu.get_barrier_semaphore()

    def other(step):
        return lax.rem(rank + step, devices)

    staged = [
        pltpu.make_async_copy(positions_hbm, positions, loads.at[0]),
        pltpu.make_async_copy(charges_hbm, charges, loads.at[1]),
        pltpu.make_async_copy(counts_hbm, counts, loads.at[2]),
        pltpu.make_async_copy(shift_hbm, shift_raw, loads.at[3]),
        pltpu.make_async_copy(far_hbm, far.at[:, pl.ds(0, far_hbm.shape[1])], loads.at[4]),
        pltpu.make_async_copy(down_hbm, down_raw, loads.at[5]),
        pltpu.make_async_copy(lattice_hbm, lattice, loads.at[6]),
        pltpu.make_async_copy(plan_hbm, plan_ref, loads.at[7]),
    ]
    for copy in staged:
        copy.start()

    def greet(step, carry):
        pl.semaphore_signal(
            barrier, inc=1, device_id=other(step), device_id_type=pl.DeviceIdType.LOGICAL
        )
        return carry

    lax.fori_loop(1, devices, greet, 0)

    lane = lax.broadcasted_iota(jnp.int32, (columns, LANES), 1)
    group = lane // SLOTS
    row8 = lax.broadcasted_iota(jnp.int32, (8, LANES), 0)
    for copy in staged[:3]:
        copy.wait()
    held = jnp.concatenate([counts[x] for x in range(block_x)], axis=0)
    limit = jnp.broadcast_to(held[:, 0:1], (columns, LANES))
    for z in range(1, block_z):
        limit = jnp.where(group == z, jnp.broadcast_to(held[:, z : z + 1], (columns, LANES)), limit)
    live = (lane % SLOTS < limit).astype(F32)
    parts = [
        jnp.concatenate([positions[c, x] for x in range(block_x)], axis=0) for c in range(3)
    ]
    parts.append(jnp.concatenate([charges[x] for x in range(block_x)], axis=0) * live)
    pieces = []
    for z in range(block_z):
        made = None
        for c in range(4):
            turn = (c - z) * SLOTS % LANES
            moved = pltpu.roll(parts[c], turn, 1) if turn else parts[c]
            made = moved if made is None else jnp.where(group == c, moved, made)
        pieces.append(made)
        for x in range(block_x):
            for pair in range(block_y // 2):
                start = x * block_y + 2 * pair
                raw[1 + pair, HALO + z, HALO + x] = made[start : start + 2]
    own = jnp.concatenate(pieces + pieces, axis=0)
    targets[...] = own.T

    pl.semaphore_wait(barrier, devices - 1)
    copies = []
    pairs = block_y // 2

    def span(move, size, halo):
        if move == 1:
            return pl.ds(size, halo), pl.ds(0, halo)
        if move == -1:
            return pl.ds(halo, halo), pl.ds(size + halo, halo)
        return pl.ds(halo, size), pl.ds(halo, size)

    for count in range(27):
        moves = (count // 9 - 1, count // 3 % 3 - 1, count % 3 - 1)
        if moves == (0, 0, 0):
            continue
        target = tuple(
            lax.rem(at[axis] + moves[axis] + numbers[axis], numbers[axis]) for axis in range(3)
        )
        from_x, to_x = span(moves[0], block_x, HALO)
        from_y, to_y = span(moves[1], pairs, 1)
        from_z, to_z = span(moves[2], block_z, HALO)
        copies.append(
            pltpu.make_async_remote_copy(
                src_ref=raw.at[from_y, from_z, from_x],
                dst_ref=raw.at[to_y, to_z, to_x],
                send_sem=sends.at[count],
                recv_sem=receives.at[count],
                device_id=target,
                device_id_type=pl.DeviceIdType.MESH,
            )
        )
    for copy in copies:
        copy.start()

    partial[pl.ds(terms * 8, partial.shape[0] - terms * 8), :] = jnp.zeros(
        (partial.shape[0] - terms * 8, LANES), F32
    )

    def moments(at_x, at_y, at_z, charge):
        quarter = SLOTS // 8
        centred_z = at_z - 0.5
        centred_y = at_y - 0.5
        powers_x = [value * charge for value in powers_of(at_x - 0.5)]
        power_y = None
        for b in range(ORDER + 1):
            power_y = None if b == 0 else (centred_y if b == 1 else power_y * centred_y)
            for a in range(ORDER + 1 - b):
                flat = powers_x[a] if b == 0 else powers_x[a] * power_y
                for height in (0, 1):
                    if a + b + height > ORDER:
                        continue
                    made = flat * centred_z if height else flat
                    total = made[:8]
                    for piece in range(1, quarter):
                        total = total + made[piece * 8 : piece * 8 + 8]
                    row = ROW_OF[(a, b, height)]
                    partial[row * 8 : row * 8 + 8, :] = total
        found = partial[pl.ds(0, padded_terms, stride=8), :]
        for line in range(1, 8):
            found = found + partial[pl.ds(line, padded_terms, stride=8), :]
        found = jnp.concatenate([found, jnp.zeros((LANES - padded_terms, LANES), F32)], axis=0)
        return found.T

    def rows_from(raw_ref, out_ref):
        out_ref[...] = jnp.zeros(out_ref.shape, F32)
        out_ref[:, :terms] = raw_ref[...].astype(F32).reshape(terms * 8, terms)

    def octant_of(ref, octant):
        return ref[pl.ds(octant, terms, stride=8), :].astype(BF16)

    own_moments = moments(
        targets[:SLOTS], targets[SLOTS : 2 * SLOTS], targets[2 * SLOTS : 3 * SLOTS], targets[3 * SLOTS :]
    )[:leaves]
    staged[3].wait()
    rows_from(shift_raw, shift_rows)
    leaf_row = lax.broadcasted_iota(jnp.int32, (leaves, terms), 0)
    leaf_octant = (
        4 * (leaf_row // block_y % 2) + 2 * (leaf_row % 2) + leaf_row // columns % 2
    )
    lifted = jnp.zeros((leaves, terms), F32)
    for octant in range(8):
        found = apply(own_moments, octant_of(shift_rows, octant))
        lifted = jnp.where(leaf_octant == octant, found, lifted)
    lines = []
    for z in range(block_z // 2):
        both = lifted[2 * z * columns : (2 * z + 1) * columns] + lifted[(2 * z + 1) * columns : (2 * z + 2) * columns]
        for x in range(block_x // 2):
            held = both[x * 8 : x * 8 + 8]
            held = held[:4] + held[4:]
            for y in range(block_y // 2):
                lines.append(held[2 * y : 2 * y + 1] + held[2 * y + 1 : 2 * y + 2])
    spare = jnp.zeros((8, LANES - terms), F32)
    own_slot = mids.at[pl.ds(pl.multiple_of(rank * 8, 8), 8)]
    own_slot[...] = jnp.concatenate([jnp.concatenate(lines, axis=0), spare], axis=1)

    def mid_copy(step):
        return pltpu.make_async_remote_copy(
            src_ref=own_slot,
            dst_ref=own_slot,
            send_sem=mid_send.at[step],
            recv_sem=mid_receive.at[step],
            device_id=other(step),
            device_id_type=pl.DeviceIdType.LOGICAL,
        )

    def send_mid(step, carry):
        mid_copy(step).start()
        return carry

    def wait_mid(step, carry):
        mid_copy(step).wait()
        return carry

    lax.fori_loop(1, devices, send_mid, 0)

    strides = (numbers[1] * numbers[2], numbers[2], 1)
    top_sizes = tuple(number // 2 for number in numbers)
    top_strides = (top_sizes[1] * top_sizes[2], top_sizes[2], 1)
    tops = devices // 8
    spots, top_spots = [], []
    for axis in range(3):
        odd = lax.rem(at[axis], 2)
        listed, top_listed = [], []
        for entry in range(7):
            shift = entry - 3
            size = numbers[axis]
            spot = lax.rem(at[axis] + shift + 4 * size, size) * strides[axis]
            if shift == -3:
                spot = jnp.where(odd == 1, spot, 4 * devices)
            if shift == 3:
                spot = jnp.where(odd == 0, spot, 4 * devices)
            listed.append(spot)
            size = top_sizes[axis]
            top_listed.append(
                lax.rem(lax.div(at[axis], 2) + shift + 4 * size, size) * top_strides[axis]
            )
        spots.append(listed)
        top_spots.append(top_listed)
    for x in range(7):
        for y in range(7):
            table[0, x * 7 + y] = spots[0][x] + spots[1][y]
            table[1, x * 7 + y] = top_spots[0][x] + top_spots[1][y]
    for z in range(7):
        table[2, z] = spots[2][z]
        table[3, z] = top_spots[2][z]
    for line, entry in ((0, 49), (1, 49), (2, 7), (3, 7)):
        table[line, entry] = jnp.int32(4 * devices)
    staged[7].wait()

    def reach_of(row):
        level, depth = plan_ref[row * PLAN + 2], plan_ref[row * PLAN + 3]
        reach[2 * row] = jnp.minimum(table[0, level] + table[2, depth], devices)
        reach[2 * row + 1] = jnp.minimum(table[1, level] + table[3, depth], tops) + devices + 1

    staged[4].wait()
    spare_width = far.shape[1] - far_hbm.shape[1]
    far[:, pl.ds(far_hbm.shape[1], spare_width)] = jnp.zeros((terms, spare_width), BF16)
    tall = lax.broadcasted_iota(jnp.int32, (padded_terms, LANES), 1)
    spare_rows = jnp.zeros((padded_terms - terms, LANES), BF16)

    def place(batch, carry):
        for local in range(2 * PLACED):
            triple = batch * (2 * PLACED) + local
            start = triple * (3 * terms)
            turn = lax.rem(start, LANES)
            base = pl.multiple_of(start - turn, LANES)
            back = lax.rem(LANES - turn, LANES)
            turned = []
            for tile in range(3):
                held = far[:, pl.ds(pl.multiple_of(base + tile * LANES, LANES), LANES)]
                turned.append(pltpu.roll(jnp.concatenate([held, spare_rows], axis=0), back, 1))
            kept = tall < LANES - turn
            for tile in range(2):
                found = jnp.where(kept, turned[tile], turned[tile + 1])
                spot = (local % 2) * 2 + tile
                operators[
                    batch * PLACED + local // 2, :, spot * LANES : (spot + 1) * LANES
                ] = found
            for kind in range(3):
                reach_of(3 * triple + kind)
        return carry

    used = operators.shape[0]
    lax.fori_loop(0, used // PLACED, place, 0)
    for row in range(used * 6, triples * 3):
        reach_of(row)

    for copy in copies:
        copy.wait()
    guard = 8

    def clear(ref):
        ref[:guard, :] = jnp.zeros((guard, LANES), F32)
        ref[ref.shape[0] - guard :, :] = jnp.zeros((guard, LANES), F32)

    clear(wide)
    for kind in range(3):
        for ref in (moments_high, moments_low, mid_high, mid_low):
            clear(ref.at[kind])

    def third(value):
        return (value, pltpu.roll(value, terms, 1), pltpu.roll(value, 2 * terms - LANES, 1))

    def halved(value):
        upper = value.astype(BF16).astype(F32)
        return upper, (value - upper).astype(BF16).astype(F32)

    def widen(z, carry):
        for x in range(wide_x):
            column = jnp.concatenate([raw[pair, z, x] for pair in range(pairs + 2)], axis=0)
            wide[pl.ds(pl.multiple_of(guard + (z * wide_x + x) * rows_y, 8), rows_y), :] = column
        return carry

    lax.fori_loop(0, wide_z, widen, 0)

    def window(tile, carry):
        start = pl.multiple_of(guard + tile * LANES, 8)
        turned = wide[pl.ds(start, LANES), :].T
        found = moments(
            turned[:SLOTS], turned[SLOTS : 2 * SLOTS], turned[2 * SLOTS : 3 * SLOTS], turned[3 * SLOTS :]
        )
        for kind, value in enumerate(third(found)):
            upper, lower = halved(value)
            moments_high[kind, pl.ds(start, LANES), :] = upper
            moments_low[kind, pl.ds(start, LANES), :] = lower
        return carry

    lax.fori_loop(0, wide_x * wide_z * rows_y // LANES, window, 0)

    near_shifts = [(x, y, z) for x in (-1, 0, 1) for y in (-1, 0, 1) for z in (-1, 0, 1)]
    lane8 = lax.broadcasted_iota(jnp.int32, (8, LANES), 1)
    group8 = lane8 // SLOTS

    def shifted(shift):
        moved = jnp.where(
            group8 == 0,
            float(shift[0]),
            jnp.where(group8 == 1, float(shift[1]), jnp.where(group8 == 2, float(shift[2]), 0.0)),
        )
        found = []
        for z in range(block_z):
            for x in range(0, block_x, 2):
                spot = (z + HALO + shift[2]) * wide_x + x + HALO + shift[0]
                low = guard + spot * rows_y + HALO + shift[1]
                high = low + rows_y - block_y
                held = jnp.where(row8 < block_y, wide[low : low + 8, :], wide[high : high + 8, :])
                found.append(held + moved)
        return found

    for pair in range((len(near_shifts) + 1) // 2):
        first = shifted(near_shifts[2 * pair])
        if 2 * pair + 1 < len(near_shifts):
            second = shifted(near_shifts[2 * pair + 1])
        else:
            second = [jnp.where(group8 < 3, value, 0.0) for value in first]
        sources[pair * LANES : (pair + 1) * LANES, :] = jnp.concatenate(first + second, axis=0).T

    odd_line = row8 % 2 == 1
    zero8 = jnp.zeros((8, LANES), F32)

    def parity(page, shift):
        if shift == -3:
            return jnp.where(odd_line, page, 0.0)
        if shift == 3:
            return jnp.where(odd_line, 0.0, page)
        return page

    def fill_pages(z, carry):
        for shift in range(-3, 4):
            spot = ((shift + 3) * wide_z + z) * starts
            for kind in range(3):
                made = []
                for x in range(wide_x):
                    start = guard + (z * wide_x + x) * rows_y + HALO + shift
                    page = jnp.where(
                        row8 < block_y,
                        moments_high[kind, pl.ds(start, 8), :],
                        moments_low[kind, pl.ds(start - block_y, 8), :],
                    )
                    made.append(parity(page, shift))
                listed = [(x, made[x], made[x + 1]) for x in range(wide_x - 1)]
                listed += [(7, zero8, made[0]), (9, zero8, made[2])]
                listed += [(8, made[5], zero8), (10, made[7], zero8)]
                for entry, low, high in listed:
                    pages[kind, spot + entry] = jnp.concatenate([low, high], axis=0).astype(BF16)
        return carry

    lax.fori_loop(0, wide_z, fill_pages, 0)
    for kind in range(6):
        for entry in range(pages.shape[1] - none):
            pages[kind, none + entry] = jnp.zeros((16, LANES), BF16)

    lax.fori_loop(1, devices, wait_mid, 0)
    mid_x, mid_z = block_x // 2 + 4, block_z // 2 + 4
    around = []
    for count in range(27):
        moves = (count // 9 - 1, count // 3 % 3 - 1, count % 3 - 1)
        there = [lax.rem(at[axis] + moves[axis] + numbers[axis], numbers[axis]) for axis in range(3)]
        around.append(((there[0] * numbers[1] + there[1]) * numbers[2] + there[2]) * 8)
    for z in range(mid_z):
        for x in range(mid_x):
            line = (z % 2 * 2 + x % 2) * 2
            listed = []
            for y in range(3):
                base = around[(x // 2 * 3 + y) * 3 + z // 2]
                listed.append(mids[pl.ds(base + line, 2), :])
            listed.append(jnp.zeros((2, LANES), F32))
            held = jnp.concatenate(listed, axis=0)
            start = guard + (z * mid_x + x) * 8
            for kind, value in enumerate(third(held)):
                upper, lower = halved(value)
                mid_high[kind, start : start + 8, :] = upper
                mid_low[kind, start : start + 8, :] = lower

    def fill_mids(z, carry):
        for shift in range(-3, 4):
            spot = ((shift + 3) * wide_z + z) * starts
            for kind in range(3):
                made = []
                for x in range(mid_x):
                    start = guard + (z * mid_x + x) * 8 + 2 + shift
                    page = jnp.where(
                        row8 < 2,
                        mid_high[kind, pl.ds(start, 8), :],
                        mid_low[kind, pl.ds(start - 2, 8), :],
                    )
                    made.append(parity(page, shift))
                moved = [pltpu.roll(page, 4, 0) for page in made]
                listed = [(x, made[x], moved[x + 1]) for x in range(mid_x - 1)]
                listed += [(7, zero8, moved[0]), (8, made[5], zero8)]
                for entry, low, high in listed:
                    page = jnp.where(row8 < 4, low, high)
                    pages[3 + kind, spot + entry] = jnp.concatenate([page, page], axis=0).astype(BF16)
        return carry

    lax.fori_loop(0, mid_z, fill_mids, 0)

    raised = jnp.zeros((devices, terms), F32)
    for octant in range(8):
        line = (octant % 2 * 2 + octant // 4) * 2 + octant // 2 % 2
        raised = raised + apply(mids[pl.ds(line, devices, stride=8), :], octant_of(shift_rows, octant))
    raised = jnp.concatenate([raised, jnp.zeros((devices, LANES - terms), F32)], axis=1)
    rank_row = lax.broadcasted_iota(jnp.int32, (devices, terms), 0)
    rank_octant = (
        4 * (rank_row // strides[0] % 2) + 2 * (rank_row // strides[1] % 2) + rank_row % 2
    )
    lifted = jnp.zeros((devices, terms), F32)
    for octant in range(8):
        found = apply(raised, octant_of(shift_rows, octant))
        lifted = jnp.where(rank_octant == octant, found, lifted)
    root = jnp.sum(lifted, axis=0, keepdims=True)
    top_rows = (tops + 7) // 8 * 8
    picker_row = lax.broadcasted_iota(jnp.int32, (top_rows, devices), 0)
    picker_rank = lax.broadcasted_iota(jnp.int32, (top_rows, devices), 1)
    parent_of = (
        picker_rank // strides[0] // 2 * top_strides[0]
        + picker_rank // strides[1] % numbers[1] // 2 * top_strides[1]
        + picker_rank % numbers[2] // 2
    )
    picker = (picker_row == parent_of).astype(F32)
    merged = lax.dot_general(
        picker, lifted, NN, precision=lax.Precision.HIGHEST, preferred_element_type=F32
    )
    merged = jnp.concatenate([merged, jnp.zeros((top_rows, LANES - terms), F32)], axis=1)
    for kind, value in enumerate(third(jnp.concatenate([raised, merged], axis=0))):
        upper, lower = halved(value)
        uppers[2 * kind] = upper
        uppers[2 * kind + 1] = lower

    def fill_uppers(line):
        def fill(entry, carry):
            for kind in range(3):
                high = jnp.broadcast_to(uppers[2 * kind, pl.ds(line[1] + entry, 1), :], (8, LANES))
                low = jnp.broadcast_to(uppers[2 * kind + 1, pl.ds(line[1] + entry, 1), :], (8, LANES))
                page = jnp.where(row8 == line[0], high, jnp.where(row8 == line[0] + 1, low, 0.0))
                upper_pages[kind, line[2] + entry] = jnp.concatenate([page, zero8], axis=0).astype(BF16)
            return carry

        return fill

    lax.fori_loop(0, devices, fill_uppers((0, 0, 0)), 0, unroll=8)
    lax.fori_loop(0, tops, fill_uppers((2, devices, devices + 1)), 0, unroll=4)
    for kind in range(3):
        upper_pages[kind, devices] = jnp.zeros((16, LANES), BF16)
        upper_pages[kind, devices + 1 + tops] = jnp.zeros((16, LANES), BF16)

    lane16 = lax.broadcasted_iota(jnp.int32, (16, LANES), 1)
    first_part = lane16 < terms
    second_part = lane16 < 2 * terms - LANES

    first_eight = lax.broadcasted_iota(jnp.int32, (16, LANES), 0) < 8

    def far_rows(triple):
        rows = [3 * triple + kind for kind in range(3)]
        spots = [[plan_ref[row * PLAN + odd] for odd in range(2)] for row in rows]

        def tiles(held):
            return jnp.concatenate(
                [
                    jnp.where(first_part, held[0], held[1]),
                    jnp.where(second_part, held[1], held[2]),
                ],
                axis=1,
            )

        found = []
        for z in range(block_z):
            for x in range(block_x // 2):
                step = z // 2 * 2 * starts + 2 * x
                found.append(tiles([pages[kind, spots[kind][z % 2] + step] for kind in range(3)]))
        held = []
        for kind in range(3):
            even, odd = pages[3 + kind, spots[kind][0]], pages[3 + kind, spots[kind][1]]
            held.append(jnp.where(first_eight, even, odd))
        found.append(tiles(held))
        held = []
        for kind, row in enumerate(rows):
            held.append(upper_pages[kind, reach[2 * row]] + upper_pages[kind, reach[2 * row + 1]])
        found.append(tiles(held))
        return jnp.concatenate(found, axis=0)

    total_rows = 2 * leaves + 32
    sums[...] = jnp.zeros(sums.shape, F32)
    per_step = sources.shape[0] // LANES * SLOTS // STEPS

    def both_step(step, totals):
        products = []
        for which in range(GROUP // 2):
            pair = step * (GROUP // 2) + which
            left = jnp.concatenate([far_rows(2 * pair), far_rows(2 * pair + 1)], axis=1)
            products.append(
                lax.dot_general(
                    left,
                    operators[jnp.minimum(pair, used - 1)],
                    NT,
                    preferred_element_type=F32,
                )
            )
        sums[...] += products[0] + products[1]
        sum_p, sum_x, sum_y, sum_z = totals
        first = step * per_step
        base = lax.div(first, SLOTS) * LANES + lax.rem(first, SLOTS)
        for line in range(per_step):
            s_x = sources[pl.ds(base + line, 1), :]
            s_y = sources[pl.ds(base + line + SLOTS, 1), :]
            s_z = sources[pl.ds(base + line + 2 * SLOTS, 1), :]
            s_q = sources[pl.ds(base + line + 3 * SLOTS, 1), :]
            d_x = targets[:SLOTS] - s_x
            d_y = targets[SLOTS : 2 * SLOTS] - s_y
            d_z = targets[2 * SLOTS : 3 * SLOTS] - s_z
            inverse = lax.rsqrt(d_x * d_x + d_y * d_y + d_z * d_z + SOFTENING)
            weight = s_q * inverse
            sum_p = sum_p + weight
            cubic = weight * (inverse * inverse)
            sum_x = sum_x + cubic * d_x
            sum_y = sum_y + cubic * d_y
            sum_z = sum_z + cubic * d_z
        return sum_p, sum_x, sum_y, sum_z

    zero = jnp.zeros((SLOTS, LANES), F32)
    near = lax.fori_loop(0, STEPS, both_step, (zero, zero, zero, zero))

    staged[5].wait()
    staged[6].wait()
    rows_from(down_raw, down_rows)
    first = 2 * leaves + 16
    held = sums[first : first + 8, :terms]
    far_upper = held[0:1] + held[1:2]
    far_top = held[2:3] + held[3:4]

    def lattice_apply(value):
        return apply(jnp.broadcast_to(value, (8, terms)), lattice[...])

    def wider(value):
        return jnp.concatenate([value, jnp.zeros((value.shape[0], LANES - terms), F32)], axis=1)

    top_local = 0.125 * (far_top + lattice_apply(root)[:1])
    octant = lax.rem(at[0], 2) * 4 + lax.rem(at[1], 2) * 2 + lax.rem(at[2], 2)
    moved = apply(jnp.broadcast_to(wider(top_local), (8, LANES)), octant_of(down_rows, octant))
    upper_local = jnp.broadcast_to(wider(0.25 * far_upper + moved[:1]), (8, LANES))
    mid_row = lax.broadcasted_iota(jnp.int32, (8, terms), 0)
    mid_octant = 4 * (mid_row // 2 % 2) + 2 * (mid_row % 2) + mid_row // 4
    held = sums[2 * leaves : 2 * leaves + 16, :terms]
    lines = []
    for z in range(2):
        for x in range(2):
            start = z * 8 + x * 4
            lines.append(held[start : start + 2] + held[start + 2 : start + 4])
    far_mid = jnp.concatenate(lines, axis=0)
    downward = [octant_of(down_rows, entry) for entry in range(8)]
    moved = jnp.zeros((8, terms), F32)
    for entry in range(8):
        moved = jnp.where(mid_octant == entry, apply(upper_local, downward[entry]), moved)
    mid_local = wider(0.5 * far_mid + moved)
    expanded = []
    for z in range(block_z):
        for x in range(block_x // 2):
            line = (z // 2 * 2 + x) * 2
            low = jnp.broadcast_to(mid_local[line : line + 1], (8, LANES))
            high = jnp.broadcast_to(mid_local[line + 1 : line + 2], (8, LANES))
            expanded.append(jnp.where(row8 % 4 < 2, low, high))
    expanded = jnp.concatenate(expanded, axis=0)
    moved = jnp.zeros((leaves, terms), F32)
    for entry in range(8):
        moved = jnp.where(leaf_octant == entry, apply(expanded, downward[entry]), moved)
    row_t = lax.broadcasted_iota(jnp.int32, (8, terms), 0)
    lines = []
    for spot in range(leaves // 8):
        low = sums[spot * 16 : spot * 16 + 8, :terms]
        high = sums[spot * 16 + 8 : spot * 16 + 16, :terms]
        low = low + pltpu.roll(low, 4, 0)
        high = high + pltpu.roll(high, 4, 0)
        lines.append(jnp.where(row_t < 4, low, high))
    local = wider(moved + jnp.concatenate(lines, axis=0))
    local_rows[...] = jnp.concatenate([local, local], axis=0).T

    u_x = targets[:SLOTS] - 0.5
    u_y = targets[SLOTS : 2 * SLOTS] - 0.5
    u_z = targets[2 * SLOTS : 3 * SLOTS] - 0.5
    value = grad_x = grad_y = grad_z = None
    for a in range(ORDER, -1, -1):
        inner = inner_y = inner_z = None
        for b in range(ORDER - a, -1, -1):
            here = local_rows[ROW_OF[(a, b, 0)] : ROW_OF[(a, b, 0)] + 1, :]
            if (a, b, 1) in ROW_OF:
                above = local_rows[ROW_OF[(a, b, 1)] : ROW_OF[(a, b, 1)] + 1, :]
                both = here + above * u_z
                inner_z = above if inner_z is None else inner_z * u_y + above
            else:
                both = here
            if inner is None:
                inner = jnp.broadcast_to(both, (SLOTS, LANES))
            else:
                inner_y = inner if inner_y is None else inner_y * u_y + inner
                inner = inner * u_y + both
        if value is None:
            value, grad_y, grad_z = inner, inner_y, inner_z
        else:
            grad_x = value if grad_x is None else grad_x * u_x + value
            value = value * u_x + inner
            if inner_y is not None:
                grad_y = inner_y if grad_y is None else grad_y * u_x + inner_y
            if inner_z is not None:
                grad_z = inner_z if grad_z is None else grad_z * u_x + inner_z

    def halves(total):
        return total + pltpu.roll(total, leaves, 1)

    self_term = targets[3 * SLOTS :] * (SOFTENING**-0.5)
    results = [
        halves(near[0]) - self_term + value,
        halves(near[1]) - grad_x,
        halves(near[2]) - grad_y,
        halves(near[3]) - grad_z,
    ]
    turned = jnp.concatenate(results, axis=0).T
    for entry in range(4):
        made = None
        for z in range(block_z):
            turn = (z - entry) * SLOTS % LANES
            held = turned[z * columns : (z + 1) * columns]
            held = pltpu.roll(held, turn, 1) if turn else held
            made = held if made is None else jnp.where(group == z, held, made)
        made = made * live
        for x in range(block_x):
            piece = made[x * block_y : (x + 1) * block_y]
            if entry == 0:
                potential_ref[x] = piece
            else:
                field_ref[entry - 1, x] = piece


def per_device(
    positions, charges, counts, moment_shift, far_operators, local_shift, lattice_operator
):
    block_x, block_y, column = charges.shape
    block_z = column // SLOTS
    sizes = (block_x, block_y, block_z)
    numbers = tuple(lax.axis_size(axis) for axis in ("gx", "gy", "gz"))
    devices = numbers[0] * numbers[1] * numbers[2]
    terms = moment_shift.shape[1]
    padded_terms = (terms + 15) // 16 * 16
    leaves = block_x * block_y * block_z
    plan, triples, none, starts = plan_table(block_x, block_z)
    offsets = offset_table().shape[0]
    wide_x, wide_z = block_x + 2 * HALO, block_z + 2 * HALO
    wide_leaves = wide_x * wide_z * (block_y + 2 * HALO)
    mid_columns = (block_x // 2 + 4) * (block_z // 2 + 4)
    tops = devices // 8
    anywhere = pl.BlockSpec(memory_space=pl.ANY)
    vmem = pl.BlockSpec(memory_space=pltpu.VMEM)
    layout = (triples, none, starts)
    batches = -(-offsets // (6 * PLACED))
    top_rows = (tops + 7) // 8 * 8
    placed = batches * PLACED
    spare = (placed * 6 * terms + 2 * LANES - far_operators.shape[1] + LANES) // LANES * LANES
    potential, field_out = pl.pallas_call(
        lambda *refs: field_kernel(sizes, numbers, layout, *refs),
        out_shape=(
            jax.ShapeDtypeStruct((block_x, block_y, column), F32),
            jax.ShapeDtypeStruct((3, block_x, block_y, column), F32),
        ),
        in_specs=[anywhere] * 8,
        out_specs=(vmem, vmem),
        scratch_shapes=[
            pltpu.VMEM(positions.shape, F32),
            pltpu.VMEM(charges.shape, F32),
            pltpu.VMEM(counts.shape, jnp.int32),
            pltpu.VMEM((terms, 8, terms), BF16),
            pltpu.VMEM((terms, far_operators.shape[1] + spare), BF16),
            pltpu.VMEM((terms, 8, terms), BF16),
            pltpu.VMEM((terms, terms), BF16),
            pltpu.VMEM((block_y // 2 + 2, wide_z, wide_x, 2, LANES), F32),
            pltpu.VMEM((wide_leaves + 16, LANES), F32),
            pltpu.VMEM((4 * SLOTS, LANES), F32),
            pltpu.VMEM((padded_terms * 8, LANES), F32),
            pltpu.VMEM((3, wide_leaves + 16, LANES), F32),
            pltpu.VMEM((3, wide_leaves + 16, LANES), F32),
            pltpu.VMEM((devices * 8, LANES), F32),
            pltpu.VMEM((terms * 8, LANES), F32),
            pltpu.VMEM((terms * 8, LANES), F32),
            pltpu.VMEM((6, devices + top_rows, LANES), F32),
            pltpu.VMEM((placed, padded_terms, 4 * LANES), BF16),
            pltpu.VMEM((14 * LANES, LANES), F32),
            pltpu.VMEM((6, none + 2 * starts + 3, 16, LANES), BF16),
            pltpu.VMEM((3, mid_columns * 8 + 16, LANES), F32),
            pltpu.VMEM((3, mid_columns * 8 + 16, LANES), F32),
            pltpu.VMEM((3, devices + tops + 2, 16, LANES), BF16),
            pltpu.VMEM((2 * leaves + 32, padded_terms), F32),
            pltpu.VMEM((LANES, LANES), F32),
            pltpu.SMEM(plan.shape, jnp.int32),
            pltpu.SMEM((4, LANES), jnp.int32),
            pltpu.SMEM((triples * 6,), jnp.int32),
            pltpu.SemaphoreType.DMA((8,)),
            pltpu.SemaphoreType.DMA((27,)),
            pltpu.SemaphoreType.DMA((27,)),
            pltpu.SemaphoreType.DMA((devices,)),
            pltpu.SemaphoreType.DMA((devices,)),
        ],
        compiler_params=pltpu.CompilerParams(
            vmem_limit_bytes=60 * 1024 * 1024, collective_id=0, has_side_effects=True
        ),
        name="fields",
    )(
        jnp.asarray(plan),
        positions,
        charges,
        counts,
        jnp.transpose(moment_shift, (1, 0, 2)),
        far_operators,
        jnp.transpose(local_shift, (1, 0, 2)),
        lattice_operator,
    )
    return potential, field_out


def solution(mesh):
    placed = (
        P(None, "gx", "gy", "gz"),
        P("gx", "gy", "gz"),
        P("gx", "gy", "gz"),
        P(),
        P(),
        P(),
        P(),
    )
    return jax.shard_map(
        per_device,
        mesh=mesh,
        in_specs=placed,
        out_specs=(P("gx", "gy", "gz"), P(None, "gx", "gy", "gz")),
        check_vma=False,
    )
```

```python
import jax
import jax.numpy as jnp
import numpy as np
from jax import lax
from jax.experimental import pallas as pl
from jax.experimental.pallas import tpu as pltpu
from jax.sharding import PartitionSpec as P

ORDER = 8
SLOTS = 32
SOFTENING = 0.0625
LANES = 128
HALO = 2
F32 = jnp.float32
BF16 = jnp.bfloat16
NT = (((1,), (1,)), ((), ()))
NN = (((1,), (0,)), ((), ()))
PLAN = 4
GROUP = 4
STEPS = 28
PLACED = 9


def offset_table():
    listed = []
    for shift_x in range(-3, 4):
        for shift_y in range(-3, 4):
            for shift_z in range(-3, 4):
                if max(abs(shift_x), abs(shift_y), abs(shift_z)) >= 2:
                    listed.append((shift_x, shift_y, shift_z))
    return np.array(listed, dtype=np.int32)


def exponent_table(degree):
    listed = []
    for accumulated in range(degree + 1):
        for height in (0, 1):
            for power_x in range(accumulated - height + 1):
                listed.append((power_x, accumulated - height - power_x, height))
    return np.array(listed, dtype=np.int32)


ROW_OF = {tuple(int(v) for v in key): row for row, key in enumerate(exponent_table(ORDER))}


def split_rows(data):
    upper = data.astype(BF16)
    lower = (data - upper.astype(F32)).astype(BF16)
    return upper, lower


def apply(data, operator):
    upper, lower = split_rows(data)
    rows = data.shape[0]
    both = jnp.concatenate([upper.astype(F32), lower.astype(F32)], axis=0).astype(BF16)
    found = lax.dot_general(both, operator, NT, preferred_element_type=F32)
    return found[:rows] + found[rows:]


def powers_of(values):
    listed = [jnp.ones_like(values)]
    for exponent in range(ORDER):
        listed.append(listed[-1] * values)
    return listed


def admits(shift, odd):
    return -2 - odd <= shift <= 3 - odd


def leaf_start(shift):
    return {-3: 7, 3: 8}.get(shift, shift + 2)


def plan_table(block_x, block_z):
    shifts = offset_table()
    wide_x, wide_z = block_x + 2 * HALO, block_z + 2 * HALO
    starts = wide_x + 3
    triples = STEPS * GROUP
    assert 3 * triples >= shifts.shape[0]
    plan = np.zeros((triples * 3, PLAN), np.int32)
    none = 7 * wide_z * starts
    plan[:, :2] = none
    plan[:, 2] = 49
    plan[:, 3] = 7
    for row, (dx, dy, dz) in enumerate(shifts):
        for z in range(2):
            if admits(dz, z):
                plan[row, z] = ((dy + 3) * wide_z + z + 2 + dz) * starts + leaf_start(dx)
        plan[row, 2] = (dx + 3) * 7 + dy + 3
        plan[row, 3] = dz + 3
    return plan.reshape(-1), triples, none, starts


def field_kernel(
    sizes,
    numbers,
    layout,
    plan_hbm,
    positions_hbm,
    charges_hbm,
    counts_hbm,
    shift_hbm,
    far_hbm,
    down_hbm,
    lattice_hbm,
    result_ref,
    positions,
    charges,
    counts,
    shift_raw,
    far,
    down_raw,
    lattice,
    raw,
    wide,
    targets,
    partial,
    moments_high,
    moments_low,
    mids,
    shift_rows,
    down_rows,
    uppers,
    operators,
    sources,
    pages,
    mid_high,
    mid_low,
    upper_pages,
    sums,
    local_rows,
    plan_ref,
    table,
    reach,
    loads,
    sends,
    receives,
    mid_send,
    mid_receive,
):
    block_x, block_y, block_z = sizes
    triples, none, starts = layout
    wide_x, wide_z = block_x + 2 * HALO, block_z + 2 * HALO
    rows_y = block_y + 2 * HALO
    columns = block_x * block_y
    leaves = columns * block_z
    terms = lattice.shape[0]
    padded_terms = operators.shape[1]
    offsets = offset_table().shape[0]
    at = tuple(lax.axis_index(axis) for axis in ("gx", "gy", "gz"))
    devices = numbers[0] * numbers[1] * numbers[2]
    rank = (at[0] * numbers[1] + at[1]) * numbers[2] + at[2]
    barrier = pltpu.get_barrier_semaphore()

    def other(step):
        return lax.rem(rank + step, devices)

    staged = [
        pltpu.make_async_copy(positions_hbm, positions, loads.at[0]),
        pltpu.make_async_copy(charges_hbm, charges, loads.at[1]),
        pltpu.make_async_copy(counts_hbm, counts, loads.at[2]),
        pltpu.make_async_copy(shift_hbm, shift_raw, loads.at[3]),
        pltpu.make_async_copy(far_hbm, far.at[:, pl.ds(0, far_hbm.shape[1])], loads.at[4]),
        pltpu.make_async_copy(down_hbm, down_raw, loads.at[5]),
        pltpu.make_async_copy(lattice_hbm, lattice, loads.at[6]),
        pltpu.make_async_copy(plan_hbm, plan_ref, loads.at[7]),
    ]
    for copy in staged:
        copy.start()

    def greet(step, carry):
        pl.semaphore_signal(
            barrier, inc=1, device_id=other(step), device_id_type=pl.DeviceIdType.LOGICAL
        )
        return carry

    lax.fori_loop(1, devices, greet, 0)

    lane = lax.broadcasted_iota(jnp.int32, (columns, LANES), 1)
    group = lane // SLOTS
    row8 = lax.broadcasted_iota(jnp.int32, (8, LANES), 0)
    for copy in staged[:3]:
        copy.wait()
    held = jnp.concatenate([counts[x] for x in range(block_x)], axis=0)
    limit = jnp.broadcast_to(held[:, 0:1], (columns, LANES))
    for z in range(1, block_z):
        limit = jnp.where(group == z, jnp.broadcast_to(held[:, z : z + 1], (columns, LANES)), limit)
    live = (lane % SLOTS < limit).astype(F32)
    parts = [
        jnp.concatenate([positions[c, x] for x in range(block_x)], axis=0) for c in range(3)
    ]
    parts.append(jnp.concatenate([charges[x] for x in range(block_x)], axis=0) * live)
    pieces = []
    for z in range(block_z):
        made = None
        for c in range(4):
            turn = (c - z) * SLOTS % LANES
            moved = pltpu.roll(parts[c], turn, 1) if turn else parts[c]
            made = moved if made is None else jnp.where(group == c, moved, made)
        pieces.append(made)
        for x in range(block_x):
            for pair in range(block_y // 2):
                start = x * block_y + 2 * pair
                raw[1 + pair, HALO + z, HALO + x] = made[start : start + 2]
    own = jnp.concatenate(pieces + pieces, axis=0)
    targets[...] = own.T

    pl.semaphore_wait(barrier, devices - 1)
    copies = []
    pairs = block_y // 2

    def span(move, size, halo):
        if move == 1:
            return pl.ds(size, halo), pl.ds(0, halo)
        if move == -1:
            return pl.ds(halo, halo), pl.ds(size + halo, halo)
        return pl.ds(halo, size), pl.ds(halo, size)

    for count in range(27):
        moves = (count // 9 - 1, count // 3 % 3 - 1, count % 3 - 1)
        if moves == (0, 0, 0):
            continue
        target = tuple(
            lax.rem(at[axis] + moves[axis] + numbers[axis], numbers[axis]) for axis in range(3)
        )
        from_x, to_x = span(moves[0], block_x, HALO)
        from_y, to_y = span(moves[1], pairs, 1)
        from_z, to_z = span(moves[2], block_z, HALO)
        copies.append(
            pltpu.make_async_remote_copy(
                src_ref=raw.at[from_y, from_z, from_x],
                dst_ref=raw.at[to_y, to_z, to_x],
                send_sem=sends.at[count],
                recv_sem=receives.at[count],
                device_id=target,
                device_id_type=pl.DeviceIdType.MESH,
            )
        )
    for copy in copies:
        copy.start()

    partial[pl.ds(terms * 8, partial.shape[0] - terms * 8), :] = jnp.zeros(
        (partial.shape[0] - terms * 8, LANES), F32
    )

    def moments(at_x, at_y, at_z, charge):
        quarter = SLOTS // 8
        centred_z = at_z - 0.5
        centred_y = at_y - 0.5
        powers_x = [value * charge for value in powers_of(at_x - 0.5)]
        power_y = None
        for b in range(ORDER + 1):
            power_y = None if b == 0 else (centred_y if b == 1 else power_y * centred_y)
            for a in range(ORDER + 1 - b):
                flat = powers_x[a] if b == 0 else powers_x[a] * power_y
                for height in (0, 1):
                    if a + b + height > ORDER:
                        continue
                    made = flat * centred_z if height else flat
                    total = made[:8]
                    for piece in range(1, quarter):
                        total = total + made[piece * 8 : piece * 8 + 8]
                    row = ROW_OF[(a, b, height)]
                    partial[row * 8 : row * 8 + 8, :] = total
        found = partial[pl.ds(0, padded_terms, stride=8), :]
        for line in range(1, 8):
            found = found + partial[pl.ds(line, padded_terms, stride=8), :]
        found = jnp.concatenate([found, jnp.zeros((LANES - padded_terms, LANES), F32)], axis=0)
        return found.T

    def rows_from(raw_ref, out_ref):
        out_ref[...] = jnp.zeros(out_ref.shape, F32)
        out_ref[:, :terms] = raw_ref[...].astype(F32).reshape(terms * 8, terms)

    def octant_of(ref, octant):
        return ref[pl.ds(octant, terms, stride=8), :].astype(BF16)

    own_moments = moments(
        targets[:SLOTS], targets[SLOTS : 2 * SLOTS], targets[2 * SLOTS : 3 * SLOTS], targets[3 * SLOTS :]
    )[:leaves]
    staged[3].wait()
    rows_from(shift_raw, shift_rows)
    leaf_row = lax.broadcasted_iota(jnp.int32, (leaves, terms), 0)
    leaf_octant = (
        4 * (leaf_row // block_y % 2) + 2 * (leaf_row % 2) + leaf_row // columns % 2
    )
    lifted = jnp.zeros((leaves, terms), F32)
    for octant in range(8):
        found = apply(own_moments, octant_of(shift_rows, octant))
        lifted = jnp.where(leaf_octant == octant, found, lifted)
    lines = []
    for z in range(block_z // 2):
        both = lifted[2 * z * columns : (2 * z + 1) * columns] + lifted[(2 * z + 1) * columns : (2 * z + 2) * columns]
        for x in range(block_x // 2):
            held = both[x * 8 : x * 8 + 8]
            held = held[:4] + held[4:]
            for y in range(block_y // 2):
                lines.append(held[2 * y : 2 * y + 1] + held[2 * y + 1 : 2 * y + 2])
    spare = jnp.zeros((8, LANES - terms), F32)
    own_slot = mids.at[pl.ds(pl.multiple_of(rank * 8, 8), 8)]
    own_slot[...] = jnp.concatenate([jnp.concatenate(lines, axis=0), spare], axis=1)

    def mid_copy(step):
        return pltpu.make_async_remote_copy(
            src_ref=own_slot,
            dst_ref=own_slot,
            send_sem=mid_send.at[step],
            recv_sem=mid_receive.at[step],
            device_id=other(step),
            device_id_type=pl.DeviceIdType.LOGICAL,
        )

    def send_mid(step, carry):
        mid_copy(step).start()
        return carry

    def wait_mid(step, carry):
        mid_copy(step).wait()
        return carry

    lax.fori_loop(1, devices, send_mid, 0)

    strides = (numbers[1] * numbers[2], numbers[2], 1)
    top_sizes = tuple(number // 2 for number in numbers)
    top_strides = (top_sizes[1] * top_sizes[2], top_sizes[2], 1)
    tops = devices // 8
    spots, top_spots = [], []
    for axis in range(3):
        odd = lax.rem(at[axis], 2)
        listed, top_listed = [], []
        for entry in range(7):
            shift = entry - 3
            size = numbers[axis]
            spot = lax.rem(at[axis] + shift + 4 * size, size) * strides[axis]
            if shift == -3:
                spot = jnp.where(odd == 1, spot, 4 * devices)
            if shift == 3:
                spot = jnp.where(odd == 0, spot, 4 * devices)
            listed.append(spot)
            size = top_sizes[axis]
            top_listed.append(
                lax.rem(lax.div(at[axis], 2) + shift + 4 * size, size) * top_strides[axis]
            )
        spots.append(listed)
        top_spots.append(top_listed)
    for x in range(7):
        for y in range(7):
            table[x * 7 + y] = spots[0][x] + spots[1][y]
            table[LANES + x * 7 + y] = top_spots[0][x] + top_spots[1][y]
    for z in range(7):
        table[2 * LANES + z] = spots[2][z]
        table[3 * LANES + z] = top_spots[2][z]
    for line, entry in ((0, 49), (1, 49), (2, 7), (3, 7)):
        table[line * LANES + entry] = jnp.int32(4 * devices)
    staged[7].wait()

    def reach_of(row):
        level, depth = plan_ref[row * PLAN + 2], plan_ref[row * PLAN + 3]
        reach[2 * row] = jnp.minimum(table[level] + table[2 * LANES + depth], devices)
        reach[2 * row + 1] = jnp.minimum(table[LANES + level] + table[3 * LANES + depth], tops) + devices + 1

    staged[4].wait()
    spare_width = far.shape[1] - far_hbm.shape[1]
    far[:, pl.ds(far_hbm.shape[1], spare_width)] = jnp.zeros((terms, spare_width), BF16)
    tall = lax.broadcasted_iota(jnp.int32, (padded_terms, LANES), 1)
    spare_rows = jnp.zeros((padded_terms - terms, LANES), BF16)

    def place(batch, carry):
        for local in range(2 * PLACED):
            triple = batch * (2 * PLACED) + local
            start = triple * (3 * terms)
            turn = start & (LANES - 1)
            base = pl.multiple_of(start - turn, LANES)
            back = (LANES - turn) & (LANES - 1)
            held = far[:, pl.ds(base, 3 * LANES)]
            turned = []
            for tile in range(3):
                piece = held[:, tile * LANES : (tile + 1) * LANES]
                turned.append(pltpu.roll(jnp.concatenate([piece, spare_rows], axis=0), back, 1))
            kept = tall < LANES - turn
            for tile in range(2):
                found = jnp.where(kept, turned[tile], turned[tile + 1])
                spot = (local % 2) * 2 + tile
                operators[
                    batch * PLACED + local // 2, :, spot * LANES : (spot + 1) * LANES
                ] = found
            for kind in range(3):
                reach_of(3 * triple + kind)
        return carry

    used = operators.shape[0]
    lax.fori_loop(0, used // PLACED, place, 0)
    for row in range(used * 6, triples * 3):
        reach_of(row)

    for copy in copies:
        copy.wait()
    guard = 8

    def clear(ref):
        ref[:guard, :] = jnp.zeros((guard, LANES), F32)
        ref[ref.shape[0] - guard :, :] = jnp.zeros((guard, LANES), F32)

    clear(wide)
    for kind in range(3):
        for ref in (moments_high, moments_low, mid_high, mid_low):
            clear(ref.at[kind])

    def third(value):
        return (value, pltpu.roll(value, terms, 1), pltpu.roll(value, 2 * terms - LANES, 1))

    def halved(value):
        upper = value.astype(BF16).astype(F32)
        return upper, (value - upper).astype(BF16).astype(F32)

    def widen(z, carry):
        for x in range(wide_x):
            column = jnp.concatenate([raw[pair, z, x] for pair in range(pairs + 2)], axis=0)
            wide[pl.ds(pl.multiple_of(guard + (z * wide_x + x) * rows_y, 8), rows_y), :] = column
        return carry

    lax.fori_loop(0, wide_z, widen, 0)

    def window(tile, carry):
        start = pl.multiple_of(guard + tile * LANES, 8)
        turned = wide[pl.ds(start, LANES), :].T
        found = moments(
            turned[:SLOTS], turned[SLOTS : 2 * SLOTS], turned[2 * SLOTS : 3 * SLOTS], turned[3 * SLOTS :]
        )
        for kind, value in enumerate(third(found)):
            upper, lower = halved(value)
            moments_high[kind, pl.ds(start, LANES), :] = upper
            moments_low[kind, pl.ds(start, LANES), :] = lower
        return carry

    lax.fori_loop(0, wide_x * wide_z * rows_y // LANES, window, 0, unroll=2)

    near_shifts = [(x, y, z) for x in (-1, 0, 1) for y in (-1, 0, 1) for z in (-1, 0, 1)]
    lane8 = lax.broadcasted_iota(jnp.int32, (8, LANES), 1)
    group8 = lane8 // SLOTS

    def shifted(shift):
        moved = jnp.where(
            group8 == 0,
            float(shift[0]),
            jnp.where(group8 == 1, float(shift[1]), jnp.where(group8 == 2, float(shift[2]), 0.0)),
        )
        found = []
        for z in range(block_z):
            for x in range(0, block_x, 2):
                spot = (z + HALO + shift[2]) * wide_x + x + HALO + shift[0]
                low = guard + spot * rows_y + HALO + shift[1]
                high = low + rows_y - block_y
                held = jnp.where(row8 < block_y, wide[low : low + 8, :], wide[high : high + 8, :])
                found.append(held + moved)
        return found

    for pair in range((len(near_shifts) + 1) // 2):
        first = shifted(near_shifts[2 * pair])
        if 2 * pair + 1 < len(near_shifts):
            second = shifted(near_shifts[2 * pair + 1])
        else:
            second = [jnp.where(group8 < 3, value, 0.0) for value in first]
        sources[pair * LANES : (pair + 1) * LANES, :] = jnp.concatenate(first + second, axis=0).T

    odd_line = row8 % 2 == 1
    zero8 = jnp.zeros((8, LANES), F32)

    def parity(page, shift):
        if shift == -3:
            return jnp.where(odd_line, page, 0.0)
        if shift == 3:
            return jnp.where(odd_line, 0.0, page)
        return page

    def fill_pages(z, carry):
        for shift in range(-3, 4):
            spot = ((shift + 3) * wide_z + z) * starts
            for kind in range(3):
                made = []
                for x in range(wide_x):
                    start = guard + (z * wide_x + x) * rows_y + HALO + shift
                    page = jnp.where(
                        row8 < block_y,
                        moments_high[kind, pl.ds(start, 8), :],
                        moments_low[kind, pl.ds(start - block_y, 8), :],
                    )
                    made.append(parity(page, shift))
                listed = [(x, made[x], made[x + 1]) for x in range(wide_x - 1)]
                listed += [(7, zero8, made[0]), (9, zero8, made[2])]
                listed += [(8, made[5], zero8), (10, made[7], zero8)]
                for entry, low, high in listed:
                    pages[kind, spot + entry] = jnp.concatenate([low, high], axis=0).astype(BF16)
        return carry

    lax.fori_loop(0, wide_z, fill_pages, 0)
    for kind in range(6):
        for entry in range(pages.shape[1] - none):
            pages[kind, none + entry] = jnp.zeros((16, LANES), BF16)

    lax.fori_loop(1, devices, wait_mid, 0)
    mid_x, mid_z = block_x // 2 + 4, block_z // 2 + 4
    around = []
    for count in range(27):
        moves = (count // 9 - 1, count // 3 % 3 - 1, count % 3 - 1)
        there = [lax.rem(at[axis] + moves[axis] + numbers[axis], numbers[axis]) for axis in range(3)]
        around.append(((there[0] * numbers[1] + there[1]) * numbers[2] + there[2]) * 8)
    for z in range(mid_z):
        for x in range(mid_x):
            line = (z % 2 * 2 + x % 2) * 2
            listed = []
            for y in range(3):
                base = around[(x // 2 * 3 + y) * 3 + z // 2]
                listed.append(mids[pl.ds(base + line, 2), :])
            listed.append(jnp.zeros((2, LANES), F32))
            held = jnp.concatenate(listed, axis=0)
            start = guard + (z * mid_x + x) * 8
            for kind, value in enumerate(third(held)):
                upper, lower = halved(value)
                mid_high[kind, start : start + 8, :] = upper
                mid_low[kind, start : start + 8, :] = lower

    def fill_mids(z, carry):
        for shift in range(-3, 4):
            spot = ((shift + 3) * wide_z + z) * starts
            for kind in range(3):
                made = []
                for x in range(mid_x):
                    start = guard + (z * mid_x + x) * 8 + 2 + shift
                    page = jnp.where(
                        row8 < 2,
                        mid_high[kind, pl.ds(start, 8), :],
                        mid_low[kind, pl.ds(start - 2, 8), :],
                    )
                    made.append(parity(page, shift))
                moved = [pltpu.roll(page, 4, 0) for page in made]
                listed = [(x, made[x], moved[x + 1]) for x in range(mid_x - 1)]
                listed += [(7, zero8, moved[0]), (8, made[5], zero8)]
                for entry, low, high in listed:
                    page = jnp.where(row8 < 4, low, high)
                    pages[3 + kind, spot + entry] = jnp.concatenate([page, page], axis=0).astype(BF16)
        return carry

    lax.fori_loop(0, mid_z, fill_mids, 0)

    raised = jnp.zeros((devices, terms), F32)
    for octant in range(8):
        line = (octant % 2 * 2 + octant // 4) * 2 + octant // 2 % 2
        raised = raised + apply(mids[pl.ds(line, devices, stride=8), :], octant_of(shift_rows, octant))
    raised = jnp.concatenate([raised, jnp.zeros((devices, LANES - terms), F32)], axis=1)
    rank_row = lax.broadcasted_iota(jnp.int32, (devices, terms), 0)
    rank_octant = (
        4 * (rank_row // strides[0] % 2) + 2 * (rank_row // strides[1] % 2) + rank_row % 2
    )
    lifted = jnp.zeros((devices, terms), F32)
    for octant in range(8):
        found = apply(raised, octant_of(shift_rows, octant))
        lifted = jnp.where(rank_octant == octant, found, lifted)
    root = jnp.sum(lifted, axis=0, keepdims=True)
    top_rows = (tops + 7) // 8 * 8
    picker_row = lax.broadcasted_iota(jnp.int32, (top_rows, devices), 0)
    picker_rank = lax.broadcasted_iota(jnp.int32, (top_rows, devices), 1)
    parent_of = (
        picker_rank // strides[0] // 2 * top_strides[0]
        + picker_rank // strides[1] % numbers[1] // 2 * top_strides[1]
        + picker_rank % numbers[2] // 2
    )
    picker = (picker_row == parent_of).astype(F32)
    merged = lax.dot_general(
        picker, lifted, NN, precision=lax.Precision.HIGHEST, preferred_element_type=F32
    )
    merged = jnp.concatenate([merged, jnp.zeros((top_rows, LANES - terms), F32)], axis=1)
    for kind, value in enumerate(third(jnp.concatenate([raised, merged], axis=0))):
        upper, lower = halved(value)
        uppers[2 * kind] = upper
        uppers[2 * kind + 1] = lower

    def fill_uppers(line):
        def fill(entry, carry):
            for kind in range(3):
                high = jnp.broadcast_to(uppers[2 * kind, pl.ds(line[1] + entry, 1), :], (8, LANES))
                low = jnp.broadcast_to(uppers[2 * kind + 1, pl.ds(line[1] + entry, 1), :], (8, LANES))
                page = jnp.where(row8 == line[0], high, jnp.where(row8 == line[0] + 1, low, 0.0))
                upper_pages[kind, line[2] + entry] = jnp.concatenate([page, zero8], axis=0).astype(BF16)
            return carry

        return fill

    lax.fori_loop(0, devices, fill_uppers((0, 0, 0)), 0, unroll=8)
    lax.fori_loop(0, tops, fill_uppers((2, devices, devices + 1)), 0, unroll=4)
    for kind in range(3):
        upper_pages[kind, devices] = jnp.zeros((16, LANES), BF16)
        upper_pages[kind, devices + 1 + tops] = jnp.zeros((16, LANES), BF16)

    lane16 = lax.broadcasted_iota(jnp.int32, (16, LANES), 1)
    first_part = lane16 < terms
    second_part = lane16 < 2 * terms - LANES

    first_eight = lax.broadcasted_iota(jnp.int32, (16, LANES), 0) < 8

    def far_rows(triple):
        rows = [3 * triple + kind for kind in range(3)]
        spots = [[plan_ref[row * PLAN + odd] for odd in range(2)] for row in rows]

        def tiles(held):
            return jnp.concatenate(
                [
                    jnp.where(first_part, held[0], held[1]),
                    jnp.where(second_part, held[1], held[2]),
                ],
                axis=1,
            )

        found = []
        for z in range(block_z):
            for x in range(block_x // 2):
                step = z // 2 * 2 * starts + 2 * x
                found.append(tiles([pages[kind, spots[kind][z % 2] + step] for kind in range(3)]))
        held = []
        for kind in range(3):
            even, odd = pages[3 + kind, spots[kind][0]], pages[3 + kind, spots[kind][1]]
            held.append(jnp.where(first_eight, even, odd))
        found.append(tiles(held))
        held = []
        for kind, row in enumerate(rows):
            held.append(upper_pages[kind, reach[2 * row]] + upper_pages[kind, reach[2 * row + 1]])
        found.append(tiles(held))
        return jnp.concatenate(found, axis=0)

    total_rows = 2 * leaves + 32
    sums[...] = jnp.zeros(sums.shape, F32)
    near_steps = sources.shape[0] // LANES
    per_step = SLOTS

    def both_step(step, totals):
        sum_p, sum_x, sum_y, sum_z = totals
        first = step * per_step
        base = lax.div(first, SLOTS) * LANES + lax.rem(first, SLOTS)
        for line in range(per_step):
            s_x = sources[pl.ds(base + line, 1), :]
            s_y = sources[pl.ds(base + line + SLOTS, 1), :]
            s_z = sources[pl.ds(base + line + 2 * SLOTS, 1), :]
            s_q = sources[pl.ds(base + line + 3 * SLOTS, 1), :]
            d_x = targets[:SLOTS] - s_x
            d_y = targets[SLOTS : 2 * SLOTS] - s_y
            d_z = targets[2 * SLOTS : 3 * SLOTS] - s_z
            inverse = lax.rsqrt(d_x * d_x + d_y * d_y + d_z * d_z + SOFTENING)
            weight = s_q * inverse
            sum_p = sum_p + weight
            cubic = weight * (inverse * inverse)
            sum_x = sum_x + cubic * d_x
            sum_y = sum_y + cubic * d_y
            sum_z = sum_z + cubic * d_z
        return sum_p, sum_x, sum_y, sum_z

    def far_step(step, carry):
        added = []
        for which in range(14):
            pair = step * 14 + which
            left = jnp.concatenate([far_rows(2 * pair), far_rows(2 * pair + 1)], axis=1)
            added.append(lax.dot_general(left, operators[jnp.minimum(pair, used - 1)], NT, preferred_element_type=F32))
        total = added[0]
        for value in added[1:]:
            total = total + value
        sums[...] += total
        return carry

    lax.fori_loop(0, STEPS * GROUP // 28, far_step, 0)
    zero = jnp.zeros((SLOTS, LANES), F32)
    near = lax.fori_loop(0, near_steps, both_step, (zero, zero, zero, zero))

    staged[5].wait()
    staged[6].wait()
    rows_from(down_raw, down_rows)
    first = 2 * leaves + 16
    held = sums[first : first + 8, :terms]
    far_upper = held[0:1] + held[1:2]
    far_top = held[2:3] + held[3:4]

    def lattice_apply(value):
        return apply(jnp.broadcast_to(value, (8, terms)), lattice[...])

    def wider(value):
        return jnp.concatenate([value, jnp.zeros((value.shape[0], LANES - terms), F32)], axis=1)

    top_local = 0.125 * (far_top + lattice_apply(root)[:1])
    octant = lax.rem(at[0], 2) * 4 + lax.rem(at[1], 2) * 2 + lax.rem(at[2], 2)
    moved = apply(jnp.broadcast_to(wider(top_local), (8, LANES)), octant_of(down_rows, octant))
    upper_local = jnp.broadcast_to(wider(0.25 * far_upper + moved[:1]), (8, LANES))
    mid_row = lax.broadcasted_iota(jnp.int32, (8, terms), 0)
    mid_octant = 4 * (mid_row // 2 % 2) + 2 * (mid_row % 2) + mid_row // 4
    held = sums[2 * leaves : 2 * leaves + 16, :terms]
    lines = []
    for z in range(2):
        for x in range(2):
            start = z * 8 + x * 4
            lines.append(held[start : start + 2] + held[start + 2 : start + 4])
    far_mid = jnp.concatenate(lines, axis=0)
    downward = [octant_of(down_rows, entry) for entry in range(8)]
    moved = jnp.zeros((8, terms), F32)
    for entry in range(8):
        moved = jnp.where(mid_octant == entry, apply(upper_local, downward[entry]), moved)
    mid_local = wider(0.5 * far_mid + moved)
    expanded = []
    for z in range(block_z):
        for x in range(block_x // 2):
            line = (z // 2 * 2 + x) * 2
            low = jnp.broadcast_to(mid_local[line : line + 1], (8, LANES))
            high = jnp.broadcast_to(mid_local[line + 1 : line + 2], (8, LANES))
            expanded.append(jnp.where(row8 % 4 < 2, low, high))
    expanded = jnp.concatenate(expanded, axis=0)
    moved = jnp.zeros((leaves, terms), F32)
    for entry in range(8):
        moved = jnp.where(leaf_octant == entry, apply(expanded, downward[entry]), moved)
    row_t = lax.broadcasted_iota(jnp.int32, (8, terms), 0)
    lines = []
    for spot in range(leaves // 8):
        low = sums[spot * 16 : spot * 16 + 8, :terms]
        high = sums[spot * 16 + 8 : spot * 16 + 16, :terms]
        low = low + pltpu.roll(low, 4, 0)
        high = high + pltpu.roll(high, 4, 0)
        lines.append(jnp.where(row_t < 4, low, high))
    local = wider(moved + jnp.concatenate(lines, axis=0))
    local_rows[...] = jnp.concatenate([local, local], axis=0).T

    u_x = targets[:SLOTS] - 0.5
    u_y = targets[SLOTS : 2 * SLOTS] - 0.5
    u_z = targets[2 * SLOTS : 3 * SLOTS] - 0.5
    value = grad_x = grad_y = grad_z = None
    for a in range(ORDER, -1, -1):
        inner = inner_y = inner_z = None
        for b in range(ORDER - a, -1, -1):
            here = local_rows[ROW_OF[(a, b, 0)] : ROW_OF[(a, b, 0)] + 1, :]
            if (a, b, 1) in ROW_OF:
                above = local_rows[ROW_OF[(a, b, 1)] : ROW_OF[(a, b, 1)] + 1, :]
                both = here + above * u_z
                inner_z = above if inner_z is None else inner_z * u_y + above
            else:
                both = here
            if inner is None:
                inner = jnp.broadcast_to(both, (SLOTS, LANES))
            else:
                inner_y = inner if inner_y is None else inner_y * u_y + inner
                inner = inner * u_y + both
        if value is None:
            value, grad_y, grad_z = inner, inner_y, inner_z
        else:
            grad_x = value if grad_x is None else grad_x * u_x + value
            value = value * u_x + inner
            if inner_y is not None:
                grad_y = inner_y if grad_y is None else grad_y * u_x + inner_y
            if inner_z is not None:
                grad_z = inner_z if grad_z is None else grad_z * u_x + inner_z

    def halves(total):
        return total + pltpu.roll(total, leaves, 1)

    self_term = targets[3 * SLOTS :] * (SOFTENING**-0.5)
    results = [
        halves(near[0]) - self_term + value,
        halves(near[1]) - grad_x,
        halves(near[2]) - grad_y,
        halves(near[3]) - grad_z,
    ]
    turned = jnp.concatenate(results, axis=0).T
    for entry in range(4):
        made = None
        for z in range(block_z):
            turn = (z - entry) * SLOTS % LANES
            held = turned[z * columns : (z + 1) * columns]
            held = pltpu.roll(held, turn, 1) if turn else held
            made = held if made is None else jnp.where(group == z, held, made)
        made = made * live
        for x in range(block_x):
            piece = made[x * block_y : (x + 1) * block_y]
            result_ref[entry, x] = piece


def part_kernel(result_ref, potential_ref, field_ref, sems):
    copies = [
        pltpu.make_async_copy(result_ref.at[0], potential_ref, sems.at[0]),
        pltpu.make_async_copy(result_ref.at[pl.ds(1, 3)], field_ref, sems.at[1]),
    ]
    for copy in copies:
        copy.start()
    for copy in copies:
        copy.wait()


def per_device(
    positions, charges, counts, moment_shift, far_operators, local_shift, lattice_operator
):
    block_x, block_y, column = charges.shape
    block_z = column // SLOTS
    sizes = (block_x, block_y, block_z)
    numbers = tuple(lax.axis_size(axis) for axis in ("gx", "gy", "gz"))
    devices = numbers[0] * numbers[1] * numbers[2]
    terms = moment_shift.shape[1]
    padded_terms = (terms + 15) // 16 * 16
    leaves = block_x * block_y * block_z
    plan, triples, none, starts = plan_table(block_x, block_z)
    offsets = offset_table().shape[0]
    wide_x, wide_z = block_x + 2 * HALO, block_z + 2 * HALO
    wide_leaves = wide_x * wide_z * (block_y + 2 * HALO)
    mid_columns = (block_x // 2 + 4) * (block_z // 2 + 4)
    tops = devices // 8
    anywhere = pl.BlockSpec(memory_space=pltpu.HBM)
    vmem = pl.BlockSpec(memory_space=pltpu.VMEM)
    layout = (triples, none, starts)
    batches = -(-offsets // (6 * PLACED))
    top_rows = (tops + 7) // 8 * 8
    placed = batches * PLACED
    spare = (placed * 6 * terms + 2 * LANES - far_operators.shape[1] + LANES) // LANES * LANES
    result = pl.pallas_call(
        lambda *refs: field_kernel(sizes, numbers, layout, *refs),
        out_shape=pltpu.VMEM((4, block_x, block_y, column), F32),
        in_specs=[anywhere] * 8,
        out_specs=vmem,
        scratch_shapes=[
            pltpu.VMEM(positions.shape, F32),
            pltpu.VMEM(charges.shape, F32),
            pltpu.VMEM(counts.shape, jnp.int32),
            pltpu.VMEM((terms, 8, terms), BF16),
            pltpu.VMEM((terms, far_operators.shape[1] + spare), BF16),
            pltpu.VMEM((terms, 8, terms), BF16),
            pltpu.VMEM((terms, terms), BF16),
            pltpu.VMEM((block_y // 2 + 2, wide_z, wide_x, 2, LANES), F32),
            pltpu.VMEM((wide_leaves + 16, LANES), F32),
            pltpu.VMEM((4 * SLOTS, LANES), F32),
            pltpu.VMEM((padded_terms * 8, LANES), F32),
            pltpu.VMEM((3, wide_leaves + 16, LANES), F32),
            pltpu.VMEM((3, wide_leaves + 16, LANES), F32),
            pltpu.VMEM((devices * 8, LANES), F32),
            pltpu.VMEM((terms * 8, LANES), F32),
            pltpu.VMEM((terms * 8, LANES), F32),
            pltpu.VMEM((6, devices + top_rows, LANES), F32),
            pltpu.VMEM((placed, padded_terms, 4 * LANES), BF16),
            pltpu.VMEM((14 * LANES, LANES), F32),
            pltpu.VMEM((6, none + 2 * starts + 3, 16, LANES), BF16),
            pltpu.VMEM((3, mid_columns * 8 + 16, LANES), F32),
            pltpu.VMEM((3, mid_columns * 8 + 16, LANES), F32),
            pltpu.VMEM((3, devices + tops + 2, 16, LANES), BF16),
            pltpu.VMEM((2 * leaves + 32, padded_terms), F32),
            pltpu.VMEM((LANES, LANES), F32),
            pltpu.SMEM(plan.shape, jnp.int32),
            pltpu.SMEM((4 * LANES,), jnp.int32),
            pltpu.SMEM((triples * 6,), jnp.int32),
            pltpu.SemaphoreType.DMA((8,)),
            pltpu.SemaphoreType.DMA((27,)),
            pltpu.SemaphoreType.DMA((27,)),
            pltpu.SemaphoreType.DMA((devices,)),
            pltpu.SemaphoreType.DMA((devices,)),
        ],
        compiler_params=pltpu.CompilerParams(
            vmem_limit_bytes=60 * 1024 * 1024, collective_id=0, has_side_effects=True
        ),
        name="fields",
    )(
        jnp.asarray(plan),
        positions,
        charges,
        counts,
        jnp.transpose(moment_shift, (1, 0, 2)),
        far_operators,
        jnp.transpose(local_shift, (1, 0, 2)),
        lattice_operator,
    )
    return pl.pallas_call(
        part_kernel,
        out_shape=(
            jax.ShapeDtypeStruct((block_x, block_y, column), F32),
            jax.ShapeDtypeStruct((3, block_x, block_y, column), F32),
        ),
        in_specs=[vmem],
        out_specs=(anywhere, anywhere),
        scratch_shapes=[pltpu.SemaphoreType.DMA((2,))],
        compiler_params=pltpu.CompilerParams(vmem_limit_bytes=4 * 1024 * 1024),
        name="part",
    )(result)


def solution(mesh):
    placed = (
        P(None, "gx", "gy", "gz"),
        P("gx", "gy", "gz"),
        P("gx", "gy", "gz"),
        P(),
        P(),
        P(),
        P(),
    )
    return jax.shard_map(
        per_device,
        mesh=mesh,
        in_specs=placed,
        out_specs=(P("gx", "gy", "gz"), P(None, "gx", "gy", "gz")),
        check_vma=False,
    )
```

```python
import jax
import jax.numpy as jnp
import numpy as np
from jax import lax
from jax.experimental import pallas as pl
from jax.experimental.pallas import tpu as pltpu
from jax.sharding import PartitionSpec as P

ORDER = 8
SLOTS = 32
SOFTENING = 0.0625
LANES = 128
HALO = 2
F32 = jnp.float32
BF16 = jnp.bfloat16
NT = (((1,), (1,)), ((), ()))
NN = (((1,), (0,)), ((), ()))
PLAN = 4
GROUP = 4
STEPS = 28
PLACED = 9


def offset_table():
    listed = []
    for shift_x in range(-3, 4):
        for shift_y in range(-3, 4):
            for shift_z in range(-3, 4):
                if max(abs(shift_x), abs(shift_y), abs(shift_z)) >= 2:
                    listed.append((shift_x, shift_y, shift_z))
    return np.array(listed, dtype=np.int32)


def exponent_table(degree):
    listed = []
    for accumulated in range(degree + 1):
        for height in (0, 1):
            for power_x in range(accumulated - height + 1):
                listed.append((power_x, accumulated - height - power_x, height))
    return np.array(listed, dtype=np.int32)


ROW_OF = {tuple(int(v) for v in key): row for row, key in enumerate(exponent_table(ORDER))}


def split_rows(data):
    upper = data.astype(BF16)
    lower = (data - upper.astype(F32)).astype(BF16)
    return upper, lower


def apply(data, operator):
    upper, lower = split_rows(data)
    rows = data.shape[0]
    both = jnp.concatenate([upper.astype(F32), lower.astype(F32)], axis=0).astype(BF16)
    found = lax.dot_general(both, operator, NT, preferred_element_type=F32)
    return found[:rows] + found[rows:]


def powers_of(values):
    listed = [jnp.ones_like(values)]
    for exponent in range(ORDER):
        listed.append(listed[-1] * values)
    return listed


def admits(shift, odd):
    return -2 - odd <= shift <= 3 - odd


def leaf_start(shift):
    return {-3: 7, 3: 8}.get(shift, shift + 2)


def plan_table(block_x, block_z):
    shifts = offset_table()
    wide_x, wide_z = block_x + 2 * HALO, block_z + 2 * HALO
    starts = wide_x + 3
    triples = STEPS * GROUP
    assert 3 * triples >= shifts.shape[0]
    plan = np.zeros((triples * 3, PLAN), np.int32)
    none = 7 * wide_z * starts
    plan[:, :2] = none
    plan[:, 2] = 49
    plan[:, 3] = 7
    for row, (dx, dy, dz) in enumerate(shifts):
        for z in range(2):
            if admits(dz, z):
                plan[row, z] = ((dy + 3) * wide_z + z + 2 + dz) * starts + leaf_start(dx)
        plan[row, 2] = (dx + 3) * 7 + dy + 3
        plan[row, 3] = dz + 3
    return plan.reshape(-1), triples, none, starts


def field_kernel(
    sizes,
    numbers,
    layout,
    plan_hbm,
    positions_hbm,
    charges_hbm,
    counts_hbm,
    shift_hbm,
    far_hbm,
    down_hbm,
    lattice_hbm,
    result_ref,
    positions,
    charges,
    counts,
    shift_raw,
    far,
    down_raw,
    lattice,
    raw,
    wide,
    targets,
    partial,
    moments_high,
    moments_low,
    mids,
    shift_rows,
    down_rows,
    uppers,
    operators,
    sources,
    pages,
    mid_high,
    mid_low,
    upper_pages,
    sums,
    local_rows,
    plan_ref,
    table,
    reach,
    loads,
    sends,
    receives,
    mid_send,
    mid_receive,
    arrived,
    upper_send,
    upper_receive,
):
    block_x, block_y, block_z = sizes
    triples, none, starts = layout
    wide_x, wide_z = block_x + 2 * HALO, block_z + 2 * HALO
    rows_y = block_y + 2 * HALO
    columns = block_x * block_y
    leaves = columns * block_z
    terms = lattice.shape[0]
    padded_terms = operators.shape[1]
    offsets = offset_table().shape[0]
    at = tuple(lax.axis_index(axis) for axis in ("gx", "gy", "gz"))
    devices = numbers[0] * numbers[1] * numbers[2]
    rank = (at[0] * numbers[1] + at[1]) * numbers[2] + at[2]
    barrier = pltpu.get_barrier_semaphore()

    def other(step):
        if devices & (devices - 1) == 0:
            return (rank + step) & (devices - 1)
        return lax.rem(rank + step, devices)

    def each_other(action):
        if devices <= 64:
            for step in range(1, devices):
                action(step, 0)
        else:
            lax.fori_loop(1, devices, action, 0)

    staged = [
        pltpu.make_async_copy(positions_hbm, positions, loads.at[0]),
        pltpu.make_async_copy(charges_hbm, charges, loads.at[1]),
        pltpu.make_async_copy(counts_hbm, counts, loads.at[2]),
        pltpu.make_async_copy(shift_hbm, shift_raw, loads.at[3]),
        pltpu.make_async_copy(far_hbm, far.at[:, pl.ds(0, far_hbm.shape[1])], loads.at[4]),
        pltpu.make_async_copy(down_hbm, down_raw, loads.at[5]),
        pltpu.make_async_copy(lattice_hbm, lattice, loads.at[6]),
        pltpu.make_async_copy(plan_hbm, plan_ref, loads.at[7]),
    ]
    for copy in staged:
        copy.start()

    def greet(step, carry):
        pl.semaphore_signal(
            barrier, inc=1, device_id=other(step), device_id_type=pl.DeviceIdType.LOGICAL
        )
        return carry

    each_other(greet)

    lane = lax.broadcasted_iota(jnp.int32, (columns, LANES), 1)
    group = lane // SLOTS
    row8 = lax.broadcasted_iota(jnp.int32, (8, LANES), 0)
    for copy in staged[:3]:
        copy.wait()
    held = jnp.concatenate([counts[x] for x in range(block_x)], axis=0)
    limit = jnp.broadcast_to(held[:, 0:1], (columns, LANES))
    for z in range(1, block_z):
        limit = jnp.where(group == z, jnp.broadcast_to(held[:, z : z + 1], (columns, LANES)), limit)
    live = (lane % SLOTS < limit).astype(F32)
    parts = [
        jnp.concatenate([positions[c, x] for x in range(block_x)], axis=0) for c in range(3)
    ]
    parts.append(jnp.concatenate([charges[x] for x in range(block_x)], axis=0) * live)
    pieces = []
    for z in range(block_z):
        made = None
        for c in range(4):
            turn = (c - z) * SLOTS % LANES
            moved = pltpu.roll(parts[c], turn, 1) if turn else parts[c]
            made = moved if made is None else jnp.where(group == c, moved, made)
        pieces.append(made)
        for x in range(block_x):
            for pair in range(block_y // 2):
                start = x * block_y + 2 * pair
                raw[1 + pair, HALO + z, HALO + x] = made[start : start + 2]
    own = jnp.concatenate(pieces + pieces, axis=0)
    targets[...] = own.T

    pl.semaphore_wait(barrier, devices - 1)
    pairs = block_y // 2

    def span(move, size, halo):
        if move == 1:
            return pl.ds(size, halo), pl.ds(0, halo)
        if move == -1:
            return pl.ds(halo, halo), pl.ds(size + halo, halo)
        return pl.ds(halo, size), pl.ds(halo, size)

    direct, relayed = [], []
    for count in range(27):
        moves = (count // 9 - 1, count // 3 % 3 - 1, count % 3 - 1)
        if moves == (0, 0, 0):
            continue
        from_x, to_x = span(moves[0], block_x, HALO)
        from_y, to_y = span(moves[1], pairs, 1)
        from_z, to_z = span(moves[2], block_z, HALO)
        relay = moves[0] != 0 and moves[1:] != (0, 0)
        steps = (0 if relay else moves[0],) + moves[1:]
        target = tuple(
            lax.rem(at[axis] + steps[axis] + numbers[axis], numbers[axis]) for axis in range(3)
        )
        copy = pltpu.make_async_remote_copy(
            src_ref=raw.at[from_y, from_z, to_x if relay else from_x],
            dst_ref=raw.at[to_y, to_z, to_x],
            send_sem=sends.at[count],
            recv_sem=receives.at[count],
            device_id=target,
            device_id_type=pl.DeviceIdType.MESH,
        )
        (relayed if relay else direct).append((moves, copy))
    along_x = [copy for moves, copy in direct if moves[0] != 0]
    beside = [copy for moves, copy in direct if moves[0] == 0]
    relayed = [copy for moves, copy in relayed]
    for copy in along_x + beside:
        copy.start()

    partial[pl.ds(terms * 8, partial.shape[0] - terms * 8), :] = jnp.zeros(
        (partial.shape[0] - terms * 8, LANES), F32
    )

    def moments(at_x, at_y, at_z, charge):
        quarter = SLOTS // 8
        centred_z = at_z - 0.5
        centred_y = at_y - 0.5
        powers_x = [value * charge for value in powers_of(at_x - 0.5)]
        power_y = None
        for b in range(ORDER + 1):
            power_y = None if b == 0 else (centred_y if b == 1 else power_y * centred_y)
            for a in range(ORDER + 1 - b):
                flat = powers_x[a] if b == 0 else powers_x[a] * power_y
                for height in (0, 1):
                    if a + b + height > ORDER:
                        continue
                    made = flat * centred_z if height else flat
                    total = made[:8]
                    for piece in range(1, quarter):
                        total = total + made[piece * 8 : piece * 8 + 8]
                    row = ROW_OF[(a, b, height)]
                    partial[row * 8 : row * 8 + 8, :] = total
        found = partial[pl.ds(0, padded_terms, stride=8), :]
        for line in range(1, 8):
            found = found + partial[pl.ds(line, padded_terms, stride=8), :]
        found = jnp.concatenate([found, jnp.zeros((LANES - padded_terms, LANES), F32)], axis=0)
        return found.T

    def rows_from(raw_ref, out_ref):
        out_ref[...] = jnp.zeros(out_ref.shape, F32)
        out_ref[:, :terms] = raw_ref[...].astype(F32).reshape(terms * 8, terms)

    def octant_of(ref, octant):
        return ref[pl.ds(octant, terms, stride=8), :].astype(BF16)

    own_moments = moments(
        targets[:SLOTS], targets[SLOTS : 2 * SLOTS], targets[2 * SLOTS : 3 * SLOTS], targets[3 * SLOTS :]
    )[:leaves]
    staged[3].wait()
    rows_from(shift_raw, shift_rows)
    leaf_row = lax.broadcasted_iota(jnp.int32, (leaves, terms), 0)
    leaf_octant = (
        4 * (leaf_row // block_y % 2) + 2 * (leaf_row % 2) + leaf_row // columns % 2
    )
    lifted = jnp.zeros((leaves, terms), F32)
    for octant in range(8):
        found = apply(own_moments, octant_of(shift_rows, octant))
        lifted = jnp.where(leaf_octant == octant, found, lifted)
    lines = []
    for z in range(block_z // 2):
        both = lifted[2 * z * columns : (2 * z + 1) * columns] + lifted[(2 * z + 1) * columns : (2 * z + 2) * columns]
        for x in range(block_x // 2):
            held = both[x * 8 : x * 8 + 8]
            held = held[:4] + held[4:]
            for y in range(block_y // 2):
                lines.append(held[2 * y : 2 * y + 1] + held[2 * y + 1 : 2 * y + 2])
    spare = jnp.zeros((8, LANES - terms), F32)
    own_slot = mids.at[pl.ds(pl.multiple_of(rank * 8, 8), 8)]
    own_mids = jnp.concatenate([jnp.concatenate(lines, axis=0), spare], axis=1)
    own_slot[...] = own_mids

    mid_copies = []
    for count in range(27):
        moves = (count // 9 - 1, count // 3 % 3 - 1, count % 3 - 1)
        if moves == (0, 0, 0) or any(moves[axis] == -1 and numbers[axis] == 2 for axis in range(3)):
            continue
        target = tuple(
            lax.rem(at[axis] + moves[axis] + numbers[axis], numbers[axis]) for axis in range(3)
        )
        mid_copies.append(
            pltpu.make_async_remote_copy(
                src_ref=own_slot,
                dst_ref=own_slot,
                send_sem=mid_send.at[count],
                recv_sem=mid_receive.at[count],
                device_id=target,
                device_id_type=pl.DeviceIdType.MESH,
            )
        )
    for copy in mid_copies:
        copy.start()
    row_eight = lax.broadcasted_iota(jnp.int32, (8, terms), 0)
    lifted = jnp.zeros((8, terms), F32)
    for octant in range(8):
        line = (octant % 2 * 2 + octant // 4) * 2 + octant // 2 % 2
        found = apply(own_mids, octant_of(shift_rows, octant))
        lifted = jnp.where(row_eight == line, found, lifted)
    own_upper = jnp.concatenate([jnp.sum(lifted, axis=0, keepdims=True), spare[:1]], axis=1)
    upper_slot = arrived.at[rank]
    upper_slot[...] = own_upper

    def upper_copy(step):
        return pltpu.make_async_remote_copy(
            src_ref=upper_slot,
            dst_ref=upper_slot,
            send_sem=upper_send.at[step],
            recv_sem=upper_receive.at[step],
            device_id=other(step),
            device_id_type=pl.DeviceIdType.LOGICAL,
        )

    def send_upper(step, carry):
        upper_copy(step).start()
        return carry

    def wait_upper(step, carry):
        upper_copy(step).wait()
        return carry

    each_other(send_upper)

    strides = (numbers[1] * numbers[2], numbers[2], 1)
    top_sizes = tuple(number // 2 for number in numbers)
    top_strides = (top_sizes[1] * top_sizes[2], top_sizes[2], 1)
    tops = devices // 8
    spots, top_spots = [], []
    for axis in range(3):
        odd = lax.rem(at[axis], 2)
        listed, top_listed = [], []
        for entry in range(7):
            shift = entry - 3
            size = numbers[axis]
            spot = lax.rem(at[axis] + shift + 4 * size, size) * strides[axis]
            if shift == -3:
                spot = jnp.where(odd == 1, spot, 4 * devices)
            if shift == 3:
                spot = jnp.where(odd == 0, spot, 4 * devices)
            listed.append(spot)
            size = top_sizes[axis]
            top_listed.append(
                lax.rem(lax.div(at[axis], 2) + shift + 4 * size, size) * top_strides[axis]
            )
        spots.append(listed)
        top_spots.append(top_listed)
    for x in range(7):
        for y in range(7):
            table[x * 7 + y] = spots[0][x] + spots[1][y]
            table[LANES + x * 7 + y] = top_spots[0][x] + top_spots[1][y]
    for z in range(7):
        table[2 * LANES + z] = spots[2][z]
        table[3 * LANES + z] = top_spots[2][z]
    for line, entry in ((0, 49), (1, 49), (2, 7), (3, 7)):
        table[line * LANES + entry] = jnp.int32(4 * devices)
    staged[7].wait()

    def reach_of(row):
        level, depth = plan_ref[row * PLAN + 2], plan_ref[row * PLAN + 3]
        reach[2 * row] = jnp.minimum(table[level] + table[2 * LANES + depth], devices)
        reach[2 * row + 1] = jnp.minimum(table[LANES + level] + table[3 * LANES + depth], tops) + devices + 1

    staged[4].wait()
    spare_width = far.shape[1] - far_hbm.shape[1]
    far[:, pl.ds(far_hbm.shape[1], spare_width)] = jnp.zeros((terms, spare_width), BF16)
    tall = lax.broadcasted_iota(jnp.int32, (padded_terms, LANES), 1)
    spare_rows = jnp.zeros((padded_terms - terms, LANES), BF16)

    def place(batch, carry):
        for local in range(2 * PLACED):
            triple = batch * (2 * PLACED) + local
            start = triple * (3 * terms)
            turn = start & (LANES - 1)
            base = pl.multiple_of(start - turn, LANES)
            back = (LANES - turn) & (LANES - 1)
            held = far[:, pl.ds(base, 3 * LANES)]
            turned = []
            for tile in range(3):
                piece = held[:, tile * LANES : (tile + 1) * LANES]
                turned.append(pltpu.roll(jnp.concatenate([piece, spare_rows], axis=0), back, 1))
            kept = tall < LANES - turn
            for tile in range(2):
                found = jnp.where(kept, turned[tile], turned[tile + 1])
                spot = (local % 2) * 2 + tile
                operators[
                    batch * PLACED + local // 2, :, spot * LANES : (spot + 1) * LANES
                ] = found
            for kind in range(3):
                reach_of(3 * triple + kind)
        return carry

    used = operators.shape[0]
    batches = used // PLACED
    lax.fori_loop(0, batches // 2, place, 0)
    for copy in along_x:
        copy.wait()
    for copy in relayed:
        copy.start()
    lax.fori_loop(batches // 2, batches, place, 0)
    for row in range(used * 6, triples * 3):
        reach_of(row)

    guard = 8

    def clear(ref):
        ref[:guard, :] = jnp.zeros((guard, LANES), F32)
        ref[ref.shape[0] - guard :, :] = jnp.zeros((guard, LANES), F32)

    clear(wide)
    for kind in range(3):
        for ref in (moments_high, moments_low, mid_high, mid_low):
            clear(ref.at[kind])

    def third(value):
        return (value, pltpu.roll(value, terms, 1), pltpu.roll(value, 2 * terms - LANES, 1))

    def halved(value):
        upper = value.astype(BF16).astype(F32)
        return upper, (value - upper).astype(BF16).astype(F32)

    odd_line = row8 % 2 == 1
    zero8 = jnp.zeros((8, LANES), F32)

    def parity(page, shift):
        if shift == -3:
            return jnp.where(odd_line, page, 0.0)
        if shift == 3:
            return jnp.where(odd_line, 0.0, page)
        return page

    for copy in mid_copies:
        copy.wait()
    mid_x, mid_z = block_x // 2 + 4, block_z // 2 + 4
    around = []
    for count in range(27):
        moves = (count // 9 - 1, count // 3 % 3 - 1, count % 3 - 1)
        there = [lax.rem(at[axis] + moves[axis] + numbers[axis], numbers[axis]) for axis in range(3)]
        around.append(((there[0] * numbers[1] + there[1]) * numbers[2] + there[2]) * 8)
    for z in range(mid_z):
        for x in range(mid_x):
            line = (z % 2 * 2 + x % 2) * 2
            listed = []
            for y in range(3):
                base = around[(x // 2 * 3 + y) * 3 + z // 2]
                listed.append(mids[pl.ds(base + line, 2), :])
            listed.append(jnp.zeros((2, LANES), F32))
            held = jnp.concatenate(listed, axis=0)
            start = guard + (z * mid_x + x) * 8
            for kind, value in enumerate(third(held)):
                upper, lower = halved(value)
                mid_high[kind, start : start + 8, :] = upper
                mid_low[kind, start : start + 8, :] = lower

    def fill_mids(z, carry):
        for shift in range(-3, 4):
            spot = ((shift + 3) * wide_z + z) * starts
            for kind in range(3):
                made = []
                for x in range(mid_x):
                    start = guard + (z * mid_x + x) * 8 + 2 + shift
                    page = jnp.where(
                        row8 < 2,
                        mid_high[kind, pl.ds(start, 8), :],
                        mid_low[kind, pl.ds(start - 2, 8), :],
                    )
                    made.append(parity(page, shift))
                moved = [pltpu.roll(page, 4, 0) for page in made]
                listed = [(x, made[x], moved[x + 1]) for x in range(mid_x - 1)]
                listed += [(7, zero8, moved[0]), (8, made[5], zero8)]
                for entry, low, high in listed:
                    page = jnp.where(row8 < 4, low, high)
                    pages[3 + kind, spot + entry] = jnp.concatenate([page, page], axis=0).astype(BF16)
        return carry

    lax.fori_loop(0, mid_z, fill_mids, 0)

    each_other(wait_upper)
    raised = arrived[:, 0, :]
    rank_row = lax.broadcasted_iota(jnp.int32, (devices, terms), 0)
    rank_octant = (
        4 * (rank_row // strides[0] % 2) + 2 * (rank_row // strides[1] % 2) + rank_row % 2
    )
    lifted = jnp.zeros((devices, terms), F32)
    for octant in range(8):
        found = apply(raised, octant_of(shift_rows, octant))
        lifted = jnp.where(rank_octant == octant, found, lifted)
    root = jnp.sum(lifted, axis=0, keepdims=True)
    top_rows = (tops + 7) // 8 * 8
    picker_row = lax.broadcasted_iota(jnp.int32, (top_rows, devices), 0)
    picker_rank = lax.broadcasted_iota(jnp.int32, (top_rows, devices), 1)
    parent_of = (
        picker_rank // strides[0] // 2 * top_strides[0]
        + picker_rank // strides[1] % numbers[1] // 2 * top_strides[1]
        + picker_rank % numbers[2] // 2
    )
    picker = (picker_row == parent_of).astype(F32)
    merged = lax.dot_general(
        picker, lifted, NN, precision=lax.Precision.HIGHEST, preferred_element_type=F32
    )
    merged = jnp.concatenate([merged, jnp.zeros((top_rows, LANES - terms), F32)], axis=1)
    for kind, value in enumerate(third(jnp.concatenate([raised, merged], axis=0))):
        upper, lower = halved(value)
        uppers[2 * kind] = upper
        uppers[2 * kind + 1] = lower

    def fill_uppers(line):
        def fill(entry, carry):
            for kind in range(3):
                high = jnp.broadcast_to(uppers[2 * kind, pl.ds(line[1] + entry, 1), :], (8, LANES))
                low = jnp.broadcast_to(uppers[2 * kind + 1, pl.ds(line[1] + entry, 1), :], (8, LANES))
                page = jnp.where(row8 == line[0], high, jnp.where(row8 == line[0] + 1, low, 0.0))
                upper_pages[kind, line[2] + entry] = jnp.concatenate([page, zero8], axis=0).astype(BF16)
            return carry

        return fill

    lax.fori_loop(0, devices, fill_uppers((0, 0, 0)), 0, unroll=8)
    lax.fori_loop(0, tops, fill_uppers((2, devices, devices + 1)), 0, unroll=4)
    for kind in range(3):
        upper_pages[kind, devices] = jnp.zeros((16, LANES), BF16)
        upper_pages[kind, devices + 1 + tops] = jnp.zeros((16, LANES), BF16)

    for copy in beside + relayed:
        copy.wait()
    def widen(z, carry):
        for x in range(wide_x):
            column = jnp.concatenate([raw[pair, z, x] for pair in range(pairs + 2)], axis=0)
            wide[pl.ds(pl.multiple_of(guard + (z * wide_x + x) * rows_y, 8), rows_y), :] = column
        return carry

    lax.fori_loop(0, wide_z, widen, 0)

    def window(tile, carry):
        start = pl.multiple_of(guard + tile * LANES, 8)
        turned = wide[pl.ds(start, LANES), :].T
        found = moments(
            turned[:SLOTS], turned[SLOTS : 2 * SLOTS], turned[2 * SLOTS : 3 * SLOTS], turned[3 * SLOTS :]
        )
        for kind, value in enumerate(third(found)):
            upper, lower = halved(value)
            moments_high[kind, pl.ds(start, LANES), :] = upper
            moments_low[kind, pl.ds(start, LANES), :] = lower
        return carry

    lax.fori_loop(0, wide_x * wide_z * rows_y // LANES, window, 0, unroll=4)

    near_shifts = [(x, y, z) for x in (-1, 0, 1) for y in (-1, 0, 1) for z in (-1, 0, 1)]
    lane8 = lax.broadcasted_iota(jnp.int32, (8, LANES), 1)
    group8 = lane8 // SLOTS

    def shifted(shift):
        moved = jnp.where(
            group8 == 0,
            float(shift[0]),
            jnp.where(group8 == 1, float(shift[1]), jnp.where(group8 == 2, float(shift[2]), 0.0)),
        )
        found = []
        for z in range(block_z):
            for x in range(0, block_x, 2):
                spot = (z + HALO + shift[2]) * wide_x + x + HALO + shift[0]
                low = guard + spot * rows_y + HALO + shift[1]
                high = low + rows_y - block_y
                held = jnp.where(row8 < block_y, wide[low : low + 8, :], wide[high : high + 8, :])
                found.append(held + moved)
        return found

    for pair in range((len(near_shifts) + 1) // 2):
        first = shifted(near_shifts[2 * pair])
        if 2 * pair + 1 < len(near_shifts):
            second = shifted(near_shifts[2 * pair + 1])
        else:
            second = [jnp.where(group8 < 3, value, 0.0) for value in first]
        sources[pair * LANES : (pair + 1) * LANES, :] = jnp.concatenate(first + second, axis=0).T

    def fill_pages(z, carry):
        for shift in range(-3, 4):
            spot = ((shift + 3) * wide_z + z) * starts
            for kind in range(3):
                made = []
                for x in range(wide_x):
                    start = guard + (z * wide_x + x) * rows_y + HALO + shift
                    page = jnp.where(
                        row8 < block_y,
                        moments_high[kind, pl.ds(start, 8), :],
                        moments_low[kind, pl.ds(start - block_y, 8), :],
                    )
                    made.append(parity(page, shift))
                listed = [(x, made[x], made[x + 1]) for x in range(wide_x - 1)]
                listed += [(7, zero8, made[0]), (9, zero8, made[2])]
                listed += [(8, made[5], zero8), (10, made[7], zero8)]
                for entry, low, high in listed:
                    pages[kind, spot + entry] = jnp.concatenate([low, high], axis=0).astype(BF16)
        return carry

    lax.fori_loop(0, wide_z, fill_pages, 0)
    for kind in range(6):
        for entry in range(pages.shape[1] - none):
            pages[kind, none + entry] = jnp.zeros((16, LANES), BF16)

    lane16 = lax.broadcasted_iota(jnp.int32, (16, LANES), 1)
    first_part = lane16 < terms
    second_part = lane16 < 2 * terms - LANES

    first_eight = lax.broadcasted_iota(jnp.int32, (16, LANES), 0) < 8

    def far_rows(triple):
        rows = [3 * triple + kind for kind in range(3)]
        spots = [[plan_ref[row * PLAN + odd] for odd in range(2)] for row in rows]

        def tiles(held):
            return jnp.concatenate(
                [
                    jnp.where(first_part, held[0], held[1]),
                    jnp.where(second_part, held[1], held[2]),
                ],
                axis=1,
            )

        found = []
        for z in range(block_z):
            for x in range(block_x // 2):
                step = z // 2 * 2 * starts + 2 * x
                found.append(tiles([pages[kind, spots[kind][z % 2] + step] for kind in range(3)]))
        held = []
        for kind in range(3):
            even, odd = pages[3 + kind, spots[kind][0]], pages[3 + kind, spots[kind][1]]
            held.append(jnp.where(first_eight, even, odd))
        found.append(tiles(held))
        held = []
        for kind, row in enumerate(rows):
            held.append(upper_pages[kind, reach[2 * row]] + upper_pages[kind, reach[2 * row + 1]])
        found.append(tiles(held))
        return jnp.concatenate(found, axis=0)

    total_rows = 2 * leaves + 32
    sums[...] = jnp.zeros(sums.shape, F32)
    near_steps = sources.shape[0] // LANES // 2

    def near_step(step, totals):
        sum_p, sum_x, sum_y, sum_z = totals
        for row in range(2 * SLOTS):
            base = step * (2 * LANES) + row // SLOTS * LANES
            line = row % SLOTS
            s_x = sources[pl.ds(base + line, 1), :]
            s_y = sources[pl.ds(base + line + SLOTS, 1), :]
            s_z = sources[pl.ds(base + line + 2 * SLOTS, 1), :]
            s_q = sources[pl.ds(base + line + 3 * SLOTS, 1), :]
            d_x = targets[:SLOTS] - s_x
            d_y = targets[SLOTS : 2 * SLOTS] - s_y
            d_z = targets[2 * SLOTS : 3 * SLOTS] - s_z
            inverse = lax.rsqrt(d_x * d_x + d_y * d_y + d_z * d_z + SOFTENING)
            weight = s_q * inverse
            sum_p = sum_p + weight
            cubic = weight * (inverse * inverse)
            sum_x = sum_x + cubic * d_x
            sum_y = sum_y + cubic * d_y
            sum_z = sum_z + cubic * d_z
        return sum_p, sum_x, sum_y, sum_z

    def far_step(step, carry):
        added = []
        for which in range(14):
            pair = step * 14 + which
            left = jnp.concatenate([far_rows(2 * pair), far_rows(2 * pair + 1)], axis=1)
            added.append(lax.dot_general(left, operators[jnp.minimum(pair, used - 1)], NT, preferred_element_type=F32))
        total = added[0]
        for value in added[1:]:
            total = total + value
        sums[...] += total
        return carry

    lax.fori_loop(0, STEPS * GROUP // 28, far_step, 0)
    zero = jnp.zeros((SLOTS, LANES), F32)
    near = lax.fori_loop(0, near_steps, near_step, (zero, zero, zero, zero))

    staged[5].wait()
    staged[6].wait()
    rows_from(down_raw, down_rows)
    first = 2 * leaves + 16
    held = sums[first : first + 8, :terms]
    far_upper = held[0:1] + held[1:2]
    far_top = held[2:3] + held[3:4]

    def lattice_apply(value):
        return apply(jnp.broadcast_to(value, (8, terms)), lattice[...])

    def wider(value):
        return jnp.concatenate([value, jnp.zeros((value.shape[0], LANES - terms), F32)], axis=1)

    top_local = 0.125 * (far_top + lattice_apply(root)[:1])
    octant = lax.rem(at[0], 2) * 4 + lax.rem(at[1], 2) * 2 + lax.rem(at[2], 2)
    moved = apply(jnp.broadcast_to(wider(top_local), (8, LANES)), octant_of(down_rows, octant))
    upper_local = jnp.broadcast_to(wider(0.25 * far_upper + moved[:1]), (8, LANES))
    mid_row = lax.broadcasted_iota(jnp.int32, (8, terms), 0)
    mid_octant = 4 * (mid_row // 2 % 2) + 2 * (mid_row % 2) + mid_row // 4
    held = sums[2 * leaves : 2 * leaves + 16, :terms]
    lines = []
    for z in range(2):
        for x in range(2):
            start = z * 8 + x * 4
            lines.append(held[start : start + 2] + held[start + 2 : start + 4])
    far_mid = jnp.concatenate(lines, axis=0)
    downward = [octant_of(down_rows, entry) for entry in range(8)]
    moved = jnp.zeros((8, terms), F32)
    for entry in range(8):
        moved = jnp.where(mid_octant == entry, apply(upper_local, downward[entry]), moved)
    mid_local = wider(0.5 * far_mid + moved)
    expanded = []
    for z in range(block_z):
        for x in range(block_x // 2):
            line = (z // 2 * 2 + x) * 2
            low = jnp.broadcast_to(mid_local[line : line + 1], (8, LANES))
            high = jnp.broadcast_to(mid_local[line + 1 : line + 2], (8, LANES))
            expanded.append(jnp.where(row8 % 4 < 2, low, high))
    expanded = jnp.concatenate(expanded, axis=0)
    moved = jnp.zeros((leaves, terms), F32)
    for entry in range(8):
        moved = jnp.where(leaf_octant == entry, apply(expanded, downward[entry]), moved)
    row_t = lax.broadcasted_iota(jnp.int32, (8, terms), 0)
    lines = []
    for spot in range(leaves // 8):
        low = sums[spot * 16 : spot * 16 + 8, :terms]
        high = sums[spot * 16 + 8 : spot * 16 + 16, :terms]
        low = low + pltpu.roll(low, 4, 0)
        high = high + pltpu.roll(high, 4, 0)
        lines.append(jnp.where(row_t < 4, low, high))
    local = wider(moved + jnp.concatenate(lines, axis=0))
    local_rows[...] = jnp.concatenate([local, local], axis=0).T

    u_x = targets[:SLOTS] - 0.5
    u_y = targets[SLOTS : 2 * SLOTS] - 0.5
    u_z = targets[2 * SLOTS : 3 * SLOTS] - 0.5
    value = grad_x = grad_y = grad_z = None
    for a in range(ORDER, -1, -1):
        inner = inner_y = inner_z = None
        for b in range(ORDER - a, -1, -1):
            here = local_rows[ROW_OF[(a, b, 0)] : ROW_OF[(a, b, 0)] + 1, :]
            if (a, b, 1) in ROW_OF:
                above = local_rows[ROW_OF[(a, b, 1)] : ROW_OF[(a, b, 1)] + 1, :]
                both = here + above * u_z
                inner_z = above if inner_z is None else inner_z * u_y + above
            else:
                both = here
            if inner is None:
                inner = jnp.broadcast_to(both, (SLOTS, LANES))
            else:
                inner_y = inner if inner_y is None else inner_y * u_y + inner
                inner = inner * u_y + both
        if value is None:
            value, grad_y, grad_z = inner, inner_y, inner_z
        else:
            grad_x = value if grad_x is None else grad_x * u_x + value
            value = value * u_x + inner
            if inner_y is not None:
                grad_y = inner_y if grad_y is None else grad_y * u_x + inner_y
            if inner_z is not None:
                grad_z = inner_z if grad_z is None else grad_z * u_x + inner_z

    def halves(total):
        return total + pltpu.roll(total, leaves, 1)

    self_term = targets[3 * SLOTS :] * (SOFTENING**-0.5)
    results = [
        halves(near[0]) - self_term + value,
        halves(near[1]) - grad_x,
        halves(near[2]) - grad_y,
        halves(near[3]) - grad_z,
    ]
    turned = jnp.concatenate(results, axis=0).T
    for entry in range(4):
        made = None
        for z in range(block_z):
            turn = (z - entry) * SLOTS % LANES
            held = turned[z * columns : (z + 1) * columns]
            held = pltpu.roll(held, turn, 1) if turn else held
            made = held if made is None else jnp.where(group == z, held, made)
        made = made * live
        for x in range(block_x):
            piece = made[x * block_y : (x + 1) * block_y]
            result_ref[entry, x] = piece


def part_kernel(result_ref, potential_ref, field_ref, sems):
    copies = [
        pltpu.make_async_copy(result_ref.at[0], potential_ref, sems.at[0]),
        pltpu.make_async_copy(result_ref.at[pl.ds(1, 3)], field_ref, sems.at[1]),
    ]
    for copy in copies:
        copy.start()
    for copy in copies:
        copy.wait()


def per_device(
    positions, charges, counts, moment_shift, far_operators, local_shift, lattice_operator
):
    block_x, block_y, column = charges.shape
    block_z = column // SLOTS
    sizes = (block_x, block_y, block_z)
    numbers = tuple(lax.axis_size(axis) for axis in ("gx", "gy", "gz"))
    devices = numbers[0] * numbers[1] * numbers[2]
    terms = moment_shift.shape[1]
    padded_terms = (terms + 15) // 16 * 16
    leaves = block_x * block_y * block_z
    plan, triples, none, starts = plan_table(block_x, block_z)
    offsets = offset_table().shape[0]
    wide_x, wide_z = block_x + 2 * HALO, block_z + 2 * HALO
    wide_leaves = wide_x * wide_z * (block_y + 2 * HALO)
    mid_columns = (block_x // 2 + 4) * (block_z // 2 + 4)
    tops = devices // 8
    anywhere = pl.BlockSpec(memory_space=pltpu.HBM)
    vmem = pl.BlockSpec(memory_space=pltpu.VMEM)
    layout = (triples, none, starts)
    batches = -(-offsets // (6 * PLACED))
    top_rows = (tops + 7) // 8 * 8
    placed = batches * PLACED
    spare = (placed * 6 * terms + 2 * LANES - far_operators.shape[1] + LANES) // LANES * LANES
    result = pl.pallas_call(
        lambda *refs: field_kernel(sizes, numbers, layout, *refs),
        out_shape=pltpu.VMEM((4, block_x, block_y, column), F32),
        in_specs=[anywhere] * 8,
        out_specs=vmem,
        scratch_shapes=[
            pltpu.VMEM(positions.shape, F32),
            pltpu.VMEM(charges.shape, F32),
            pltpu.VMEM(counts.shape, jnp.int32),
            pltpu.VMEM((terms, 8, terms), BF16),
            pltpu.VMEM((terms, far_operators.shape[1] + spare), BF16),
            pltpu.VMEM((terms, 8, terms), BF16),
            pltpu.VMEM((terms, terms), BF16),
            pltpu.VMEM((block_y // 2 + 2, wide_z, wide_x, 2, LANES), F32),
            pltpu.VMEM((wide_leaves + 16, LANES), F32),
            pltpu.VMEM((4 * SLOTS, LANES), F32),
            pltpu.VMEM((padded_terms * 8, LANES), F32),
            pltpu.VMEM((3, wide_leaves + 16, LANES), F32),
            pltpu.VMEM((3, wide_leaves + 16, LANES), F32),
            pltpu.VMEM((devices * 8, LANES), F32),
            pltpu.VMEM((terms * 8, LANES), F32),
            pltpu.VMEM((terms * 8, LANES), F32),
            pltpu.VMEM((6, devices + top_rows, LANES), F32),
            pltpu.VMEM((placed, padded_terms, 4 * LANES), BF16),
            pltpu.VMEM((14 * LANES, LANES), F32),
            pltpu.VMEM((6, none + 2 * starts + 3, 16, LANES), BF16),
            pltpu.VMEM((3, mid_columns * 8 + 16, LANES), F32),
            pltpu.VMEM((3, mid_columns * 8 + 16, LANES), F32),
            pltpu.VMEM((3, devices + tops + 2, 16, LANES), BF16),
            pltpu.VMEM((2 * leaves + 32, padded_terms), F32),
            pltpu.VMEM((LANES, LANES), F32),
            pltpu.SMEM(plan.shape, jnp.int32),
            pltpu.SMEM((4 * LANES,), jnp.int32),
            pltpu.SMEM((triples * 6,), jnp.int32),
            pltpu.SemaphoreType.DMA((8,)),
            pltpu.SemaphoreType.DMA((27,)),
            pltpu.SemaphoreType.DMA((27,)),
            pltpu.SemaphoreType.DMA((27,)),
            pltpu.SemaphoreType.DMA((27,)),
            pltpu.VMEM((devices, 1, LANES), F32),
            pltpu.SemaphoreType.DMA((devices,)),
            pltpu.SemaphoreType.DMA((devices,)),
        ],
        compiler_params=pltpu.CompilerParams(
            vmem_limit_bytes=60 * 1024 * 1024, collective_id=0, has_side_effects=True
        ),
        name="fields",
    )(
        jnp.asarray(plan),
        positions,
        charges,
        counts,
        jnp.transpose(moment_shift, (1, 0, 2)),
        far_operators,
        jnp.transpose(local_shift, (1, 0, 2)),
        lattice_operator,
    )
    return pl.pallas_call(
        part_kernel,
        out_shape=(
            jax.ShapeDtypeStruct((block_x, block_y, column), F32),
            jax.ShapeDtypeStruct((3, block_x, block_y, column), F32),
        ),
        in_specs=[vmem],
        out_specs=(anywhere, anywhere),
        scratch_shapes=[pltpu.SemaphoreType.DMA((2,))],
        compiler_params=pltpu.CompilerParams(vmem_limit_bytes=4 * 1024 * 1024),
        name="part",
    )(result)


def solution(mesh):
    placed = (
        P(None, "gx", "gy", "gz"),
        P("gx", "gy", "gz"),
        P("gx", "gy", "gz"),
        P(),
        P(),
        P(),
        P(),
    )
    return jax.shard_map(
        per_device,
        mesh=mesh,
        in_specs=placed,
        out_specs=(P("gx", "gy", "gz"), P(None, "gx", "gy", "gz")),
        check_vma=False,
    )
```

```python
import jax
import jax.numpy as jnp
import numpy as np
from jax import lax
from jax.experimental import pallas as pl
from jax.experimental.pallas import tpu as pltpu
from jax.sharding import PartitionSpec as P

ORDER = 8
SLOTS = 32
SOFTENING = 0.0625
LANES = 128
HALO = 2
F32 = jnp.float32
BF16 = jnp.bfloat16
NT = (((1,), (1,)), ((), ()))
NN = (((1,), (0,)), ((), ()))
PLAN = 4
GROUP = 4
STEPS = 28
PLACED = 9


def offset_table():
    listed = []
    for shift_x in range(-3, 4):
        for shift_y in range(-3, 4):
            for shift_z in range(-3, 4):
                if max(abs(shift_x), abs(shift_y), abs(shift_z)) >= 2:
                    listed.append((shift_x, shift_y, shift_z))
    return np.array(listed, dtype=np.int32)


def exponent_table(degree):
    listed = []
    for accumulated in range(degree + 1):
        for height in (0, 1):
            for power_x in range(accumulated - height + 1):
                listed.append((power_x, accumulated - height - power_x, height))
    return np.array(listed, dtype=np.int32)


ROW_OF = {tuple(int(v) for v in key): row for row, key in enumerate(exponent_table(ORDER))}


def split_rows(data):
    upper = data.astype(BF16)
    lower = (data - upper.astype(F32)).astype(BF16)
    return upper, lower


def apply(data, operator):
    upper, lower = split_rows(data)
    rows = data.shape[0]
    both = jnp.concatenate([upper.astype(F32), lower.astype(F32)], axis=0).astype(BF16)
    found = lax.dot_general(both, operator, NT, preferred_element_type=F32)
    return found[:rows] + found[rows:]


def powers_of(values):
    listed = [jnp.ones_like(values)]
    for exponent in range(ORDER):
        listed.append(listed[-1] * values)
    return listed


def admits(shift, odd):
    return -2 - odd <= shift <= 3 - odd


def leaf_start(shift):
    return {-3: 7, 3: 8}.get(shift, shift + 2)


def plan_table(block_x, block_z):
    shifts = offset_table()
    wide_x, wide_z = block_x + 2 * HALO, block_z + 2 * HALO
    starts = wide_x + 3
    triples = STEPS * GROUP
    assert 3 * triples >= shifts.shape[0]
    plan = np.zeros((triples * 3, PLAN), np.int32)
    none = 7 * wide_z * starts
    plan[:, :2] = none
    plan[:, 2] = 49
    plan[:, 3] = 7
    for row, (dx, dy, dz) in enumerate(shifts):
        for z in range(2):
            if admits(dz, z):
                plan[row, z] = ((dy + 3) * wide_z + z + 2 + dz) * starts + leaf_start(dx)
        plan[row, 2] = (dx + 3) * 7 + dy + 3
        plan[row, 3] = dz + 3
    return plan.reshape(-1), triples, none, starts


def field_kernel(
    sizes,
    numbers,
    layout,
    plan_hbm,
    positions_hbm,
    charges_hbm,
    counts_hbm,
    shift_hbm,
    far_hbm,
    down_hbm,
    lattice_hbm,
    result_ref,
    positions,
    charges,
    counts,
    shift_raw,
    far,
    down_raw,
    lattice,
    raw,
    wide,
    targets,
    partial,
    moments_high,
    moments_low,
    mids,
    shift_rows,
    down_rows,
    uppers,
    operators,
    sources,
    pages,
    mid_high,
    mid_low,
    upper_pages,
    sums,
    local_rows,
    plan_ref,
    table,
    reach,
    loads,
    sends,
    receives,
    mid_send,
    mid_receive,
    arrived,
    upper_send,
    upper_receive,
):
    block_x, block_y, block_z = sizes
    triples, none, starts = layout
    wide_x, wide_z = block_x + 2 * HALO, block_z + 2 * HALO
    rows_y = block_y + 2 * HALO
    columns = block_x * block_y
    leaves = columns * block_z
    terms = lattice.shape[0]
    padded_terms = operators.shape[1]
    offsets = offset_table().shape[0]
    at = tuple(lax.axis_index(axis) for axis in ("gx", "gy", "gz"))
    devices = numbers[0] * numbers[1] * numbers[2]
    rank = (at[0] * numbers[1] + at[1]) * numbers[2] + at[2]
    barrier = pltpu.get_barrier_semaphore()

    def other(step):
        if devices & (devices - 1) == 0:
            return (rank + step) & (devices - 1)
        return lax.rem(rank + step, devices)

    def each_other(action):
        if devices <= 64:
            for step in range(1, devices):
                action(step, 0)
        else:
            lax.fori_loop(1, devices, action, 0)

    staged = [
        pltpu.make_async_copy(positions_hbm, positions, loads.at[0]),
        pltpu.make_async_copy(charges_hbm, charges, loads.at[1]),
        pltpu.make_async_copy(counts_hbm, counts, loads.at[2]),
        pltpu.make_async_copy(shift_hbm, shift_raw, loads.at[3]),
        pltpu.make_async_copy(far_hbm, far.at[:, pl.ds(0, far_hbm.shape[1])], loads.at[4]),
        pltpu.make_async_copy(down_hbm, down_raw, loads.at[5]),
        pltpu.make_async_copy(lattice_hbm, lattice, loads.at[6]),
        pltpu.make_async_copy(plan_hbm, plan_ref, loads.at[7]),
    ]
    for copy in staged:
        copy.start()

    def greet(step, carry):
        pl.semaphore_signal(
            barrier, inc=1, device_id=other(step), device_id_type=pl.DeviceIdType.LOGICAL
        )
        return carry

    each_other(greet)

    lane = lax.broadcasted_iota(jnp.int32, (columns, LANES), 1)
    group = lane // SLOTS
    row8 = lax.broadcasted_iota(jnp.int32, (8, LANES), 0)
    for copy in staged[:3]:
        copy.wait()
    held = jnp.concatenate([counts[x] for x in range(block_x)], axis=0)
    limit = jnp.broadcast_to(held[:, 0:1], (columns, LANES))
    for z in range(1, block_z):
        limit = jnp.where(group == z, jnp.broadcast_to(held[:, z : z + 1], (columns, LANES)), limit)
    live = (lane % SLOTS < limit).astype(F32)
    parts = [
        jnp.concatenate([positions[c, x] for x in range(block_x)], axis=0) for c in range(3)
    ]
    parts.append(jnp.concatenate([charges[x] for x in range(block_x)], axis=0) * live)
    pieces = []
    for z in range(block_z):
        made = None
        for c in range(4):
            turn = (c - z) * SLOTS % LANES
            moved = pltpu.roll(parts[c], turn, 1) if turn else parts[c]
            made = moved if made is None else jnp.where(group == c, moved, made)
        pieces.append(made)
        for x in range(block_x):
            for pair in range(block_y // 2):
                start = x * block_y + 2 * pair
                raw[1 + pair, HALO + z, HALO + x] = made[start : start + 2]
    own = jnp.concatenate(pieces + pieces, axis=0)
    targets[...] = own.T

    pl.semaphore_wait(barrier, devices - 1)
    pairs = block_y // 2

    def span(move, size, halo):
        if move == 1:
            return pl.ds(size, halo), pl.ds(0, halo)
        if move == -1:
            return pl.ds(halo, halo), pl.ds(size + halo, halo)
        return pl.ds(halo, size), pl.ds(halo, size)

    direct, relayed = [], []
    for count in range(27):
        moves = (count // 9 - 1, count // 3 % 3 - 1, count % 3 - 1)
        if moves == (0, 0, 0):
            continue
        from_x, to_x = span(moves[0], block_x, HALO)
        from_y, to_y = span(moves[1], pairs, 1)
        from_z, to_z = span(moves[2], block_z, HALO)
        relay = moves[0] != 0 and moves[1:] != (0, 0)
        steps = (0 if relay else moves[0],) + moves[1:]
        target = tuple(
            lax.rem(at[axis] + steps[axis] + numbers[axis], numbers[axis]) for axis in range(3)
        )
        copy = pltpu.make_async_remote_copy(
            src_ref=raw.at[from_y, from_z, to_x if relay else from_x],
            dst_ref=raw.at[to_y, to_z, to_x],
            send_sem=sends.at[count],
            recv_sem=receives.at[count],
            device_id=target,
            device_id_type=pl.DeviceIdType.MESH,
        )
        (relayed if relay else direct).append((moves, copy))
    direct.sort(key=lambda held: held[0][2] == 0)
    relayed.sort(key=lambda held: held[0][2] == 0)
    along_x = [copy for moves, copy in direct if moves[0] != 0]
    beside = [copy for moves, copy in direct if moves[0] == 0]
    relayed = [copy for moves, copy in relayed]
    for copy in along_x + beside:
        copy.start()

    partial[pl.ds(terms * 8, partial.shape[0] - terms * 8), :] = jnp.zeros(
        (partial.shape[0] - terms * 8, LANES), F32
    )

    def moments(at_x, at_y, at_z, charge):
        quarter = SLOTS // 8
        centred_z = at_z - 0.5
        centred_y = at_y - 0.5
        powers_x = [value * charge for value in powers_of(at_x - 0.5)]
        power_y = None
        for b in range(ORDER + 1):
            power_y = None if b == 0 else (centred_y if b == 1 else power_y * centred_y)
            for a in range(ORDER + 1 - b):
                flat = powers_x[a] if b == 0 else powers_x[a] * power_y
                for height in (0, 1):
                    if a + b + height > ORDER:
                        continue
                    made = flat * centred_z if height else flat
                    total = made[:8]
                    for piece in range(1, quarter):
                        total = total + made[piece * 8 : piece * 8 + 8]
                    row = ROW_OF[(a, b, height)]
                    partial[row * 8 : row * 8 + 8, :] = total
        found = partial[pl.ds(0, padded_terms, stride=8), :]
        for line in range(1, 8):
            found = found + partial[pl.ds(line, padded_terms, stride=8), :]
        found = jnp.concatenate([found, jnp.zeros((LANES - padded_terms, LANES), F32)], axis=0)
        return found.T

    def rows_from(raw_ref, out_ref):
        out_ref[...] = jnp.zeros(out_ref.shape, F32)
        out_ref[:, :terms] = raw_ref[...].astype(F32).reshape(terms * 8, terms)

    def octant_of(ref, octant):
        return ref[pl.ds(octant, terms, stride=8), :].astype(BF16)

    own_moments = moments(
        targets[:SLOTS], targets[SLOTS : 2 * SLOTS], targets[2 * SLOTS : 3 * SLOTS], targets[3 * SLOTS :]
    )[:leaves]
    staged[3].wait()
    rows_from(shift_raw, shift_rows)
    leaf_row = lax.broadcasted_iota(jnp.int32, (leaves, terms), 0)
    leaf_octant = (
        4 * (leaf_row // block_y % 2) + 2 * (leaf_row % 2) + leaf_row // columns % 2
    )
    lifted = jnp.zeros((leaves, terms), F32)
    for octant in range(8):
        found = apply(own_moments, octant_of(shift_rows, octant))
        lifted = jnp.where(leaf_octant == octant, found, lifted)
    lines = []
    for z in range(block_z // 2):
        both = lifted[2 * z * columns : (2 * z + 1) * columns] + lifted[(2 * z + 1) * columns : (2 * z + 2) * columns]
        for x in range(block_x // 2):
            held = both[x * 8 : x * 8 + 8]
            held = held[:4] + held[4:]
            for y in range(block_y // 2):
                lines.append(held[2 * y : 2 * y + 1] + held[2 * y + 1 : 2 * y + 2])
    spare = jnp.zeros((8, LANES - terms), F32)
    own_slot = mids.at[pl.ds(pl.multiple_of(rank * 8, 8), 8)]
    own_mids = jnp.concatenate([jnp.concatenate(lines, axis=0), spare], axis=1)
    own_slot[...] = own_mids

    mid_copies = []
    for count in range(27):
        moves = (count // 9 - 1, count // 3 % 3 - 1, count % 3 - 1)
        if moves == (0, 0, 0) or any(moves[axis] == -1 and numbers[axis] == 2 for axis in range(3)):
            continue
        target = tuple(
            lax.rem(at[axis] + moves[axis] + numbers[axis], numbers[axis]) for axis in range(3)
        )
        mid_copies.append(
            pltpu.make_async_remote_copy(
                src_ref=own_slot,
                dst_ref=own_slot,
                send_sem=mid_send.at[count],
                recv_sem=mid_receive.at[count],
                device_id=target,
                device_id_type=pl.DeviceIdType.MESH,
            )
        )
    for copy in mid_copies:
        copy.start()
    row_eight = lax.broadcasted_iota(jnp.int32, (8, terms), 0)
    lifted = jnp.zeros((8, terms), F32)
    for octant in range(8):
        line = (octant % 2 * 2 + octant // 4) * 2 + octant // 2 % 2
        found = apply(own_mids, octant_of(shift_rows, octant))
        lifted = jnp.where(row_eight == line, found, lifted)
    own_upper = jnp.concatenate([jnp.sum(lifted, axis=0, keepdims=True), spare[:1]], axis=1)
    upper_slot = arrived.at[rank]
    upper_slot[...] = own_upper

    def upper_copy(step):
        return pltpu.make_async_remote_copy(
            src_ref=upper_slot,
            dst_ref=upper_slot,
            send_sem=upper_send.at[step],
            recv_sem=upper_receive.at[step],
            device_id=other(step),
            device_id_type=pl.DeviceIdType.LOGICAL,
        )

    def send_upper(step, carry):
        upper_copy(step).start()
        return carry

    def wait_upper(step, carry):
        upper_copy(step).wait()
        return carry

    each_other(send_upper)

    strides = (numbers[1] * numbers[2], numbers[2], 1)
    top_sizes = tuple(number // 2 for number in numbers)
    top_strides = (top_sizes[1] * top_sizes[2], top_sizes[2], 1)
    tops = devices // 8
    spots, top_spots = [], []
    for axis in range(3):
        odd = lax.rem(at[axis], 2)
        listed, top_listed = [], []
        for entry in range(7):
            shift = entry - 3
            size = numbers[axis]
            spot = lax.rem(at[axis] + shift + 4 * size, size) * strides[axis]
            if shift == -3:
                spot = jnp.where(odd == 1, spot, 4 * devices)
            if shift == 3:
                spot = jnp.where(odd == 0, spot, 4 * devices)
            listed.append(spot)
            size = top_sizes[axis]
            top_listed.append(
                lax.rem(lax.div(at[axis], 2) + shift + 4 * size, size) * top_strides[axis]
            )
        spots.append(listed)
        top_spots.append(top_listed)
    for x in range(7):
        for y in range(7):
            table[x * 7 + y] = spots[0][x] + spots[1][y]
            table[LANES + x * 7 + y] = top_spots[0][x] + top_spots[1][y]
    for z in range(7):
        table[2 * LANES + z] = spots[2][z]
        table[3 * LANES + z] = top_spots[2][z]
    for line, entry in ((0, 49), (1, 49), (2, 7), (3, 7)):
        table[line * LANES + entry] = jnp.int32(4 * devices)
    staged[7].wait()

    def reach_of(row):
        level, depth = plan_ref[row * PLAN + 2], plan_ref[row * PLAN + 3]
        reach[2 * row] = jnp.minimum(table[level] + table[2 * LANES + depth], devices)
        reach[2 * row + 1] = jnp.minimum(table[LANES + level] + table[3 * LANES + depth], tops) + devices + 1

    staged[4].wait()
    spare_width = far.shape[1] - far_hbm.shape[1]
    far[:, pl.ds(far_hbm.shape[1], spare_width)] = jnp.zeros((terms, spare_width), BF16)
    tall = lax.broadcasted_iota(jnp.int32, (padded_terms, LANES), 1)
    spare_rows = jnp.zeros((padded_terms - terms, LANES), BF16)

    def place(batch, carry):
        for local in range(2 * PLACED):
            triple = batch * (2 * PLACED) + local
            start = triple * (3 * terms)
            turn = start & (LANES - 1)
            base = pl.multiple_of(start - turn, LANES)
            back = (LANES - turn) & (LANES - 1)
            held = far[:, pl.ds(base, 3 * LANES)]
            turned = []
            for tile in range(3):
                piece = held[:, tile * LANES : (tile + 1) * LANES]
                turned.append(pltpu.roll(jnp.concatenate([piece, spare_rows], axis=0), back, 1))
            kept = tall < LANES - turn
            for tile in range(2):
                found = jnp.where(kept, turned[tile], turned[tile + 1])
                spot = (local % 2) * 2 + tile
                operators[
                    batch * PLACED + local // 2, :, spot * LANES : (spot + 1) * LANES
                ] = found
            for kind in range(3):
                reach_of(3 * triple + kind)
        return carry

    used = operators.shape[0]
    batches = used // PLACED
    lax.fori_loop(0, batches // 2, place, 0)
    for copy in along_x:
        copy.wait()
    for copy in relayed:
        copy.start()
    lax.fori_loop(batches // 2, batches, place, 0)
    for row in range(used * 6, triples * 3):
        reach_of(row)

    guard = 8

    def clear(ref):
        ref[:guard, :] = jnp.zeros((guard, LANES), F32)
        ref[ref.shape[0] - guard :, :] = jnp.zeros((guard, LANES), F32)

    clear(wide)
    for kind in range(3):
        for ref in (moments_high, moments_low, mid_high, mid_low):
            clear(ref.at[kind])

    def third(value):
        return (value, pltpu.roll(value, terms, 1), pltpu.roll(value, 2 * terms - LANES, 1))

    def halved(value):
        upper = value.astype(BF16).astype(F32)
        return upper, (value - upper).astype(BF16).astype(F32)

    odd_line = row8 % 2 == 1
    zero8 = jnp.zeros((8, LANES), F32)

    def parity(page, shift):
        if shift == -3:
            return jnp.where(odd_line, page, 0.0)
        if shift == 3:
            return jnp.where(odd_line, 0.0, page)
        return page

    for kind in range(6):
        for entry in range(pages.shape[1] - none):
            pages[kind, none + entry] = jnp.zeros((16, LANES), BF16)
    staged[5].wait()
    staged[6].wait()
    rows_from(down_raw, down_rows)
    sums[...] = jnp.zeros(sums.shape, F32)
    for copy in mid_copies:
        copy.wait()
    mid_x, mid_z = block_x // 2 + 4, block_z // 2 + 4
    around = []
    for count in range(27):
        moves = (count // 9 - 1, count // 3 % 3 - 1, count % 3 - 1)
        there = [lax.rem(at[axis] + moves[axis] + numbers[axis], numbers[axis]) for axis in range(3)]
        around.append(((there[0] * numbers[1] + there[1]) * numbers[2] + there[2]) * 8)
    for z in range(mid_z):
        for x in range(mid_x):
            line = (z % 2 * 2 + x % 2) * 2
            listed = []
            for y in range(3):
                base = around[(x // 2 * 3 + y) * 3 + z // 2]
                listed.append(mids[pl.ds(base + line, 2), :])
            listed.append(jnp.zeros((2, LANES), F32))
            held = jnp.concatenate(listed, axis=0)
            start = guard + (z * mid_x + x) * 8
            for kind, value in enumerate(third(held)):
                upper, lower = halved(value)
                mid_high[kind, start : start + 8, :] = upper
                mid_low[kind, start : start + 8, :] = lower

    def fill_mids(z, carry):
        for shift in range(-3, 4):
            spot = ((shift + 3) * wide_z + z) * starts
            for kind in range(3):
                made = []
                for x in range(mid_x):
                    start = guard + (z * mid_x + x) * 8 + 2 + shift
                    page = jnp.where(
                        row8 < 2,
                        mid_high[kind, pl.ds(start, 8), :],
                        mid_low[kind, pl.ds(start - 2, 8), :],
                    )
                    made.append(parity(page, shift))
                moved = [pltpu.roll(page, 4, 0) for page in made]
                listed = [(x, made[x], moved[x + 1]) for x in range(mid_x - 1)]
                listed += [(7, zero8, moved[0]), (8, made[5], zero8)]
                for entry, low, high in listed:
                    page = jnp.where(row8 < 4, low, high)
                    pages[3 + kind, spot + entry] = jnp.concatenate([page, page], axis=0).astype(BF16)
        return carry

    lax.fori_loop(0, mid_z, fill_mids, 0)

    each_other(wait_upper)
    raised = arrived[:, 0, :]
    rank_row = lax.broadcasted_iota(jnp.int32, (devices, terms), 0)
    rank_octant = (
        4 * (rank_row // strides[0] % 2) + 2 * (rank_row // strides[1] % 2) + rank_row % 2
    )
    lifted = jnp.zeros((devices, terms), F32)
    for octant in range(8):
        found = apply(raised, octant_of(shift_rows, octant))
        lifted = jnp.where(rank_octant == octant, found, lifted)
    root = jnp.sum(lifted, axis=0, keepdims=True)
    top_rows = (tops + 7) // 8 * 8
    picker_row = lax.broadcasted_iota(jnp.int32, (top_rows, devices), 0)
    picker_rank = lax.broadcasted_iota(jnp.int32, (top_rows, devices), 1)
    parent_of = (
        picker_rank // strides[0] // 2 * top_strides[0]
        + picker_rank // strides[1] % numbers[1] // 2 * top_strides[1]
        + picker_rank % numbers[2] // 2
    )
    picker = (picker_row == parent_of).astype(F32)
    merged = lax.dot_general(
        picker, lifted, NN, precision=lax.Precision.HIGHEST, preferred_element_type=F32
    )
    merged = jnp.concatenate([merged, jnp.zeros((top_rows, LANES - terms), F32)], axis=1)
    for kind, value in enumerate(third(jnp.concatenate([raised, merged], axis=0))):
        upper, lower = halved(value)
        uppers[2 * kind] = upper
        uppers[2 * kind + 1] = lower

    def fill_uppers(line):
        def fill(entry, carry):
            for kind in range(3):
                high = jnp.broadcast_to(uppers[2 * kind, pl.ds(line[1] + entry, 1), :], (8, LANES))
                low = jnp.broadcast_to(uppers[2 * kind + 1, pl.ds(line[1] + entry, 1), :], (8, LANES))
                page = jnp.where(row8 == line[0], high, jnp.where(row8 == line[0] + 1, low, 0.0))
                upper_pages[kind, line[2] + entry] = jnp.concatenate([page, zero8], axis=0).astype(BF16)
            return carry

        return fill

    lax.fori_loop(0, devices, fill_uppers((0, 0, 0)), 0, unroll=8)
    lax.fori_loop(0, tops, fill_uppers((2, devices, devices + 1)), 0, unroll=4)
    for kind in range(3):
        upper_pages[kind, devices] = jnp.zeros((16, LANES), BF16)
        upper_pages[kind, devices + 1 + tops] = jnp.zeros((16, LANES), BF16)

    for copy in beside + relayed:
        copy.wait()
    def widen(z, carry):
        for x in range(wide_x):
            column = jnp.concatenate([raw[pair, z, x] for pair in range(pairs + 2)], axis=0)
            wide[pl.ds(pl.multiple_of(guard + (z * wide_x + x) * rows_y, 8), rows_y), :] = column
        return carry

    lax.fori_loop(0, wide_z, widen, 0)

    def window(tile, carry):
        start = pl.multiple_of(guard + tile * LANES, 8)
        turned = wide[pl.ds(start, LANES), :].T
        found = moments(
            turned[:SLOTS], turned[SLOTS : 2 * SLOTS], turned[2 * SLOTS : 3 * SLOTS], turned[3 * SLOTS :]
        )
        for kind, value in enumerate(third(found)):
            upper, lower = halved(value)
            moments_high[kind, pl.ds(start, LANES), :] = upper
            moments_low[kind, pl.ds(start, LANES), :] = lower
        return carry

    lax.fori_loop(0, wide_x * wide_z * rows_y // LANES, window, 0, unroll=4)

    near_shifts = [(x, y, z) for x in (-1, 0, 1) for y in (-1, 0, 1) for z in (-1, 0, 1)]
    lane8 = lax.broadcasted_iota(jnp.int32, (8, LANES), 1)
    group8 = lane8 // SLOTS

    def shifted(shift):
        moved = jnp.where(
            group8 == 0,
            float(shift[0]),
            jnp.where(group8 == 1, float(shift[1]), jnp.where(group8 == 2, float(shift[2]), 0.0)),
        )
        found = []
        for z in range(block_z):
            for x in range(0, block_x, 2):
                spot = (z + HALO + shift[2]) * wide_x + x + HALO + shift[0]
                low = guard + spot * rows_y + HALO + shift[1]
                high = low + rows_y - block_y
                held = jnp.where(row8 < block_y, wide[low : low + 8, :], wide[high : high + 8, :])
                found.append(held + moved)
        return found

    for pair in range((len(near_shifts) + 1) // 2):
        first = shifted(near_shifts[2 * pair])
        if 2 * pair + 1 < len(near_shifts):
            second = shifted(near_shifts[2 * pair + 1])
        else:
            second = [jnp.where(group8 < 3, value, 0.0) for value in first]
        sources[pair * LANES : (pair + 1) * LANES, :] = jnp.concatenate(first + second, axis=0).T

    def fill_pages(z, carry):
        for shift in range(-3, 4):
            spot = ((shift + 3) * wide_z + z) * starts
            for kind in range(3):
                made = []
                for x in range(wide_x):
                    start = guard + (z * wide_x + x) * rows_y + HALO + shift
                    page = jnp.where(
                        row8 < block_y,
                        moments_high[kind, pl.ds(start, 8), :],
                        moments_low[kind, pl.ds(start - block_y, 8), :],
                    )
                    made.append(parity(page, shift))
                listed = [(x, made[x], made[x + 1]) for x in range(wide_x - 1)]
                listed += [(7, zero8, made[0]), (9, zero8, made[2])]
                listed += [(8, made[5], zero8), (10, made[7], zero8)]
                for entry, low, high in listed:
                    pages[kind, spot + entry] = jnp.concatenate([low, high], axis=0).astype(BF16)
        return carry

    lax.fori_loop(0, wide_z, fill_pages, 0)

    lane16 = lax.broadcasted_iota(jnp.int32, (16, LANES), 1)
    first_part = lane16 < terms
    second_part = lane16 < 2 * terms - LANES

    first_eight = lax.broadcasted_iota(jnp.int32, (16, LANES), 0) < 8

    def far_rows(triple):
        rows = [3 * triple + kind for kind in range(3)]
        spots = [[plan_ref[row * PLAN + odd] for odd in range(2)] for row in rows]

        def tiles(held):
            return jnp.concatenate(
                [
                    jnp.where(first_part, held[0], held[1]),
                    jnp.where(second_part, held[1], held[2]),
                ],
                axis=1,
            )

        found = []
        for z in range(block_z):
            for x in range(block_x // 2):
                step = z // 2 * 2 * starts + 2 * x
                found.append(tiles([pages[kind, spots[kind][z % 2] + step] for kind in range(3)]))
        held = []
        for kind in range(3):
            even, odd = pages[3 + kind, spots[kind][0]], pages[3 + kind, spots[kind][1]]
            held.append(jnp.where(first_eight, even, odd))
        found.append(tiles(held))
        held = []
        for kind, row in enumerate(rows):
            held.append(upper_pages[kind, reach[2 * row]] + upper_pages[kind, reach[2 * row + 1]])
        found.append(tiles(held))
        return jnp.concatenate(found, axis=0)

    total_rows = 2 * leaves + 32
    near_steps = sources.shape[0] // LANES // 2

    def near_step(step, totals):
        sum_p, sum_x, sum_y, sum_z = totals
        for row in range(2 * SLOTS):
            base = step * (2 * LANES) + row // SLOTS * LANES
            line = row % SLOTS
            s_x = sources[pl.ds(base + line, 1), :]
            s_y = sources[pl.ds(base + line + SLOTS, 1), :]
            s_z = sources[pl.ds(base + line + 2 * SLOTS, 1), :]
            s_q = sources[pl.ds(base + line + 3 * SLOTS, 1), :]
            d_x = targets[:SLOTS] - s_x
            d_y = targets[SLOTS : 2 * SLOTS] - s_y
            d_z = targets[2 * SLOTS : 3 * SLOTS] - s_z
            inverse = lax.rsqrt(d_x * d_x + d_y * d_y + d_z * d_z + SOFTENING)
            weight = s_q * inverse
            sum_p = sum_p + weight
            cubic = weight * (inverse * inverse)
            sum_x = sum_x + cubic * d_x
            sum_y = sum_y + cubic * d_y
            sum_z = sum_z + cubic * d_z
        return sum_p, sum_x, sum_y, sum_z

    def far_step(step, carry):
        added = []
        for which in range(14):
            pair = step * 14 + which
            left = jnp.concatenate([far_rows(2 * pair), far_rows(2 * pair + 1)], axis=1)
            added.append(lax.dot_general(left, operators[jnp.minimum(pair, used - 1)], NT, preferred_element_type=F32))
        total = added[0]
        for value in added[1:]:
            total = total + value
        sums[...] += total
        return carry

    lax.fori_loop(0, STEPS * GROUP // 28, far_step, 0)
    zero = jnp.zeros((SLOTS, LANES), F32)
    near = lax.fori_loop(0, near_steps, near_step, (zero, zero, zero, zero))

    first = 2 * leaves + 16
    held = sums[first : first + 8, :terms]
    far_upper = held[0:1] + held[1:2]
    far_top = held[2:3] + held[3:4]

    def lattice_apply(value):
        return apply(jnp.broadcast_to(value, (8, terms)), lattice[...])

    def wider(value):
        return jnp.concatenate([value, jnp.zeros((value.shape[0], LANES - terms), F32)], axis=1)

    top_local = 0.125 * (far_top + lattice_apply(root)[:1])
    octant = lax.rem(at[0], 2) * 4 + lax.rem(at[1], 2) * 2 + lax.rem(at[2], 2)
    moved = apply(jnp.broadcast_to(wider(top_local), (8, LANES)), octant_of(down_rows, octant))
    upper_local = jnp.broadcast_to(wider(0.25 * far_upper + moved[:1]), (8, LANES))
    mid_row = lax.broadcasted_iota(jnp.int32, (8, terms), 0)
    mid_octant = 4 * (mid_row // 2 % 2) + 2 * (mid_row % 2) + mid_row // 4
    held = sums[2 * leaves : 2 * leaves + 16, :terms]
    lines = []
    for z in range(2):
        for x in range(2):
            start = z * 8 + x * 4
            lines.append(held[start : start + 2] + held[start + 2 : start + 4])
    far_mid = jnp.concatenate(lines, axis=0)
    downward = [octant_of(down_rows, entry) for entry in range(8)]
    moved = jnp.zeros((8, terms), F32)
    for entry in range(8):
        moved = jnp.where(mid_octant == entry, apply(upper_local, downward[entry]), moved)
    mid_local = wider(0.5 * far_mid + moved)
    expanded = []
    for z in range(block_z):
        for x in range(block_x // 2):
            line = (z // 2 * 2 + x) * 2
            low = jnp.broadcast_to(mid_local[line : line + 1], (8, LANES))
            high = jnp.broadcast_to(mid_local[line + 1 : line + 2], (8, LANES))
            expanded.append(jnp.where(row8 % 4 < 2, low, high))
    expanded = jnp.concatenate(expanded, axis=0)
    moved = jnp.zeros((leaves, terms), F32)
    for entry in range(8):
        moved = jnp.where(leaf_octant == entry, apply(expanded, downward[entry]), moved)
    row_t = lax.broadcasted_iota(jnp.int32, (8, terms), 0)
    lines = []
    for spot in range(leaves // 8):
        low = sums[spot * 16 : spot * 16 + 8, :terms]
        high = sums[spot * 16 + 8 : spot * 16 + 16, :terms]
        low = low + pltpu.roll(low, 4, 0)
        high = high + pltpu.roll(high, 4, 0)
        lines.append(jnp.where(row_t < 4, low, high))
    local = wider(moved + jnp.concatenate(lines, axis=0))
    local_rows[...] = jnp.concatenate([local, local], axis=0).T

    u_x = targets[:SLOTS] - 0.5
    u_y = targets[SLOTS : 2 * SLOTS] - 0.5
    u_z = targets[2 * SLOTS : 3 * SLOTS] - 0.5
    value = grad_x = grad_y = grad_z = None
    for a in range(ORDER, -1, -1):
        inner = inner_y = inner_z = None
        for b in range(ORDER - a, -1, -1):
            here = local_rows[ROW_OF[(a, b, 0)] : ROW_OF[(a, b, 0)] + 1, :]
            if (a, b, 1) in ROW_OF:
                above = local_rows[ROW_OF[(a, b, 1)] : ROW_OF[(a, b, 1)] + 1, :]
                both = here + above * u_z
                inner_z = above if inner_z is None else inner_z * u_y + above
            else:
                both = here
            if inner is None:
                inner = jnp.broadcast_to(both, (SLOTS, LANES))
            else:
                inner_y = inner if inner_y is None else inner_y * u_y + inner
                inner = inner * u_y + both
        if value is None:
            value, grad_y, grad_z = inner, inner_y, inner_z
        else:
            grad_x = value if grad_x is None else grad_x * u_x + value
            value = value * u_x + inner
            if inner_y is not None:
                grad_y = inner_y if grad_y is None else grad_y * u_x + inner_y
            if inner_z is not None:
                grad_z = inner_z if grad_z is None else grad_z * u_x + inner_z

    def halves(total):
        return total + pltpu.roll(total, leaves, 1)

    self_term = targets[3 * SLOTS :] * (SOFTENING**-0.5)
    results = [
        halves(near[0]) - self_term + value,
        halves(near[1]) - grad_x,
        halves(near[2]) - grad_y,
        halves(near[3]) - grad_z,
    ]
    turned = jnp.concatenate(results, axis=0).T
    for entry in range(4):
        made = None
        for z in range(block_z):
            turn = (z - entry) * SLOTS % LANES
            held = turned[z * columns : (z + 1) * columns]
            held = pltpu.roll(held, turn, 1) if turn else held
            made = held if made is None else jnp.where(group == z, held, made)
        made = made * live
        for x in range(block_x):
            piece = made[x * block_y : (x + 1) * block_y]
            result_ref[entry, x] = piece


def part_kernel(result_ref, potential_ref, field_ref, sems):
    copies = [
        pltpu.make_async_copy(result_ref.at[0], potential_ref, sems.at[0]),
        pltpu.make_async_copy(result_ref.at[pl.ds(1, 3)], field_ref, sems.at[1]),
    ]
    for copy in copies:
        copy.start()
    for copy in copies:
        copy.wait()


def per_device(
    positions, charges, counts, moment_shift, far_operators, local_shift, lattice_operator
):
    block_x, block_y, column = charges.shape
    block_z = column // SLOTS
    sizes = (block_x, block_y, block_z)
    numbers = tuple(lax.axis_size(axis) for axis in ("gx", "gy", "gz"))
    devices = numbers[0] * numbers[1] * numbers[2]
    terms = moment_shift.shape[1]
    padded_terms = (terms + 15) // 16 * 16
    leaves = block_x * block_y * block_z
    plan, triples, none, starts = plan_table(block_x, block_z)
    offsets = offset_table().shape[0]
    wide_x, wide_z = block_x + 2 * HALO, block_z + 2 * HALO
    wide_leaves = wide_x * wide_z * (block_y + 2 * HALO)
    mid_columns = (block_x // 2 + 4) * (block_z // 2 + 4)
    tops = devices // 8
    anywhere = pl.BlockSpec(memory_space=pltpu.HBM)
    vmem = pl.BlockSpec(memory_space=pltpu.VMEM)
    layout = (triples, none, starts)
    batches = -(-offsets // (6 * PLACED))
    top_rows = (tops + 7) // 8 * 8
    placed = batches * PLACED
    spare = (placed * 6 * terms + 2 * LANES - far_operators.shape[1] + LANES) // LANES * LANES
    result = pl.pallas_call(
        lambda *refs: field_kernel(sizes, numbers, layout, *refs),
        out_shape=pltpu.VMEM((4, block_x, block_y, column), F32),
        in_specs=[anywhere] * 8,
        out_specs=vmem,
        scratch_shapes=[
            pltpu.VMEM(positions.shape, F32),
            pltpu.VMEM(charges.shape, F32),
            pltpu.VMEM(counts.shape, jnp.int32),
            pltpu.VMEM((terms, 8, terms), BF16),
            pltpu.VMEM((terms, far_operators.shape[1] + spare), BF16),
            pltpu.VMEM((terms, 8, terms), BF16),
            pltpu.VMEM((terms, terms), BF16),
            pltpu.VMEM((block_y // 2 + 2, wide_z, wide_x, 2, LANES), F32),
            pltpu.VMEM((wide_leaves + 16, LANES), F32),
            pltpu.VMEM((4 * SLOTS, LANES), F32),
            pltpu.VMEM((padded_terms * 8, LANES), F32),
            pltpu.VMEM((3, wide_leaves + 16, LANES), F32),
            pltpu.VMEM((3, wide_leaves + 16, LANES), F32),
            pltpu.VMEM((devices * 8, LANES), F32),
            pltpu.VMEM((terms * 8, LANES), F32),
            pltpu.VMEM((terms * 8, LANES), F32),
            pltpu.VMEM((6, devices + top_rows, LANES), F32),
            pltpu.VMEM((placed, padded_terms, 4 * LANES), BF16),
            pltpu.VMEM((14 * LANES, LANES), F32),
            pltpu.VMEM((6, none + 2 * starts + 3, 16, LANES), BF16),
            pltpu.VMEM((3, mid_columns * 8 + 16, LANES), F32),
            pltpu.VMEM((3, mid_columns * 8 + 16, LANES), F32),
            pltpu.VMEM((3, devices + tops + 2, 16, LANES), BF16),
            pltpu.VMEM((2 * leaves + 32, padded_terms), F32),
            pltpu.VMEM((LANES, LANES), F32),
            pltpu.SMEM(plan.shape, jnp.int32),
            pltpu.SMEM((4 * LANES,), jnp.int32),
            pltpu.SMEM((triples * 6,), jnp.int32),
            pltpu.SemaphoreType.DMA((8,)),
            pltpu.SemaphoreType.DMA((27,)),
            pltpu.SemaphoreType.DMA((27,)),
            pltpu.SemaphoreType.DMA((27,)),
            pltpu.SemaphoreType.DMA((27,)),
            pltpu.VMEM((devices, 1, LANES), F32),
            pltpu.SemaphoreType.DMA((devices,)),
            pltpu.SemaphoreType.DMA((devices,)),
        ],
        compiler_params=pltpu.CompilerParams(
            vmem_limit_bytes=60 * 1024 * 1024, collective_id=0, has_side_effects=True
        ),
        name="fields",
    )(
        jnp.asarray(plan),
        positions,
        charges,
        counts,
        jnp.transpose(moment_shift, (1, 0, 2)),
        far_operators,
        jnp.transpose(local_shift, (1, 0, 2)),
        lattice_operator,
    )
    return pl.pallas_call(
        part_kernel,
        out_shape=(
            jax.ShapeDtypeStruct((block_x, block_y, column), F32),
            jax.ShapeDtypeStruct((3, block_x, block_y, column), F32),
        ),
        in_specs=[vmem],
        out_specs=(anywhere, anywhere),
        scratch_shapes=[pltpu.SemaphoreType.DMA((2,))],
        compiler_params=pltpu.CompilerParams(vmem_limit_bytes=4 * 1024 * 1024),
        name="part",
    )(result)


def solution(mesh):
    placed = (
        P(None, "gx", "gy", "gz"),
        P("gx", "gy", "gz"),
        P("gx", "gy", "gz"),
        P(),
        P(),
        P(),
        P(),
    )
    return jax.shard_map(
        per_device,
        mesh=mesh,
        in_specs=placed,
        out_specs=(P("gx", "gy", "gz"), P(None, "gx", "gy", "gz")),
        check_vma=False,
    )
```
